32 devices in a mesh: dp: 16 (over z, x, core), rep: 2 (over y).
Axes of the slice: x: 2, y: 2, z: 4, core: 2. Of those that a mesh axis runs over, the one named last changes fastest.
Arguments:
- tokens: bfloat16 [48, 261, 768], P('dp'), may hold values from -6 to 6
- text_len: int32 [48], P('dp'), may hold values from 1 to 64, as said below
- routes: int32 [48, 261], P('dp'), may hold values from 0 to 2, as said below
- attn_gain: float32 [768], replicated, may hold values from 0.5 to 1.5
- attn_shift: float32 [768], replicated, may hold values from -1 to 1
- w_qkv: bfloat16 [3, 768, 768], P(None, 'dp', 'rep'), may hold values from -0.21875 to 0.21875
- b_qv: float32 [2, 768], P(None, 'rep'), may hold values from -1.5 to 1.5
- w_out: bfloat16 [768, 768], P('dp', 'rep'), may hold values from -1.25 to 1.25
- b_out: float32 [768], replicated, may hold values from -0.5 to 0.5
- ffn_gain: float32 [768], replicated, may hold values from 0.5 to 1.5
- ffn_shift: float32 [768], replicated, may hold values from -1 to 1
- w_up: bfloat16 [3, 768, 3072], P(None, 'dp', 'rep'), may hold values from -0.21875 to 0.21875
- b_up: float32 [3, 3072], P(None, 'rep'), may hold values from -1.5 to 1.5
- w_down: bfloat16 [3, 768, 3072], P(None, 'dp', 'rep'), may hold values from -0.15625 to 0.15625
- b_down: float32 [3, 768], replicated, may hold values from -0.5 to 0.5
- cotangent: bfloat16 [48, 261, 768], P('dp'), may hold values from -6 to 6
Outputs:
- output: bfloat16 [48, 261, 768], P('dp')
- grad_tokens: float32 [48, 261, 768], P('dp')
- grad_w_qkv: float32 [3, 768, 768], P(None, 'dp', 'rep')
- grad_w_out: float32 [768, 768], P('dp', 'rep')
- grad_w_up: float32 [3, 768, 3072], P(None, 'dp', 'rep')
- grad_w_down: float32 [3, 768, 3072], P(None, 'dp', 'rep')
- grad_b_qv: float32 [2, 768], P(None, 'rep')
- grad_b_out: float32 [768], replicated
- grad_b_up: float32 [3, 3072], P(None, 'rep')
- grad_b_down: float32 [3, 768], replicated
- grad_norms: float32 [4, 768], replicated
The draws below stay inside these ranges and needn't reach their ends.
Inputs may be any that keep to these rules, and one draw needn't show every extreme that they name: `text_len`: text rows in use of each item; some item uses all 64 in every draw. `routes`: routing by modality: each item either sends its first 197 rows to expert 0 and its other rows to expert 1, or sends all its rows to expert 2; both kinds of item occur in every draw.
All inputs are finite; a program needn't handle non-finite values.
Results may differ from the reference program's by a relative error of at most 0.014.
Values may be sent and summed in bfloat16 or wider, within the bound.
No kernel may reach another device: no remote copies, remote signals or barrier semaphores. Data moves between devices by JAX's collectives and lax.ppermute only.
A program may use at most 192 MiB of HBM per device.

```python
import math
import jax
import jax.numpy as jnp
from jax import lax

D = 768
HEADS = 12
HDIM = 64
FF = 3072
EXPERTS = 3
IMG = 197
TXT = 64
SEQ = 261
ITEMS_DEV = 3
ITEMS = 48
N_DP = 16


def draw_text_len(key, part):
    first_key = jax.random.fold_in(key, 11)
    second_key = jax.random.fold_in(key, 23)
    lengths = jax.random.randint(first_key, (ITEMS,), 1, TXT + 1)
    chosen = jax.random.randint(second_key, (), 0, ITEMS)
    return jnp.where(jnp.arange(ITEMS) == chosen, TXT, lengths).astype(jnp.int32)


def draw_routes(key, part):
    kind_key = jax.random.fold_in(key, 37)
    order_key = jax.random.fold_in(key, 41)
    joint_item = jax.random.randint(kind_key, (ITEMS,), 0, 3) == 0
    order = jax.random.permutation(order_key, ITEMS)
    item_ids = jnp.arange(ITEMS)
    joint_item = jnp.where(item_ids == order[0], False, joint_item)
    joint_item = jnp.where(item_ids == order[1], True, joint_item)
    split_rows = (jnp.arange(SEQ) >= IMG).astype(jnp.int32)[None, :]
    return jnp.where(joint_item[:, None], 2, split_rows).astype(jnp.int32)


def block_scale(stream_key, extent, shards, low, largest):
    factor_of = 1.0
    for axis_at, blocks in shards:
        steps = jax.random.uniform(jax.random.fold_in(jax.random.fold_in(stream_key, 6), axis_at), (blocks,), jnp.float32, low / len(shards), largest / len(shards))
        factor_of = factor_of * jnp.repeat(jnp.exp(steps), extent[axis_at] // blocks).reshape((-1,) + (1,) * (len(extent) - 1 - axis_at))
    return factor_of


def noise(stream_key, extent, deviation, reach, cuts=(), kind=jnp.bfloat16):
    entries = deviation * jax.random.normal(stream_key, extent, jnp.float32)
    if cuts:
        entries = entries * block_scale(stream_key, extent, cuts, -0.22, 0.18)
    return jnp.clip(entries, -reach, reach).astype(kind)


def setup_inputs(seed: int = 0) -> dict:
    splits = jax.random.split(jax.random.key(seed), 17)
    tokens = noise(splits[0], (ITEMS, SEQ, D), 1.0, 6.0, ((0, 16),))
    text_len = draw_text_len(jax.random.fold_in(splits[16], 71), 0)
    routes = draw_routes(jax.random.fold_in(splits[16], 71), 0)
    attn_gain = jnp.clip(1.0 + 0.1 * jax.random.normal(splits[3], (D,), jnp.float32), 0.5, 1.5)
    attn_shift = noise(splits[4], (D,), 0.2, 1.0, (), jnp.float32)
    w_qkv = noise(splits[5], (3, D, D), D ** -0.5, 0.21875, ((1, 16), (2, 2)))
    b_qv = noise(splits[6], (2, D), 0.3, 1.5, ((1, 2),), jnp.float32)
    w_out = noise(splits[7], (D, D), (D // 32) ** -0.5, 1.25, ((0, 16), (1, 2)))
    b_out = noise(splits[8], (D,), 0.1, 0.5, (), jnp.float32)
    ffn_gain = jnp.clip(1.0 + 0.1 * jax.random.normal(splits[9], (D,), jnp.float32), 0.5, 1.5)
    ffn_shift = noise(splits[10], (D,), 0.2, 1.0, (), jnp.float32)
    w_up = noise(splits[11], (EXPERTS, D, FF), D ** -0.5, 0.21875, ((1, 16), (2, 2)))
    b_up = noise(splits[12], (EXPERTS, FF), 0.3, 1.5, ((1, 2),), jnp.float32)
    w_down = noise(splits[13], (EXPERTS, D, FF), (FF // 2) ** -0.5, 0.15625, ((1, 16), (2, 2)))
    b_down = noise(splits[14], (EXPERTS, D), 0.1, 0.5, (), jnp.float32)
    cotangent = noise(splits[15], (ITEMS, SEQ, D), 1.0, 6.0, ((0, 16),))
    return dict(tokens=tokens, text_len=text_len, routes=routes, attn_gain=attn_gain, attn_shift=attn_shift, w_qkv=w_qkv, b_qv=b_qv, w_out=w_out, b_out=b_out, ffn_gain=ffn_gain, ffn_shift=ffn_shift, w_up=w_up, b_up=b_up, w_down=w_down, b_down=b_down, cotangent=cotangent)


@jax.custom_vjp
def low(v):
    return lax.optimization_barrier(v.astype(jnp.bfloat16)).astype(jnp.float32)

@jax.custom_vjp
def low_back(v):
    return v

def low_keep(v):
    return (low(v), None)

def low_pass(kept, grad):
    return (grad,)

def back_keep(v):
    return (v, None)

def back_low(kept, grad):
    return (low(grad),)
low.defvjp(low_keep, low_pass)
low_back.defvjp(back_keep, back_low)
HIGHEST = lax.Precision.HIGHEST
EPSILON = 1e-05

def norm_rows(vector, gain_vec, shift_vec):
    row_mean = lax.optimization_barrier(jnp.mean(vector, axis=-1, keepdims=True))
    centred = vector - row_mean
    row_var = lax.optimization_barrier(jnp.mean(centred * centred, axis=-1, keepdims=True))
    return centred * lax.rsqrt(row_var + EPSILON) * gain_vec + shift_vec

def block_forward(params, portion, text_lengths, route_ids):
    attn_gain, attn_shift, w_qkv, b_qv, w_out, b_out, ffn_gain, ffn_shift, w_up, b_up, w_down, b_down = params
    item_count = portion.shape[0]
    row_count = item_count * SEQ
    inputs = portion.reshape(row_count, D)
    first_normed = low(norm_rows(inputs, attn_gain, attn_shift))
    projected = jnp.einsum('rd,tde->tre', first_normed, w_qkv, precision=HIGHEST)
    bias_rows = jnp.stack([b_qv[0], jnp.zeros_like(b_qv[0]), b_qv[1]])
    projected = low(low_back(projected + bias_rows[:, None, :]))
    head_split = projected.reshape(3, item_count, SEQ, HEADS, HDIM)
    queries, key_rows, values = (head_split[0], head_split[1], head_split[2])
    score_scale = 1.0 / math.sqrt(HDIM)
    raw_scores = jnp.einsum('ishd,ijhd->ihsj', queries, key_rows, precision=HIGHEST) * score_scale
    key_ok = jnp.arange(SEQ, dtype=jnp.int32)[None, :] < (IMG + text_lengths)[:, None]
    raw_scores = jnp.where(key_ok[:, None, None, :], raw_scores, -1e+30)
    raw_scores = low_back(raw_scores)
    attn_probs = low(jax.nn.softmax(raw_scores, axis=-1))
    context = jnp.einsum('ihsj,ijhd->ishd', attn_probs, values, precision=HIGHEST).reshape(row_count, D)
    context = low(low_back(context))
    branch_one = low_back(jnp.dot(context, w_out.T, precision=HIGHEST) + b_out)
    residual = inputs + branch_one
    second_normed = low(norm_rows(residual, ffn_gain, ffn_shift))
    pre_act = jnp.einsum('rd,edf->erf', second_normed, w_up, precision=HIGHEST) + b_up[:, None, :]
    pre_act = low_back(pre_act)
    active = low(jax.nn.gelu(pre_act, approximate=False))
    expert_out = jnp.einsum('erf,edf->erd', active, w_down, precision=HIGHEST)
    route_pick = (route_ids.reshape(row_count)[None, :] == jnp.arange(EXPERTS, dtype=jnp.int32)[:, None]).astype(jnp.float32)
    branch_two = lax.optimization_barrier(jnp.sum(route_pick[:, :, None] * expert_out, axis=0)) + jnp.dot(route_pick.T, b_down, precision=HIGHEST)
    branch_two = low_back(branch_two)
    return (residual + branch_two).reshape(item_count, SEQ, D)

def reference(tokens, text_len, routes, attn_gain, attn_shift, w_qkv, b_qv, w_out, b_out, ffn_gain, ffn_shift, w_up, b_up, w_down, b_down, cotangent):
    params = tuple((arr.astype(jnp.float32) for arr in (attn_gain, attn_shift, w_qkv, b_qv, w_out, b_out, ffn_gain, ffn_shift, w_up, b_up, w_down, b_down)))
    inputs = tokens.astype(jnp.float32)
    length_blocks = text_len.reshape(N_DP, ITEMS_DEV)
    route_blocks = routes.reshape(N_DP, ITEMS_DEV, SEQ)

    def forward(all_rows, weights):

        def one_block(running, portion):
            return (running, block_forward(weights, portion[0], portion[1], portion[2]))
        _, result = lax.scan(jax.checkpoint(one_block), jnp.zeros((), jnp.float32), (all_rows.reshape(N_DP, ITEMS_DEV, SEQ, D), length_blocks, route_blocks))
        return result.reshape(ITEMS, SEQ, D)
    result, pullback = jax.vjp(forward, inputs, params)
    grad_tokens, grads = pullback(cotangent.astype(jnp.float32))
    grad_norms = jnp.stack([grads[0], grads[1], grads[6], grads[7]])
    return (result.astype(jnp.bfloat16), grad_tokens, grads[2], grads[4], grads[8], grads[10], grads[3], grads[5], grads[9], grads[11], grad_norms)
```

```python
import functools
import math

import jax
import jax.numpy as jnp
from jax import lax
from jax.experimental import pallas as pl
from jax.experimental.pallas import tpu as pltpu
from jax.sharding import PartitionSpec as P

HDIM = 64
IMG = 197
EPSILON = 1e-05
ROOT_HALF = 0.7071067811865476
INV_ROOT_TAU = 0.3989422804014327
SUB = 16
LANES = 128
BF = jnp.bfloat16
F32 = jnp.float32

NN = (((1,), (0,)), ((), ()))
NT = (((1,), (1,)), ((), ()))
TN = (((0,), (0,)), ((), ()))


def up_to(n, m):
    return -(-n // m) * m


def dot(a, b, dims):
    return lax.dot_general(a, b, dims, preferred_element_type=F32)


def full(shape):
    zeros = (0,) * len(shape)
    return pl.BlockSpec(shape, lambda *_: zeros)


def per_item(shape):
    zeros = (0,) * (len(shape) - 1)
    return pl.BlockSpec(shape, lambda i, *_: (i,) + zeros)


ANY = pl.BlockSpec(memory_space=pl.ANY)


def params():
    return pltpu.CompilerParams(vmem_limit_bytes=60 * 1024 * 1024)


def cost(flops, nbytes, trans=0):
    return pl.CostEstimate(flops=int(flops), transcendentals=int(trans), bytes_accessed=int(nbytes))


def normed(v):
    centred = v - jnp.mean(v, axis=-1, keepdims=True)
    var = jnp.mean(centred * centred, axis=-1, keepdims=True)
    spread = lax.rsqrt(var + EPSILON)
    return centred * spread, spread


def norm_back(grad, hat, spread, gain):
    scaled = grad * gain
    return spread * (
        scaled
        - jnp.mean(scaled, axis=-1, keepdims=True)
        - hat * jnp.mean(scaled * hat, axis=-1, keepdims=True)
    )


def place_copies(off_ref, pieces, dest, sems):
    copies = []
    for n, piece in enumerate(pieces):
        subs, _, rows, _ = piece.shape
        for j in range(subs):
            at = off_ref[n * subs + j]
            copies.append(
                pltpu.make_async_copy(
                    piece.at[j],
                    dest.at[:, pl.ds(pl.multiple_of(at, SUB), rows), :],
                    sems.at[n * subs + j],
                )
            )
    return copies


def k_proj(off_ref, tok_ref, gain_ref, shift_ref, bias_ref, *rest):
    a_ref, qkv_ref, w_ref, sems = rest[-4:]
    pieces = rest[:-4]
    first = pl.program_id(0) == 0

    @pl.when(first)
    def _():
        for c in place_copies(off_ref, pieces, w_ref, sems):
            c.start()

    hat, _ = normed(tok_ref[0].astype(F32))
    a_ref[0] = (hat * gain_ref[...] + shift_ref[...]).astype(BF)

    @pl.when(first)
    def _():
        for c in place_copies(off_ref, pieces, w_ref, sems):
            c.wait()

    a = a_ref[0]
    for t in range(3):
        qkv_ref[t, 0] = (dot(a, w_ref[t], NN) + bias_ref[t : t + 1, :]).astype(BF)


def project(tokens, gain, shift, bias, pieces, offsets):
    items, rows, width = tokens.shape
    planes, cols = pieces[0].shape[1], pieces[0].shape[3]
    count = len(pieces) * pieces[0].shape[0]
    grid_spec = pltpu.PrefetchScalarGridSpec(
        num_scalar_prefetch=1,
        grid=(items,),
        in_specs=[
            per_item((1, rows, width)),
            full((1, width)),
            full((1, width)),
            full((3, cols)),
        ]
        + [ANY] * len(pieces),
        out_specs=[
            per_item((1, rows, width)),
            pl.BlockSpec((3, 1, rows, cols), lambda i, *_: (0, i, 0, 0)),
            full((planes, width, cols)),
        ],
        scratch_shapes=[pltpu.SemaphoreType.DMA((count,))],
    )
    return pl.pallas_call(
        k_proj,
        grid_spec=grid_spec,
        out_shape=[
            jax.ShapeDtypeStruct((items, rows, width), BF),
            jax.ShapeDtypeStruct((3, items, rows, cols), BF),
            jax.ShapeDtypeStruct((planes, width, cols), BF),
        ],
        compiler_params=params(),
        cost_estimate=cost(2 * items * rows * width * 3 * cols, 8 * width * cols * 2),
        name="project",
    )(offsets, tokens, gain[None], shift[None], bias, *pieces)


def k_attend(len_ref, q_ref, k_ref, v_ref, c_ref, *, scale):
    rows, width = c_ref.shape
    valid = lax.broadcasted_iota(jnp.int32, (1, rows), 1) < IMG + len_ref[0]
    low = lax.broadcasted_iota(jnp.int32, (1, LANES), 1) < HDIM
    for pair in range(width // LANES):
        cols = slice(pair * LANES, (pair + 1) * LANES)
        q, k, v = q_ref[0, 0, :, cols], k_ref[0, 0, :, cols], v_ref[0, 0, :, cols]
        both = []
        for side in (low, ~low):
            s = dot(q * side.astype(BF), k, NT) * scale
            s = jnp.where(valid, s, -1e30)
            e = jnp.exp(s - jnp.max(s, axis=-1, keepdims=True))
            p = (e / jnp.sum(e, axis=-1, keepdims=True)).astype(BF)
            both.append(dot(p, v, NN))
        c_ref[:, cols] = jnp.where(low, both[0], both[1]).astype(BF)


def attend(item, text_len, qkv, scale):
    _, _, rows, cols = qkv.shape
    spec = [
        pl.BlockSpec((1, 1, rows, cols), lambda i, *_, t=t: (t, item, 0, 0)) for t in range(3)
    ]
    grid_spec = pltpu.PrefetchScalarGridSpec(
        num_scalar_prefetch=1,
        grid=(1,),
        in_specs=spec,
        out_specs=full((rows, cols)),
    )
    return pl.pallas_call(
        functools.partial(k_attend, scale=scale),
        grid_spec=grid_spec,
        out_shape=jax.ShapeDtypeStruct((rows, cols), BF),
        compiler_params=params(),
        cost_estimate=cost(4 * rows * rows * cols * 4, 8 * rows * cols, rows * rows * 6),
        name="attend",
    )(text_len[item : item + 1], qkv, qkv, qkv)


def k_residual(tok_ref, cm_ref, cp_ref, wm_ref, wp_ref, bias_ref, gain_ref, shift_ref, h_ref, b_ref):
    y = dot(cm_ref[...], wm_ref[0], NT) + dot(cp_ref[...], wp_ref[0], NT)
    h = tok_ref[0].astype(F32) + (y + bias_ref[...])
    h_ref[...] = h
    hat, _ = normed(h)
    b_ref[...] = (hat * gain_ref[...] + shift_ref[...]).astype(BF)


def residual(item, tokens, mine, theirs, w_mine, w_theirs, bias, gain, shift):
    _, rows, width = tokens.shape
    cols = mine.shape[1]
    last = w_mine.shape[0] - 1
    return pl.pallas_call(
        k_residual,
        grid=(1,),
        in_specs=[
            pl.BlockSpec((1, rows, width), lambda i: (item, 0, 0)),
            full((rows, cols)),
            full((rows, cols)),
            pl.BlockSpec((1, width, cols), lambda i: (last, 0, 0)),
            full((1, width, cols)),
            full((1, width)),
            full((1, width)),
            full((1, width)),
        ],
        out_specs=[full((rows, width)), full((rows, width))],
        out_shape=[
            jax.ShapeDtypeStruct((rows, width), F32),
            jax.ShapeDtypeStruct((rows, width), BF),
        ],
        compiler_params=params(),
        cost_estimate=cost(4 * rows * cols * width, 10 * rows * width),
        name="residual",
    )(tokens, mine, theirs, w_mine, w_theirs, bias[None], gain[None], shift[None])


def segments(rows):
    head = up_to(IMG, SUB)
    tail = IMG // SUB * SUB
    return (0, head), (tail, rows - tail), head


def segment_masks(rows):
    (a0, an), (b0, bn), _ = segments(rows)
    in_a = lax.broadcasted_iota(jnp.int32, (an, 1), 0) + a0 < IMG
    in_b = lax.broadcasted_iota(jnp.int32, (bn, 1), 0) + b0 >= IMG
    return in_a, in_b


def masked_parts(g_ref):
    rows = g_ref.shape[1]
    (a0, an), (b0, bn), _ = segments(rows)
    in_a, in_b = segment_masks(rows)
    g_a = jnp.where(in_a, g_ref[0, a0 : a0 + an, :].astype(F32), 0.0)
    g_b = jnp.where(in_b, g_ref[0, b0 : b0 + bn, :].astype(F32), 0.0)
    return g_a, g_b


def write_chunks(slot_ref, acc_ref, outs):
    _, total, width = acc_ref.shape
    count = sum(o.shape[0] for o in outs)
    rows = total // count
    per = outs[0].shape[0]
    for c in range(count):
        slot = slot_ref[c]
        for n, out in enumerate(outs):

            @pl.when((slot >= n * per) & (slot < (n + 1) * per))
            def _(out=out, n=n):
                out[slot - n * per] = acc_ref[:, c * rows : (c + 1) * rows, :].astype(BF)


def k_up(e_ref, off_ref, slot_ref, b_ref, g_ref, bias_ref, *rest, n_out, own):
    scratch = rest[-3:]
    w_s, dw_s, sems = scratch
    outs = rest[-3 - n_out - 3 : -3]
    act_ref, slope_ref, gbd_ref = outs[:3]
    dw_refs = outs[3:]
    pieces = rest[: -3 - n_out - 3]
    i = pl.program_id(0)

    @pl.when(i == 0)
    def _():
        for c in place_copies(off_ref, pieces, w_s, sems):
            c.start()
        dw_s[...] = jnp.zeros_like(dw_s)
        gbd_ref[...] = jnp.zeros_like(gbd_ref)
        for c in place_copies(off_ref, pieces, w_s, sems):
            c.wait()

    rows = b_ref.shape[1]
    seg_a, seg_b, head = segments(rows)
    at = 0
    for which, (lo, n), g in zip((0, 1), (seg_a, seg_b), masked_parts(g_ref)):
        e = e_ref[which, i]
        u = dot(b_ref[0, lo : lo + n, :], w_s[e], NN) + bias_ref[pl.ds(e, 1), :]
        cdf = 0.5 * (1.0 + lax.erf(u * ROOT_HALF))
        act = (u * cdf).astype(BF)
        act_ref[0, at : at + n, :] = act
        slope_ref[0, at : at + n, :] = (cdf + u * jnp.exp(-0.5 * u * u) * INV_ROOT_TAU).astype(BF)
        dw_s[e] += dot(g.astype(BF), act, TN)

        @pl.when(i < own)
        def _(g=g, e=e):
            gbd_ref[pl.ds(e, 1), :] += jnp.sum(g, axis=0, keepdims=True)

        at += n

    @pl.when(i == pl.num_programs(0) - 1)
    def _():
        write_chunks(slot_ref, dw_s, dw_refs)


def chunk_outs(chunks):
    return [full(c) for c in chunks], [jax.ShapeDtypeStruct(c, BF) for c in chunks]


def experts_up(experts, offsets, slots, b, g, bias, pieces, chunks, own):
    items, rows, width = b.shape
    e_count, _, hidden = pieces[0].shape[1:]
    count = len(pieces) * pieces[0].shape[0]
    (_, an), (_, bn), _ = segments(rows)
    chunk_specs, chunk_shapes = chunk_outs(chunks)
    grid_spec = pltpu.PrefetchScalarGridSpec(
        num_scalar_prefetch=3,
        grid=(items,),
        in_specs=[per_item((1, rows, width)), per_item((1, rows, width)), full((e_count, hidden))]
        + [ANY] * len(pieces),
        out_specs=[
            per_item((1, an + bn, hidden)),
            per_item((1, an + bn, hidden)),
            full((e_count, width)),
        ]
        + chunk_specs,
        scratch_shapes=[
            pltpu.VMEM((e_count, width, hidden), BF),
            pltpu.VMEM((e_count, width, hidden), F32),
            pltpu.SemaphoreType.DMA((count,)),
        ],
    )
    return pl.pallas_call(
        functools.partial(k_up, n_out=len(chunks), own=own),
        grid_spec=grid_spec,
        out_shape=[
            jax.ShapeDtypeStruct((items, an + bn, hidden), BF),
            jax.ShapeDtypeStruct((items, an + bn, hidden), BF),
            jax.ShapeDtypeStruct((e_count, width), F32),
        ]
        + chunk_shapes,
        compiler_params=params(),
        cost_estimate=cost(
            4 * items * rows * width * hidden, 8 * e_count * width * hidden, items * rows * hidden
        ),
        name="experts_up",
    )(experts, offsets, slots, b, g, bias, *pieces)


def k_back(e_ref, off_ref, g_ref, slope_ref, *rest, n_up):
    w_up, w_down, sem_up, sem_down = rest[-4:]
    du_ref, db_ref, gbu_ref = rest[-7:-4]
    ups, downs = rest[:n_up], rest[n_up:-7]
    i = pl.program_id(0)

    @pl.when(i == 0)
    def _():
        for c in place_copies(off_ref, downs, w_down, sem_down):
            c.start()
        for c in place_copies(off_ref, ups, w_up, sem_up):
            c.start()
        gbu_ref[...] = jnp.zeros_like(gbu_ref)
        for c in place_copies(off_ref, downs, w_down, sem_down):
            c.wait()
        for c in place_copies(off_ref, ups, w_up, sem_up):
            c.wait()

    rows = g_ref.shape[1]
    seg_a, seg_b, head = segments(rows)
    tail = seg_b[0]
    at = 0
    both = []
    for which, (lo, n), g in zip((0, 1), (seg_a, seg_b), masked_parts(g_ref)):
        e = e_ref[which, i]
        dact = dot(g.astype(BF), w_down[e], NN)
        du = (dact * slope_ref[0, at : at + n, :].astype(F32)).astype(BF)
        du_ref[0, at : at + n, :] = du
        gbu_ref[pl.ds(e, 1), :] += jnp.sum(du.astype(F32), axis=0, keepdims=True)
        both.append(dot(du, w_up[e], NT))
        at += n
    db_ref[0, :tail, :] = both[0][:tail].astype(BF)
    db_ref[0, tail:head, :] = (both[0][tail:] + both[1][: head - tail]).astype(BF)
    db_ref[0, head:, :] = both[1][head - tail :].astype(BF)


def experts_back(experts, offsets, g, slope, ups, downs):
    items, rows, width = g.shape
    e_count, _, hidden = ups[0].shape[1:]
    count = len(ups) * ups[0].shape[0]
    seg_rows = slope.shape[1]
    grid_spec = pltpu.PrefetchScalarGridSpec(
        num_scalar_prefetch=2,
        grid=(items,),
        in_specs=[per_item((1, rows, width)), per_item((1, seg_rows, hidden))]
        + [ANY] * (len(ups) + len(downs)),
        out_specs=[
            per_item((1, seg_rows, hidden)),
            per_item((1, rows, width)),
            full((e_count, hidden)),
        ],
        scratch_shapes=[
            pltpu.VMEM((e_count, width, hidden), BF),
            pltpu.VMEM((e_count, width, hidden), BF),
            pltpu.SemaphoreType.DMA((count,)),
            pltpu.SemaphoreType.DMA((count,)),
        ],
    )
    return pl.pallas_call(
        functools.partial(k_back, n_up=len(ups)),
        grid_spec=grid_spec,
        out_shape=[
            jax.ShapeDtypeStruct((items, seg_rows, hidden), BF),
            jax.ShapeDtypeStruct((items, rows, width), BF),
            jax.ShapeDtypeStruct((e_count, hidden), F32),
        ],
        compiler_params=params(),
        cost_estimate=cost(4 * items * rows * width * hidden, 8 * e_count * width * hidden),
        name="experts_back",
    )(experts, offsets, g, slope, *ups, *downs)


def k_up_grad(e_ref, slot_ref, b_ref, du_ref, *rest):
    dw_s = rest[-1]
    dw_refs = rest[:-1]
    i = pl.program_id(0)

    @pl.when(i == 0)
    def _():
        dw_s[...] = jnp.zeros_like(dw_s)

    seg_a, seg_b, _ = segments(b_ref.shape[1])
    at = 0
    for which, (lo, n) in zip((0, 1), (seg_a, seg_b)):
        e = e_ref[which, i]
        dw_s[e] += dot(b_ref[0, lo : lo + n, :], du_ref[0, at : at + n, :], TN)
        at += n

    @pl.when(i == pl.num_programs(0) - 1)
    def _():
        write_chunks(slot_ref, dw_s, dw_refs)


def experts_up_grad(experts, slots, b, du, chunks, e_count):
    items, rows, width = b.shape
    seg_rows, hidden = du.shape[1:]
    chunk_specs, chunk_shapes = chunk_outs(chunks)
    grid_spec = pltpu.PrefetchScalarGridSpec(
        num_scalar_prefetch=2,
        grid=(items,),
        in_specs=[per_item((1, rows, width)), per_item((1, seg_rows, hidden))],
        out_specs=chunk_specs,
        scratch_shapes=[pltpu.VMEM((e_count, width, hidden), F32)],
    )
    return pl.pallas_call(
        k_up_grad,
        grid_spec=grid_spec,
        out_shape=chunk_shapes,
        compiler_params=params(),
        cost_estimate=cost(2 * items * rows * width * hidden, 4 * e_count * width * hidden),
        name="experts_up_grad",
    )(experts, slots, b, du)


def k_down(e_ref, off_ref, act_ref, *rest):
    z_ref, w_down, sems = rest[-3:]
    pieces = rest[:-3]
    i = pl.program_id(0)

    @pl.when(i == 0)
    def _():
        for c in place_copies(off_ref, pieces, w_down, sems):
            c.start()
        for c in place_copies(off_ref, pieces, w_down, sems):
            c.wait()

    rows = z_ref.shape[1]
    seg_a, seg_b, head = segments(rows)
    tail = seg_b[0]
    z_a = dot(act_ref[0, : seg_a[1], :], w_down[e_ref[0, i]], NT)
    z_b = dot(act_ref[0, seg_a[1] :, :], w_down[e_ref[1, i]], NT)
    image = lax.broadcasted_iota(jnp.int32, (head - tail, 1), 0) + tail < IMG
    z_ref[0, :tail, :] = z_a[:tail].astype(BF)
    z_ref[0, tail:head, :] = jnp.where(image, z_a[tail:], z_b[: head - tail]).astype(BF)
    z_ref[0, head:, :] = z_b[head - tail :].astype(BF)


def experts_down(experts, offsets, act, pieces, rows):
    items, seg_rows, hidden = act.shape
    e_count = pieces[0].shape[1]
    width = sum(p.shape[0] * p.shape[2] for p in pieces)
    count = len(pieces) * pieces[0].shape[0]
    grid_spec = pltpu.PrefetchScalarGridSpec(
        num_scalar_prefetch=2,
        grid=(items,),
        in_specs=[per_item((1, seg_rows, hidden))] + [ANY] * len(pieces),
        out_specs=per_item((1, rows, width)),
        scratch_shapes=[
            pltpu.VMEM((e_count, width, hidden), BF),
            pltpu.SemaphoreType.DMA((count,)),
        ],
    )
    return pl.pallas_call(
        k_down,
        grid_spec=grid_spec,
        out_shape=jax.ShapeDtypeStruct((items, rows, width), BF),
        compiler_params=params(),
        cost_estimate=cost(2 * items * rows * width * hidden, 4 * e_count * width * hidden),
        name="experts_down",
    )(experts, offsets, act, *pieces)


def k_output(e_ref, h_ref, zm_ref, zp_ref, bias_ref, o_ref):
    i = pl.program_id(0)
    rows, keep = h_ref.shape[1], o_ref.shape[1]
    image = lax.broadcasted_iota(jnp.int32, (rows, 1), 0) < IMG
    bias = jnp.where(image, bias_ref[pl.ds(e_ref[0, i], 1), :], bias_ref[pl.ds(e_ref[1, i], 1), :])
    out = h_ref[0] + ((zm_ref[0].astype(F32) + zp_ref[0].astype(F32)) + bias)
    o_ref[0] = out[:keep].astype(BF)


def finish_output(experts, h, mine, theirs, bias, keep):
    items, rows, width = h.shape
    grid_spec = pltpu.PrefetchScalarGridSpec(
        num_scalar_prefetch=1,
        grid=(items,),
        in_specs=[per_item((1, rows, width))] * 3 + [full(bias.shape)],
        out_specs=per_item((1, keep, width)),
    )
    return pl.pallas_call(
        k_output,
        grid_spec=grid_spec,
        out_shape=jax.ShapeDtypeStruct((items, keep, width), BF),
        compiler_params=params(),
        cost_estimate=cost(8 * items * rows * width, 10 * items * rows * width),
        name="finish_output",
    )(experts, h, mine, theirs, bias)


def k_attend_back(
    len_ref, dm_ref, dp_ref, h_ref, g_ref, tok_ref, q_ref, k_ref, v_ref, w_ref, fgain_ref, again_ref,
    dh_ref, dy_ref, dqkv_ref, da_ref, sums_ref, bias_ref, *, scale,
):
    rows, width = dh_ref.shape
    cols = q_ref.shape[3]
    db = dm_ref[...].astype(F32) + dp_ref[...].astype(F32)
    hat, spread = normed(h_ref[...])
    dh = g_ref[0].astype(F32) + norm_back(db, hat, spread, fgain_ref[...])
    dh_ref[...] = dh
    dy = dh.astype(BF)
    dy_ref[...] = dy
    sums_ref[0:1, :] = jnp.sum(db * hat, axis=0, keepdims=True)
    sums_ref[1:2, :] = jnp.sum(db, axis=0, keepdims=True)
    sums_ref[2:3, :] = jnp.sum(dy.astype(F32), axis=0, keepdims=True)
    dctx = dot(dy, w_ref[3], NN).astype(BF)
    valid = lax.broadcasted_iota(jnp.int32, (rows, 1), 0) < IMG + len_ref[0]
    low = lax.broadcasted_iota(jnp.int32, (1, LANES), 1) < HDIM
    for pair in range(cols // LANES):
        at = slice(pair * LANES, (pair + 1) * LANES)
        q, k, v = q_ref[0, 0, :, at], k_ref[0, 0, :, at], v_ref[0, 0, :, at]
        dc = dctx[:, at]
        parts = []
        for side in (low, ~low):
            only = side.astype(BF)
            s = dot(k * only, q, NT) * scale
            s = jnp.where(valid, s, -1e30)
            e = jnp.exp(s - jnp.max(s, axis=0, keepdims=True))
            p = e / jnp.sum(e, axis=0, keepdims=True)
            dp = dot(v * only, dc, NT)
            ds = (p * (dp - jnp.sum(p * dp, axis=0, keepdims=True))).astype(BF)
            parts.append((dot(ds, k, TN), dot(ds, q, NN), dot(p.astype(BF), dc, NN)))
        dqkv_ref[0, :, at] = (jnp.where(low, parts[0][0], parts[1][0]) * scale).astype(BF)
        dqkv_ref[1, :, at] = (jnp.where(low, parts[0][1], parts[1][1]) * scale).astype(BF)
        dqkv_ref[2, :, at] = jnp.where(low, parts[0][2], parts[1][2]).astype(BF)
    da = dot(dqkv_ref[0], w_ref[0], NT)
    da += dot(dqkv_ref[1], w_ref[1], NT)
    da += dot(dqkv_ref[2], w_ref[2], NT)
    bias_ref[0:1, :] = jnp.sum(dqkv_ref[0].astype(F32), axis=0, keepdims=True)
    bias_ref[1:2, :] = jnp.sum(dqkv_ref[2].astype(F32), axis=0, keepdims=True)
    hat, _ = normed(tok_ref[0].astype(F32))
    sums_ref[3:4, :] = jnp.sum(da * hat, axis=0, keepdims=True)
    sums_ref[4:5, :] = jnp.sum(da, axis=0, keepdims=True)
    da_ref[...] = da.astype(BF)


def attend_back(item, text_len, mine, theirs, h, g, tokens, qkv, weights, ffn_gain, attn_gain, scale):
    rows, width = h.shape
    cols = qkv.shape[3]
    item_spec = pl.BlockSpec((1, rows, width), lambda i, *_: (item, 0, 0))
    grid_spec = pltpu.PrefetchScalarGridSpec(
        num_scalar_prefetch=1,
        grid=(1,),
        in_specs=[full((rows, width))] * 3
        + [item_spec, item_spec]
        + [pl.BlockSpec((1, 1, rows, cols), lambda i, *_, t=t: (t, item, 0, 0)) for t in range(3)]
        + [full(weights.shape), full((1, width)), full((1, width))],
        out_specs=[
            full((rows, width)),
            full((rows, width)),
            full((3, rows, cols)),
            full((rows, width)),
            full((5, width)),
            full((2, cols)),
        ],
    )
    return pl.pallas_call(
        functools.partial(k_attend_back, scale=scale),
        grid_spec=grid_spec,
        out_shape=[
            jax.ShapeDtypeStruct((rows, width), F32),
            jax.ShapeDtypeStruct((rows, width), BF),
            jax.ShapeDtypeStruct((3, rows, cols), BF),
            jax.ShapeDtypeStruct((rows, width), BF),
            jax.ShapeDtypeStruct((5, width), F32),
            jax.ShapeDtypeStruct((2, cols), F32),
        ],
        compiler_params=params(),
        cost_estimate=cost(
            8 * rows * cols * width + 20 * rows * rows * cols, 30 * rows * width, rows * rows * 6
        ),
        name="attend_back",
    )(
        text_len[item : item + 1], mine, theirs, h, g, tokens, qkv, qkv, qkv, weights,
        ffn_gain[None], attn_gain[None],
    )


def k_attn_grad(slot_ref, *rest, items, n_out):
    acc = rest[-1]
    outs = rest[-1 - n_out : -1]
    a_refs, d_refs = rest[:items], rest[items : 2 * items]
    y_refs, c_refs = rest[2 * items : 3 * items], rest[3 * items : 4 * items]
    for n in range(items):
        for t in range(4):
            left, right = (a_refs[n][0], d_refs[n][t]) if t < 3 else (y_refs[n][...], c_refs[n][...])
            part = dot(left, right, TN)
            if n == 0:
                acc[t] = part
            else:
                acc[t] += part
    write_chunks(slot_ref, acc, outs)


def attn_grad(slots, a, dqkv, dy, ctx, chunks):
    items, rows, width = a.shape
    cols = ctx[0].shape[1]
    chunk_specs, chunk_shapes = chunk_outs(chunks)
    grid_spec = pltpu.PrefetchScalarGridSpec(
        num_scalar_prefetch=1,
        grid=(1,),
        in_specs=[
            pl.BlockSpec((1, rows, width), lambda i, *_, n=n: (n, 0, 0)) for n in range(items)
        ]
        + [full((3, rows, cols))] * items
        + [full((rows, width))] * items
        + [full((rows, cols))] * items,
        out_specs=chunk_specs,
        scratch_shapes=[pltpu.VMEM((4, width, cols), F32)],
    )
    return pl.pallas_call(
        functools.partial(k_attn_grad, items=items, n_out=len(chunks)),
        grid_spec=grid_spec,
        out_shape=chunk_shapes,
        compiler_params=params(),
        cost_estimate=cost(8 * items * rows * width * cols, 16 * width * cols),
        name="attn_grad",
    )(slots, *([a] * items), *dqkv, *dy, *ctx)


def k_token_grad(dh_ref, dm_ref, dp_ref, tok_ref, gain_ref, buf_ref, o_ref):
    del buf_ref
    keep = o_ref.shape[1]
    da = dm_ref[...].astype(F32) + dp_ref[...].astype(F32)
    hat, spread = normed(tok_ref[0].astype(F32))
    out = dh_ref[...] + norm_back(da, hat, spread, gain_ref[...])
    o_ref[0] = out[:keep]


def token_grad(item, dh, mine, theirs, tokens, gain, buffer):
    rows, width = dh.shape
    keep = buffer.shape[1]
    return pl.pallas_call(
        k_token_grad,
        grid=(1,),
        in_specs=[full((rows, width))] * 3
        + [pl.BlockSpec((1, rows, width), lambda i: (item, 0, 0)), full((1, width)), ANY],
        out_specs=pl.BlockSpec((1, keep, width), lambda i: (item, 0, 0)),
        out_shape=jax.ShapeDtypeStruct(buffer.shape, F32),
        input_output_aliases={5: 0},
        compiler_params=params(),
        cost_estimate=cost(10 * rows * width, 14 * rows * width),
        name="token_grad",
    )(dh, mine, theirs, tokens, gain[None], buffer)


def swap(value, axis, size, mask):
    return lax.ppermute(value, axis, [(i, i ^ mask) for i in range(size)])


def spread_pieces(own, masks, size):
    held = [(0, own)]
    for mask in masks:
        held = held + [(r | mask, swap(piece, "dp", size, mask)) for r, piece in held]
    return held


def after(value, *others):
    return lax.optimization_barrier((value,) + others)[0]


def add_low(a, b):
    return (a.astype(F32) + b.astype(F32)).astype(BF)


def fold_chunks(chunk, masks, size):
    for n, mask in enumerate(masks):
        half = chunk.shape[0] // 2
        got = swap(chunk[half:], "dp", size, mask)
        if n == len(masks) - 1:
            return chunk[:half].astype(F32) + got.astype(F32)
        chunk = add_low(chunk[:half], got)
    return chunk.astype(F32)


def per_device(
    tokens, text_len, routes, attn_gain, attn_shift, w_qkv, b_qv, w_out, b_out, ffn_gain, ffn_shift,
    w_up, b_up, w_down, b_down, cotangent, *, dp, rep,
):
    items, seq, width = tokens.shape
    rows = up_to(seq, SUB)
    share = w_qkv.shape[1]
    cols = w_qkv.shape[2]
    hidden = w_up.shape[2] // 2
    e_count = w_up.shape[0]
    scale = 1.0 / math.sqrt(HDIM)
    me = lax.axis_index("dp")
    core = me % 2
    by_permute = share % SUB == 0
    gather_masks = [m for m in (4, 8, 16, 32, 64, 128) if m < dp] + [2]
    fold_masks = [2] + [m for m in (128, 64, 32, 16, 8, 4) if m < dp]

    def peer(value):
        return lax.ppermute(value, "rep", [(i, i ^ 1) for i in range(rep)])

    def partner(value):
        return swap(value, "dp", dp, 1)

    pad = ((0, 0), (0, rows - seq), (0, 0))
    tok = jnp.pad(tokens, pad)
    cot = jnp.pad(cotangent, pad)

    attn_shard = jnp.concatenate([w_qkv, w_out[None]], axis=0)
    my_half = lax.dynamic_slice_in_dim(w_up, core * hidden, hidden, 2)
    other_half = lax.dynamic_slice_in_dim(w_up, (1 - core) * hidden, hidden, 2)
    my_half_d = lax.dynamic_slice_in_dim(w_down, core * hidden, hidden, 2)
    other_half_d = lax.dynamic_slice_in_dim(w_down, (1 - core) * hidden, hidden, 2)
    if by_permute:
        held = spread_pieces(attn_shard[None], gather_masks, dp)
        held = held + [(r ^ 1, partner(p)) for r, p in held]
        attn_pieces = [p for _, p in held]
        attn_off = jnp.stack([(me ^ r) * share for r, _ in held]).astype(jnp.int32)
        up_own = jnp.stack([my_half, partner(other_half)])
        down_own = jnp.stack([my_half_d, partner(other_half_d)])
        up_own = after(up_own, held[dp // 2 - 1][1])
        up_held = spread_pieces(up_own, gather_masks, dp)
        down_own = after(down_own, up_held[-1][1])
        down_held = spread_pieces(down_own, gather_masks, dp)
        up_pieces, down_pieces = [p for _, p in up_held], [p for _, p in down_held]
        ffn_off = jnp.stack(
            [(me ^ r ^ j) * share for r, _ in up_held for j in (0, 1)]
        ).astype(jnp.int32)
        ids = jnp.arange(dp, dtype=jnp.int32) ^ me.astype(jnp.int32)
        slots = jnp.zeros_like(ids)
        weight = dp // 4
        for m in fold_masks:
            slots = slots + (ids & m) // m * weight
            weight //= 2
        slots = slots + (ids & 1) * (dp // 2)
        ffn_chunks = [(dp // 2, e_count, share, hidden)] * 2
        attn_chunks = [(dp // 2, 4, share, cols)] * 2
    else:
        attn_pieces = [lax.all_gather(attn_shard, "dp", axis=1, tiled=True)[None]]
        gathered = lax.all_gather(w_up, "dp", axis=1, tiled=True)
        up_pieces = [lax.dynamic_slice_in_dim(gathered, core * hidden, hidden, 2)[None]]
        gathered = lax.all_gather(w_down, "dp", axis=1, tiled=True)
        down_pieces = [lax.dynamic_slice_in_dim(gathered, core * hidden, hidden, 2)[None]]
        attn_off = ffn_off = slots = jnp.zeros((1,), jnp.int32)
        ffn_chunks = [(1, e_count, width, hidden)]
        attn_chunks = [(1, 4, width, cols)]

    experts = jnp.stack([routes[:, 0], routes[:, seq - 1]]).astype(jnp.int32)
    experts_two = jnp.concatenate([experts, partner(experts)], axis=1)
    cot_two = jnp.concatenate([cot, partner(cot)], axis=0)

    bias = jnp.stack([b_qv[0], jnp.zeros_like(b_qv[0]), b_qv[1]])
    a, qkv, attn_w = project(tok, attn_gain, attn_shift, bias, attn_pieces, attn_off)
    out_theirs = peer(attn_w[3:])
    ctx, h, b = [], [], []
    for n in range(items):
        ctx.append(attend(n, text_len, qkv, scale))
    ctx_theirs = [peer(c) for c in ctx]
    for n in range(items):
        h_n, b_n = residual(
            n, tok, ctx[n], ctx_theirs[n], attn_w, out_theirs, b_out, ffn_gain, ffn_shift
        )
        h.append(h_n)
        b.append(b_n)
    b_two = jnp.stack(b + [partner(v) for v in b])

    b_up_mine = lax.dynamic_slice_in_dim(b_up, core * hidden, hidden, 1)
    act, slope, grad_b_down, *down_grad = experts_up(
        experts_two, ffn_off, slots, b_two, cot_two, b_up_mine, up_pieces, ffn_chunks, items
    )
    du, db_two, grad_b_up = experts_back(
        experts_two, ffn_off, cot_two, slope, up_pieces, down_pieces
    )
    up_grad = experts_up_grad(experts_two, slots, b_two, du, ffn_chunks, e_count)
    db = [add_low(db_two[n], partner(db_two[items + n])) for n in range(items)]
    db_theirs = [peer(v) for v in db]

    z_two = experts_down(experts_two, ffn_off, act, down_pieces, rows)
    z = add_low(z_two[:items], partner(z_two[items:]))
    output = finish_output(experts, jnp.stack(h), z, peer(z), b_down, seq)

    dh, dy, dqkv, da, sums, bias_sums = [], [], [], [], 0.0, 0.0
    for n in range(items):
        dh_n, dy_n, dqkv_n, da_n, sums_n, bias_n = attend_back(
            n, text_len, db[n], db_theirs[n], h[n], cot, tok, qkv, attn_w, ffn_gain, attn_gain, scale
        )
        dh.append(dh_n)
        dy.append(dy_n)
        dqkv.append(dqkv_n)
        da.append(da_n)
        sums = sums + sums_n
        bias_sums = bias_sums + bias_n
    da_theirs = [peer(v) for v in da]
    attn_parts = attn_grad(slots, a, dqkv, dy, ctx, attn_chunks)
    grad_tokens = jnp.zeros((items, seq, width), F32)
    for n in range(items):
        grad_tokens = token_grad(n, dh[n], da[n], da_theirs[n], tok, attn_gain, grad_tokens)

    if by_permute:

        def finish(chunks):
            other = fold_chunks(chunks[1], fold_masks, dp)[0]
            own = fold_chunks(chunks[0], fold_masks, dp)[0]
            got = partner(other)
            first = core == 0
            return jnp.concatenate(
                [jnp.where(first, own, got), jnp.where(first, got, own)], axis=-1
            )

        grad_w_down = finish(down_grad)
        grad_w_up = finish(up_grad)
        merged = add_low(attn_parts[0], partner(attn_parts[1]))
        grad_attn = fold_chunks(merged, fold_masks, dp)[0]
        grad_w_qkv, grad_w_out = grad_attn[:3], grad_attn[3]
    else:

        def finish(chunk):
            whole = jnp.zeros((e_count, width, 2 * hidden), BF)
            whole = lax.dynamic_update_slice_in_dim(whole, chunk[0], core * hidden, 2)
            return lax.psum_scatter(whole, "dp", scatter_dimension=1, tiled=True).astype(F32)

        grad_w_down, grad_w_up = finish(down_grad[0]), finish(up_grad[0])
        grad_attn = lax.psum_scatter(attn_parts[0][0], "dp", scatter_dimension=1, tiled=True)
        grad_w_qkv, grad_w_out = grad_attn[:3].astype(F32), grad_attn[3].astype(F32)

    first_norm = sums[3:5]
    first_norm = first_norm + peer(first_norm)
    up_pair = jnp.zeros((2, e_count, hidden), F32)
    up_pair = lax.dynamic_update_slice_in_dim(up_pair, grad_b_up[None], core, 0)
    small = jnp.concatenate(
        [
            first_norm.reshape(-1),
            sums[0:3].reshape(-1),
            grad_b_down.reshape(-1),
            up_pair.reshape(-1),
            bias_sums.reshape(-1),
        ]
    ).reshape(-1, LANES)
    for mask in [1] + gather_masks:
        small = small + swap(small, "dp", dp, mask)
    small = small.reshape(-1)
    at = 0

    def take(*shape):
        nonlocal at
        n = math.prod(shape)
        piece = small[at : at + n].reshape(shape)
        at += n
        return piece

    norm_one, norm_two, grad_b_out = take(2, width), take(2, width), take(width)
    total_down = take(e_count, width)
    total_up = jnp.moveaxis(take(2, e_count, hidden), 0, 1).reshape(e_count, 2 * hidden)
    total_qv = take(2, cols)
    return (
        output,
        grad_tokens,
        grad_w_qkv,
        grad_w_out,
        grad_w_up,
        grad_w_down,
        total_qv,
        grad_b_out,
        total_up,
        total_down,
        jnp.concatenate([norm_one, norm_two], axis=0),
    )


def solution(mesh):
    body = functools.partial(per_device, dp=mesh.shape["dp"], rep=mesh.shape["rep"])
    return jax.shard_map(
        body,
        mesh=mesh,
        in_specs=(
            P("dp", None, None),
            P("dp"),
            P("dp", None),
            P(),
            P(),
            P(None, "dp", "rep"),
            P(None, "rep"),
            P("dp", "rep"),
            P(),
            P(),
            P(),
            P(None, "dp", "rep"),
            P(None, "rep"),
            P(None, "dp", "rep"),
            P(),
            P("dp", None, None),
        ),
        out_specs=(
            P("dp", None, None),
            P("dp", None, None),
            P(None, "dp", "rep"),
            P("dp", "rep"),
            P(None, "dp", "rep"),
            P(None, "dp", "rep"),
            P(None, "rep"),
            P(),
            P(None, "rep"),
            P(),
            P(),
        ),
        check_vma=False,
    )
```

```python
import functools
import math

import jax
import jax.numpy as jnp
from jax import lax
from jax.experimental import pallas as pl
from jax.experimental.pallas import tpu as pltpu
from jax.sharding import PartitionSpec as P

HDIM = 64
IMG = 197
EPSILON = 1e-05
ROOT_HALF = 0.7071067811865476
INV_ROOT_TAU = 0.3989422804014327
SUB = 16
LANES = 128
BF = jnp.bfloat16
F32 = jnp.float32

NN = (((1,), (0,)), ((), ()))
NT = (((1,), (1,)), ((), ()))
TN = (((0,), (0,)), ((), ()))


def up_to(n, m):
    return -(-n // m) * m


def dot(a, b, dims):
    return lax.dot_general(a, b, dims, preferred_element_type=F32)


def full(shape):
    zeros = (0,) * len(shape)
    return pl.BlockSpec(shape, lambda *_: zeros)


def per_item(shape):
    zeros = (0,) * (len(shape) - 1)
    return pl.BlockSpec(shape, lambda i, *_: (i,) + zeros)


ANY = pl.BlockSpec(memory_space=pl.ANY)


def params():
    return pltpu.CompilerParams(vmem_limit_bytes=60 * 1024 * 1024)


SHORT = pl.CostEstimate(flops=1, transcendentals=0, bytes_accessed=1)


def normed(v):
    centred = v - jnp.mean(v, axis=-1, keepdims=True)
    var = jnp.mean(centred * centred, axis=-1, keepdims=True)
    spread = lax.rsqrt(var + EPSILON)
    return centred * spread, spread


def norm_back(grad, hat, spread, gain):
    scaled = grad * gain
    return spread * (
        scaled
        - jnp.mean(scaled, axis=-1, keepdims=True)
        - hat * jnp.mean(scaled * hat, axis=-1, keepdims=True)
    )


def run_copies(copies, *, start=False, wait=False):
    for c in copies:
        if start:
            c.start()
        if wait:
            c.wait()


def place_copies(off_ref, pieces, dest, sems, plane=0):
    copies = []
    for n, piece in enumerate(pieces):
        subs, _, rows, _ = piece.shape
        for j in range(subs):
            at = off_ref[n * subs + j]
            copies.append(
                pltpu.make_async_copy(
                    piece.at[j, plane : plane + dest.shape[0]],
                    dest.at[:, pl.ds(pl.multiple_of(at, SUB), rows), :],
                    sems.at[n * subs + j],
                )
            )
    return copies


def k_proj(off_ref, tok_ref, vec_ref, bias_ref, *rest):
    a_ref, qkv_ref, w_ref, wo_ref, sems, out_sems = rest[-6:]
    pieces = rest[:-6]
    first = pl.program_id(0) == 0

    @pl.when(first)
    def _():
        run_copies(place_copies(off_ref, pieces, w_ref, sems), start=True)
        run_copies(place_copies(off_ref, pieces, wo_ref, out_sems, 3), start=True)

    hat, _ = normed(tok_ref[0].astype(F32))
    a_ref[0] = (hat * vec_ref[0:1, :] + vec_ref[1:2, :]).astype(BF)

    @pl.when(first)
    def _():
        run_copies(place_copies(off_ref, pieces, w_ref, sems), wait=True)
        run_copies(place_copies(off_ref, pieces, wo_ref, out_sems, 3), wait=True)

    a = a_ref[0]
    for t in range(3):
        qkv_ref[t, 0] = (dot(a, w_ref[t], NN) + bias_ref[t : t + 1, :]).astype(BF)


def project(tokens, vectors, bias, pieces, offsets):
    items, rows, width = tokens.shape
    cols = pieces[0].shape[3]
    count = len(pieces) * pieces[0].shape[0]
    grid_spec = pltpu.PrefetchScalarGridSpec(
        num_scalar_prefetch=1,
        grid=(items,),
        in_specs=[
            per_item((1, rows, width)),
            full(vectors.shape),
            full((3, cols)),
        ]
        + [ANY] * len(pieces),
        out_specs=[
            per_item((1, rows, width)),
            pl.BlockSpec((3, 1, rows, cols), lambda i, *_: (0, i, 0, 0)),
            full((3, width, cols)),
            full((1, width, cols)),
        ],
        scratch_shapes=[pltpu.SemaphoreType.DMA((count,)), pltpu.SemaphoreType.DMA((count,))],
    )
    return pl.pallas_call(
        k_proj,
        grid_spec=grid_spec,
        out_shape=[
            jax.ShapeDtypeStruct((items, rows, width), BF),
            jax.ShapeDtypeStruct((3, items, rows, cols), BF),
            jax.ShapeDtypeStruct((3, width, cols), BF),
            jax.ShapeDtypeStruct((1, width, cols), BF),
        ],
        compiler_params=params(),
        cost_estimate=SHORT,
        name="project",
    )(offsets, tokens, vectors, bias, *pieces)


def k_attend(len_ref, q_ref, k_ref, v_ref, c_ref, *, item, scale):
    rows, width = c_ref.shape
    valid = lax.broadcasted_iota(jnp.int32, (1, rows), 1) < IMG + len_ref[item]
    low = lax.broadcasted_iota(jnp.int32, (1, LANES), 1) < HDIM
    for pair in range(width // LANES):
        cols = slice(pair * LANES, (pair + 1) * LANES)
        q, k, v = q_ref[0, 0, :, cols], k_ref[0, 0, :, cols], v_ref[0, 0, :, cols]
        both = []
        for side in (low, ~low):
            s = dot(q * side.astype(BF), k, NT) * scale
            s = jnp.where(valid, s, -1e30)
            e = jnp.exp(s - jnp.max(s, axis=-1, keepdims=True))
            p = (e / jnp.sum(e, axis=-1, keepdims=True)).astype(BF)
            both.append(dot(p, v, NN))
        c_ref[:, cols] = jnp.where(low, both[0], both[1]).astype(BF)


def attend(item, text_len, qkv, scale):
    _, _, rows, cols = qkv.shape
    spec = [
        pl.BlockSpec((1, 1, rows, cols), lambda i, *_, t=t: (t, item, 0, 0)) for t in range(3)
    ]
    grid_spec = pltpu.PrefetchScalarGridSpec(
        num_scalar_prefetch=1,
        grid=(1,),
        in_specs=spec,
        out_specs=full((rows, cols)),
    )
    return pl.pallas_call(
        functools.partial(k_attend, item=item, scale=scale),
        grid_spec=grid_spec,
        out_shape=jax.ShapeDtypeStruct((rows, cols), BF),
        compiler_params=params(),
        cost_estimate=SHORT,
        name="attend",
    )(text_len, qkv, qkv, qkv)


def k_residual(tok_ref, cm_ref, cp_ref, wm_ref, wp_ref, vec_ref, *rest):
    h_ref, b_ref = rest[-2:]
    y = dot(cm_ref[...], wm_ref[0], NT) + dot(cp_ref[...], wp_ref[0], NT)
    h = tok_ref[0].astype(F32) + (y + vec_ref[2:3, :])
    h_ref[0] = h
    hat, _ = normed(h)
    b_ref[...] = (hat * vec_ref[3:4, :] + vec_ref[4:5, :]).astype(BF)


def residual(item, tokens, mine, theirs, w_mine, w_theirs, vectors, buffer):
    _, rows, width = tokens.shape
    cols = mine.shape[1]
    kept = [] if buffer is None else [buffer]
    return pl.pallas_call(
        k_residual,
        grid=(1,),
        in_specs=[
            pl.BlockSpec((1, rows, width), lambda i: (item, 0, 0)),
            full((rows, cols)),
            full((rows, cols)),
            full((1, width, cols)),
            full((1, width, cols)),
            full(vectors.shape),
        ]
        + [ANY] * len(kept),
        out_specs=[
            pl.BlockSpec((1, rows, width), lambda i: (item, 0, 0)),
            full((rows, width)),
        ],
        out_shape=[
            jax.ShapeDtypeStruct(tokens.shape, F32),
            jax.ShapeDtypeStruct((rows, width), BF),
        ],
        input_output_aliases={6: 0} if kept else {},
        compiler_params=params(),
        cost_estimate=SHORT,
        name="residual",
    )(tokens, mine, theirs, w_mine, w_theirs, vectors, *kept)


def segments(rows):
    head = up_to(IMG, SUB)
    tail = IMG // SUB * SUB
    return (0, head), (tail, rows - tail), head


def segment_masks(rows):
    (a0, an), (b0, bn), _ = segments(rows)
    in_a = lax.broadcasted_iota(jnp.int32, (an, 1), 0) + a0 < IMG
    in_b = lax.broadcasted_iota(jnp.int32, (bn, 1), 0) + b0 >= IMG
    return in_a, in_b


def masked_parts(g_ref, i):
    rows = g_ref.shape[1]
    (a0, an), (b0, bn), _ = segments(rows)
    in_a, in_b = segment_masks(rows)
    g_a = jnp.where(in_a, g_ref[i, a0 : a0 + an, :].astype(F32), 0.0)
    g_b = jnp.where(in_b, g_ref[i, b0 : b0 + bn, :].astype(F32), 0.0)
    return g_a, g_b


def item_copies(refs, dest, sems):
    copies = []
    for ref in refs:
        if len(ref.shape) == 2:
            copies.append(
                pltpu.make_async_copy(ref, dest.at[len(copies)], sems.at[len(copies)])
            )
        else:
            for j in range(ref.shape[0]):
                copies.append(
                    pltpu.make_async_copy(ref.at[j], dest.at[len(copies)], sems.at[len(copies)])
                )
    return copies


def wait_item(copies, i):
    for n, c in enumerate(copies):

        @pl.when(i == n)
        def _(c=c):
            c.wait()


def write_chunks(slot_ref, base, acc, stage, outs, sems):
    count, _, rows, _ = stage.shape
    for c in range(count):
        stage[slot_ref[base + c]] = acc[:, c * rows : (c + 1) * rows, :].astype(BF)
    per = count // len(outs)
    copies = [
        pltpu.make_async_copy(stage.at[n * per : (n + 1) * per], out, sems.at[n])
        for n, out in enumerate(outs)
    ]
    run_copies(copies, start=True)
    run_copies(copies, wait=True)


def k_up(e_ref, off_ref, bias_ref, *rest, items):
    b_refs, pieces = rest[:items], rest[items:-6]
    act_ref, slope_ref, b_s, w_s, b_sem, w_sem = rest[-6:]
    i = pl.program_id(0)
    b_copies = item_copies(b_refs, b_s, b_sem)

    @pl.when(i == 0)
    def _():
        run_copies(b_copies[:1], start=True)
        w_copies = place_copies(off_ref, pieces, w_s, w_sem)
        run_copies(w_copies, start=True)
        run_copies(b_copies[1:], start=True)
        run_copies(w_copies, wait=True)

    wait_item(b_copies, i)
    seg_a, seg_b, _ = segments(b_s.shape[1])
    at = 0
    for which, (lo, n) in zip((0, 1), (seg_a, seg_b)):
        e = e_ref[which, i]
        u = dot(b_s[i, lo : lo + n, :], w_s[e], NN) + bias_ref[pl.ds(e, 1), :]
        cdf = 0.5 * (1.0 + lax.erf(u * ROOT_HALF))
        act_ref[0, at : at + n, :] = (u * cdf).astype(BF)
        slope_ref[0, at : at + n, :] = (cdf + u * jnp.exp(-0.5 * u * u) * INV_ROOT_TAU).astype(BF)
        at += n


def experts_up(experts, offsets, b, bias, pieces):
    items = len(b)
    rows, width = b[0].shape
    e_count, _, hidden = pieces[0].shape[1:]
    count = len(pieces) * pieces[0].shape[0]
    (_, an), (_, bn), _ = segments(rows)
    grid_spec = pltpu.PrefetchScalarGridSpec(
        num_scalar_prefetch=2,
        grid=(items,),
        in_specs=[full((e_count, hidden))] + [ANY] * (items + len(pieces)),
        out_specs=[per_item((1, an + bn, hidden))] * 2,
        scratch_shapes=[
            pltpu.VMEM((items, rows, width), BF),
            pltpu.VMEM((e_count, width, hidden), BF),
            pltpu.SemaphoreType.DMA((items,)),
            pltpu.SemaphoreType.DMA((count,)),
        ],
    )
    return pl.pallas_call(
        functools.partial(k_up, items=items),
        grid_spec=grid_spec,
        out_shape=[jax.ShapeDtypeStruct((items, an + bn, hidden), BF)] * 2,
        compiler_params=params(),
        cost_estimate=SHORT,
        name="experts_up",
    )(experts, offsets, bias, *b, *pieces)


def k_weight_grad(e_ref, slot_ref, right_ref, *rest, n_left, n_out, base, own):
    lefts = rest[:n_left]
    outs = rest[n_left : n_left + n_out]
    left_s, dw_s, stage, left_sem, out_sem = rest[-5:]
    sums_ref = rest[n_left + n_out]
    i = pl.program_id(0)
    copies = item_copies(lefts, left_s, left_sem)

    @pl.when(i == 0)
    def _():
        run_copies(copies, start=True)
        dw_s[...] = jnp.zeros_like(dw_s)
        sums_ref[...] = jnp.zeros_like(sums_ref)

    wait_item(copies, i)
    at = 0
    for which, left in zip((0, 1), masked_parts(left_s, i)):
        e = e_ref[which, i]
        n = left.shape[0]
        dw_s[e] += dot(left.astype(BF), right_ref[0, at : at + n, :], TN)

        @pl.when(i < own)
        def _(left=left, e=e):
            sums_ref[pl.ds(e, 1), :] += jnp.sum(left, axis=0, keepdims=True)

        at += n

    @pl.when(i == pl.num_programs(0) - 1)
    def _():
        write_chunks(slot_ref, base, dw_s, stage, outs, out_sem)


def weight_grad(experts, slots, base, left, right, chunk, n_out, e_count, own):
    items, seg_rows, hidden = right.shape
    rows, width = left[0].shape[-2:]
    count = chunk[0] * n_out
    grid_spec = pltpu.PrefetchScalarGridSpec(
        num_scalar_prefetch=2,
        grid=(items,),
        in_specs=[per_item((1, seg_rows, hidden))] + [ANY] * len(left),
        out_specs=[ANY] * n_out + [full((e_count, width))],
        scratch_shapes=[
            pltpu.VMEM((items, rows, width), BF),
            pltpu.VMEM((e_count, width, hidden), F32),
            pltpu.VMEM((count,) + chunk[1:], BF),
            pltpu.SemaphoreType.DMA((items,)),
            pltpu.SemaphoreType.DMA((n_out,)),
        ],
    )
    return pl.pallas_call(
        functools.partial(
            k_weight_grad, n_left=len(left), n_out=n_out, base=base, own=own
        ),
        grid_spec=grid_spec,
        out_shape=[jax.ShapeDtypeStruct(chunk, BF)] * n_out
        + [jax.ShapeDtypeStruct((e_count, width), F32)],
        compiler_params=params(),
        cost_estimate=SHORT,
        name="weight_grad",
    )(experts, slots, right, *left)


def k_back(e_ref, off_ref, slope_ref, *rest, n_left, n_up, items):
    g_s, w_up, w_down, sem_g, sem_up, sem_down = rest[-6:]
    du_ref, gbu_ref = rest[-8:-6]
    db_refs = rest[-8 - items : -8]
    lefts, ups, downs = rest[:n_left], rest[n_left : n_left + n_up], rest[n_left + n_up : -8 - items]
    i = pl.program_id(0)
    copies = item_copies(lefts, g_s, sem_g)

    @pl.when(i == 0)
    def _():
        w_copies = place_copies(off_ref, downs, w_down, sem_down)
        run_copies(copies[:1] + w_copies, start=True)
        more = place_copies(off_ref, ups, w_up, sem_up)
        run_copies(more + copies[1:], start=True)
        gbu_ref[...] = jnp.zeros_like(gbu_ref)
        run_copies(w_copies + more, wait=True)

    wait_item(copies, i)
    rows = g_s.shape[1]
    seg_a, seg_b, head = segments(rows)
    tail = seg_b[0]
    at = 0
    both = []
    for which, g in zip((0, 1), masked_parts(g_s, i)):
        e = e_ref[which, i]
        n = g.shape[0]
        dact = dot(g.astype(BF), w_down[e], NN)
        du = (dact * slope_ref[0, at : at + n, :].astype(F32)).astype(BF)
        du_ref[0, at : at + n, :] = du
        gbu_ref[pl.ds(e, 1), :] += jnp.sum(du.astype(F32), axis=0, keepdims=True)
        both.append(dot(du, w_up[e], NT))
        at += n
    middle = both[0][tail:] + both[1][: head - tail]
    for n, db_ref in enumerate(db_refs):

        @pl.when(i == n)
        def _(db_ref=db_ref):
            db_ref[:tail, :] = both[0][:tail].astype(BF)
            db_ref[tail:head, :] = middle.astype(BF)
            db_ref[head:, :] = both[1][head - tail :].astype(BF)


def experts_back(experts, offsets, left, slope, ups, downs):
    rows, width = left[0].shape[-2:]
    e_count, _, hidden = ups[0].shape[1:]
    count = len(ups) * ups[0].shape[0]
    items, seg_rows, _ = slope.shape
    grid_spec = pltpu.PrefetchScalarGridSpec(
        num_scalar_prefetch=2,
        grid=(items,),
        in_specs=[per_item((1, seg_rows, hidden))]
        + [ANY] * (len(left) + len(ups) + len(downs)),
        out_specs=[full((rows, width))] * items
        + [per_item((1, seg_rows, hidden)), full((e_count, hidden))],
        scratch_shapes=[
            pltpu.VMEM((items, rows, width), BF),
            pltpu.VMEM((e_count, width, hidden), BF),
            pltpu.VMEM((e_count, width, hidden), BF),
            pltpu.SemaphoreType.DMA((items,)),
            pltpu.SemaphoreType.DMA((count,)),
            pltpu.SemaphoreType.DMA((count,)),
        ],
    )
    out = pl.pallas_call(
        functools.partial(k_back, n_left=len(left), n_up=len(ups), items=items),
        grid_spec=grid_spec,
        out_shape=[jax.ShapeDtypeStruct((rows, width), BF)] * items
        + [
            jax.ShapeDtypeStruct((items, seg_rows, hidden), BF),
            jax.ShapeDtypeStruct((e_count, hidden), F32),
        ],
        compiler_params=params(),
        cost_estimate=SHORT,
        name="experts_back",
    )(experts, offsets, slope, *left, *ups, *downs)
    return out[:items], out[items], out[items + 1]


def k_down(e_ref, off_ref, act_ref, *rest, own):
    zo_ref, zp_ref, w_down, sems = rest[-4:]
    pieces = rest[:-4]
    i = pl.program_id(0)

    @pl.when(i == 0)
    def _():
        copies = place_copies(off_ref, pieces, w_down, sems)
        run_copies(copies, start=True)
        run_copies(copies, wait=True)

    rows = zo_ref.shape[1]
    seg_a, seg_b, head = segments(rows)
    tail = seg_b[0]
    z_a = dot(act_ref[0, : seg_a[1], :], w_down[e_ref[0, i]], NT)
    z_b = dot(act_ref[0, seg_a[1] :, :], w_down[e_ref[1, i]], NT)
    image = lax.broadcasted_iota(jnp.int32, (head - tail, 1), 0) + tail < IMG
    middle = jnp.where(image, z_a[tail:], z_b[: head - tail])
    for cond, z_ref in ((i < own, zo_ref), (i >= own, zp_ref)):

        @pl.when(cond)
        def _(z_ref=z_ref):
            z_ref[0, :tail, :] = z_a[:tail].astype(BF)
            z_ref[0, tail:head, :] = middle.astype(BF)
            z_ref[0, head:, :] = z_b[head - tail :].astype(BF)


def experts_down(experts, offsets, act, pieces, rows, own):
    items, seg_rows, hidden = act.shape
    e_count = pieces[0].shape[1]
    width = sum(p.shape[0] * p.shape[2] for p in pieces)
    count = len(pieces) * pieces[0].shape[0]
    block = (1, rows, width)
    grid_spec = pltpu.PrefetchScalarGridSpec(
        num_scalar_prefetch=2,
        grid=(items,),
        in_specs=[per_item((1, seg_rows, hidden))] + [ANY] * len(pieces),
        out_specs=[
            pl.BlockSpec(block, lambda i, *_: (jnp.minimum(i, own - 1), 0, 0)),
            pl.BlockSpec(block, lambda i, *_: (jnp.maximum(i - own, 0), 0, 0)),
        ],
        scratch_shapes=[
            pltpu.VMEM((e_count, width, hidden), BF),
            pltpu.SemaphoreType.DMA((count,)),
        ],
    )
    return pl.pallas_call(
        functools.partial(k_down, own=own),
        grid_spec=grid_spec,
        out_shape=[
            jax.ShapeDtypeStruct((own, rows, width), BF),
            jax.ShapeDtypeStruct((items - own, rows, width), BF),
        ],
        compiler_params=params(),
        cost_estimate=SHORT,
        name="experts_down",
    )(experts, offsets, act, *pieces)


def k_output(e_ref, h_ref, zm_ref, zp_ref, bias_ref, o_ref):
    i = pl.program_id(0)
    rows, keep = h_ref.shape[1], o_ref.shape[1]
    image = lax.broadcasted_iota(jnp.int32, (rows, 1), 0) < IMG
    bias = jnp.where(image, bias_ref[pl.ds(e_ref[0, i], 1), :], bias_ref[pl.ds(e_ref[1, i], 1), :])
    out = h_ref[0] + ((zm_ref[0].astype(F32) + zp_ref[0].astype(F32)) + bias)
    o_ref[0] = out[:keep].astype(BF)


def finish_output(experts, h, mine, theirs, bias, keep):
    items, rows, width = h.shape
    grid_spec = pltpu.PrefetchScalarGridSpec(
        num_scalar_prefetch=1,
        grid=(items,),
        in_specs=[per_item((1, rows, width))] * 3 + [full(bias.shape)],
        out_specs=per_item((1, keep, width)),
    )
    return pl.pallas_call(
        k_output,
        grid_spec=grid_spec,
        out_shape=jax.ShapeDtypeStruct((items, keep, width), BF),
        compiler_params=params(),
        cost_estimate=SHORT,
        name="finish_output",
    )(experts, h, mine, theirs, bias)


def k_attend_back(
    len_ref, dm_ref, dp_ref, h_ref, g_ref, tok_ref, q_ref, k_ref, v_ref, w_ref, wo_ref, vec_ref,
    *rest, item, scale,
):
    dh_ref, dy_ref, dqkv_ref, da_ref, sums_ref, bias_ref = rest[-6:]
    rows, width = dh_ref.shape
    cols = q_ref.shape[3]
    db = dm_ref[...].astype(F32) + dp_ref[...].astype(F32)
    hat, spread = normed(h_ref[0])
    dh = g_ref[0].astype(F32) + norm_back(db, hat, spread, vec_ref[3:4, :])
    dh_ref[...] = dh
    dy = dh.astype(BF)
    dy_ref[...] = dy
    sums_ref[0:1, :] = jnp.sum(db * hat, axis=0, keepdims=True)
    sums_ref[1:2, :] = jnp.sum(db, axis=0, keepdims=True)
    sums_ref[2:3, :] = jnp.sum(dy.astype(F32), axis=0, keepdims=True)
    dctx = dot(dy, wo_ref[0], NN).astype(BF)
    valid = lax.broadcasted_iota(jnp.int32, (rows, 1), 0) < IMG + len_ref[item]
    low = lax.broadcasted_iota(jnp.int32, (1, LANES), 1) < HDIM
    for pair in range(cols // LANES):
        at = slice(pair * LANES, (pair + 1) * LANES)
        q, k, v = q_ref[0, 0, :, at], k_ref[0, 0, :, at], v_ref[0, 0, :, at]
        dc = dctx[:, at]
        parts = []
        for side in (low, ~low):
            only = side.astype(BF)
            s = dot(k * only, q, NT) * scale
            s = jnp.where(valid, s, -1e30)
            e = jnp.exp(s - jnp.max(s, axis=0, keepdims=True))
            p = e / jnp.sum(e, axis=0, keepdims=True)
            dp = dot(v * only, dc, NT)
            ds = (p * (dp - jnp.sum(p * dp, axis=0, keepdims=True))).astype(BF)
            parts.append((dot(ds, k, TN), dot(ds, q, NN), dot(p.astype(BF), dc, NN)))
        dqkv_ref[0, :, at] = (jnp.where(low, parts[0][0], parts[1][0]) * scale).astype(BF)
        dqkv_ref[1, :, at] = (jnp.where(low, parts[0][1], parts[1][1]) * scale).astype(BF)
        dqkv_ref[2, :, at] = jnp.where(low, parts[0][2], parts[1][2]).astype(BF)
    da = dot(dqkv_ref[0], w_ref[0], NT)
    da += dot(dqkv_ref[1], w_ref[1], NT)
    da += dot(dqkv_ref[2], w_ref[2], NT)
    bias_ref[0:1, :] = jnp.sum(dqkv_ref[0].astype(F32), axis=0, keepdims=True)
    bias_ref[1:2, :] = jnp.sum(dqkv_ref[2].astype(F32), axis=0, keepdims=True)
    hat, _ = normed(tok_ref[0].astype(F32))
    sums_ref[3:4, :] = jnp.sum(da * hat, axis=0, keepdims=True)
    sums_ref[4:5, :] = jnp.sum(da, axis=0, keepdims=True)
    da_ref[...] = da.astype(BF)
    if len(rest) > 6:
        sums_ref[...] += rest[0][...]
        bias_ref[...] += rest[1][...]


def attend_back(
    item, text_len, mine, theirs, h, g, tokens, qkv, weights, w_out, vectors, so_far, scale
):
    rows, width = h.shape[1:]
    cols = qkv.shape[3]
    item_spec = pl.BlockSpec((1, rows, width), lambda i, *_: (item, 0, 0))
    grid_spec = pltpu.PrefetchScalarGridSpec(
        num_scalar_prefetch=1,
        grid=(1,),
        in_specs=[full((rows, width))] * 2
        + [item_spec] * 3
        + [pl.BlockSpec((1, 1, rows, cols), lambda i, *_, t=t: (t, item, 0, 0)) for t in range(3)]
        + [full(weights.shape), full(w_out.shape), full(vectors.shape)]
        + [full(v.shape) for v in so_far],
        out_specs=[
            full((rows, width)),
            full((rows, width)),
            full((3, rows, cols)),
            full((rows, width)),
            full((5, width)),
            full((2, cols)),
        ],
    )
    return pl.pallas_call(
        functools.partial(k_attend_back, item=item, scale=scale),
        grid_spec=grid_spec,
        out_shape=[
            jax.ShapeDtypeStruct((rows, width), F32),
            jax.ShapeDtypeStruct((rows, width), BF),
            jax.ShapeDtypeStruct((3, rows, cols), BF),
            jax.ShapeDtypeStruct((rows, width), BF),
            jax.ShapeDtypeStruct((5, width), F32),
            jax.ShapeDtypeStruct((2, cols), F32),
        ],
        compiler_params=params(),
        cost_estimate=SHORT,
        name="attend_back",
    )(
        text_len, mine, theirs, h, g, tokens, qkv, qkv, qkv, weights, w_out, vectors, *so_far,
    )


def k_attn_grad(slot_ref, *rest, items, n_out, base):
    acc, stage, sems = rest[-3:]
    outs = rest[-3 - n_out : -3]
    a_refs, d_refs = rest[:items], rest[items : 2 * items]
    y_refs, c_refs = rest[2 * items : 3 * items], rest[3 * items : 4 * items]
    for n in range(items):
        for t in range(4):
            left, right = (a_refs[n][0], d_refs[n][t]) if t < 3 else (y_refs[n][...], c_refs[n][...])
            part = dot(left, right, TN)
            if n == 0:
                acc[t] = part
            else:
                acc[t] += part
    write_chunks(slot_ref, base, acc, stage, outs, sems)


def attn_grad(slots, base, a, dqkv, dy, ctx, chunk, n_out):
    items, rows, width = a.shape
    cols = ctx[0].shape[1]
    grid_spec = pltpu.PrefetchScalarGridSpec(
        num_scalar_prefetch=1,
        grid=(1,),
        in_specs=[
            pl.BlockSpec((1, rows, width), lambda i, *_, n=n: (n, 0, 0)) for n in range(items)
        ]
        + [full((3, rows, cols))] * items
        + [full((rows, width))] * items
        + [full((rows, cols))] * items,
        out_specs=[ANY] * n_out,
        scratch_shapes=[
            pltpu.VMEM((4, width, cols), F32),
            pltpu.VMEM((chunk[0] * n_out,) + chunk[1:], BF),
            pltpu.SemaphoreType.DMA((n_out,)),
        ],
    )
    return pl.pallas_call(
        functools.partial(k_attn_grad, items=items, n_out=n_out, base=base),
        grid_spec=grid_spec,
        out_shape=[jax.ShapeDtypeStruct(chunk, BF)] * n_out,
        compiler_params=params(),
        cost_estimate=SHORT,
        name="attn_grad",
    )(slots, *([a] * items), *dqkv, *dy, *ctx)


def k_token_grad(dh_ref, dm_ref, dp_ref, tok_ref, vec_ref, *rest):
    o_ref = rest[-1]
    keep = o_ref.shape[1]
    da = dm_ref[...].astype(F32) + dp_ref[...].astype(F32)
    hat, spread = normed(tok_ref[0].astype(F32))
    out = dh_ref[...] + norm_back(da, hat, spread, vec_ref[0:1, :])
    o_ref[0] = out[:keep]


def token_grad(item, dh, mine, theirs, tokens, vectors, keep, buffer):
    rows, width = dh.shape
    kept = [] if buffer is None else [buffer]
    return pl.pallas_call(
        k_token_grad,
        grid=(1,),
        in_specs=[full((rows, width))] * 3
        + [pl.BlockSpec((1, rows, width), lambda i: (item, 0, 0)), full(vectors.shape)]
        + [ANY] * len(kept),
        out_specs=pl.BlockSpec((1, keep, width), lambda i: (item, 0, 0)),
        out_shape=jax.ShapeDtypeStruct((tokens.shape[0], keep, width), F32),
        input_output_aliases={5: 0} if kept else {},
        compiler_params=params(),
        cost_estimate=SHORT,
        name="token_grad",
    )(dh, mine, theirs, tokens, vectors, *kept)


def swap(value, axis, size, mask):
    return lax.ppermute(value, axis, [(i, i ^ mask) for i in range(size)])


def tie(value, *others):
    return lax.optimization_barrier((value,) + others)[0]


def add_low(a, b):
    return (a.astype(F32) + b.astype(F32)).astype(BF)


def per_device(
    tokens, text_len, routes, attn_gain, attn_shift, w_qkv, b_qv, w_out, b_out, ffn_gain, ffn_shift,
    w_up, b_up, w_down, b_down, cotangent, *, dp, rep,
):
    items, seq, width = tokens.shape
    rows = up_to(seq, SUB)
    share = w_qkv.shape[1]
    cols = w_qkv.shape[2]
    hidden = w_up.shape[2] // 2
    e_count = w_up.shape[0]
    scale = 1.0 / math.sqrt(HDIM)
    me = lax.axis_index("dp")
    core = me % 2
    by_permute = dp == 16 and share % SUB == 0
    masks = [m for m in (1, 2, 4, 8, 16, 32, 64, 128) if m < dp]

    def peer(value):
        return lax.ppermute(value, "rep", [(i, i ^ 1) for i in range(rep)])

    def partner(value):
        return swap(value, "dp", dp, 1)

    def dp_swap(value, mask):
        return swap(value, "dp", dp, mask)

    def halves(w):
        mine = lax.dynamic_slice_in_dim(w, core * hidden, hidden, 2)
        other = lax.dynamic_slice_in_dim(w, (1 - core) * hidden, hidden, 2)
        return mine, other

    attn_shard = jnp.concatenate([w_qkv, w_out[None]], axis=0)
    vectors = jnp.stack([attn_gain, attn_shift, b_out, ffn_gain, ffn_shift])
    pad = ((0, 0), (0, rows - seq), (0, 0))
    tok = jnp.pad(tokens, pad)
    cot = jnp.pad(cotangent, pad)
    bias = jnp.stack([b_qv[0], jnp.zeros_like(b_qv[0]), b_qv[1]])
    experts = jnp.stack([routes[:, 0], routes[:, seq - 1]]).astype(jnp.int32)
    b_up_mine = lax.dynamic_slice_in_dim(b_up, core * hidden, hidden, 1)

    if by_permute:
        here = me.astype(jnp.int32)
        own_attn = attn_shard[None]
        za = [own_attn] + [dp_swap(own_attn, r) for r in (4, 8, 12)]
        xa = [dp_swap(p, 2) for p in za]
        attn_pieces = za + xa + [partner(p) for p in za + xa]
        rel = [0, 4, 8, 12]
        rel = rel + [r ^ 2 for r in rel]
        attn_off = (here ^ jnp.array(rel + [r ^ 1 for r in rel], jnp.int32)) * share
        rel = [r ^ j for r in rel for j in (0, 1)]
        ffn_off = (here ^ jnp.array(rel, jnp.int32)) * share
        mine, other = halves(w_up)
        up_own = jnp.stack([mine, partner(other)])
        mine, other = halves(w_down)
        down_own = jnp.stack([mine, partner(other)])
        ids = jnp.arange(dp, dtype=jnp.int32) ^ here
        slots = (ids & 1) * (dp // 2) + (ids & 2) // 2 * (dp // 4) + ids // 4
        n_out = 4
        ffn_chunk, attn_chunk = (dp // 4, e_count, share, hidden), (dp // 4, 4, share, cols)

        up_own = tie(up_own, *za)
        z1u, z2u = dp_swap(up_own, 4), dp_swap(up_own, 8)
        x0u = dp_swap(tie(up_own, *xa), 2)
    else:
        attn_pieces = [lax.all_gather(attn_shard, "dp", axis=1, tiled=True)[None]]
        gathered = lax.all_gather(w_up, "dp", axis=1, tiled=True)
        up_pieces = [halves(gathered)[0][None]]
        gathered = lax.all_gather(w_down, "dp", axis=1, tiled=True)
        down_pieces = [halves(gathered)[0][None]]
        attn_off = ffn_off = slots = jnp.zeros((1,), jnp.int32)
        n_out = 1
        ffn_chunk, attn_chunk = (1, e_count, width, hidden), (1, 4, width, cols)

    a, qkv, attn_w, out_w = project(tok, vectors, bias, attn_pieces, attn_off)
    out_theirs = peer(out_w)
    ctx, ctx_theirs = [], []
    lens = tie(text_len, out_w)
    if by_permute:
        lens = tie(text_len, out_w, z1u, x0u)
        x1u = dp_swap(tie(z1u, out_w, x0u), 2)
    for n in range(items):
        c = attend(n, lens, qkv, scale)
        ctx.append(c)
        ctx_theirs.append(peer(c))
        lens = tie(text_len, c)
        if by_permute and n == 0:
            z3u = dp_swap(tie(up_own, z2u, c), 12)
            lens = tie(text_len, c, z2u)
        if by_permute and n == 1:
            lens = tie(text_len, c, x1u)
            x2u = dp_swap(tie(z2u, x1u, c), 2)
    cot_partner = partner(tie(cot, c))
    cots = [cot, cot_partner]
    experts_partner = partner(tie(experts, c))
    experts_two = jnp.concatenate([experts, experts_partner], axis=1)
    b, b_partner = [], []
    h, vec = None, tie(vectors, *ctx)
    for n in range(items):
        h, b_n = residual(n, tok, ctx[n], ctx_theirs[n], out_w, out_theirs, vec, h)
        b.append(b_n)
        b_partner.append(partner(b_n))
        vec = tie(vectors, h)
        if by_permute and n == 0:
            vec = tie(vectors, h, x2u)
            x0d = dp_swap(tie(down_own, x2u, h), 2)
        if by_permute and n == 1:
            vec = tie(vectors, h, z3u)
            x3u = dp_swap(tie(z3u, h), 2)
            down_own = tie(down_own, z3u, h)
            z1d, z2d = dp_swap(down_own, 4), dp_swap(down_own, 8)
    b_two = b + b_partner
    up_ready = [h]
    if by_permute:
        up_pieces = [up_own, z1u, z2u, z3u, x0u, x1u, x2u, x3u]
        up_ready = [h, x0d]

    act, slope = experts_up(tie(experts_two, *up_ready), ffn_off, b_two, b_up_mine, up_pieces)
    up_ready = [act]
    if by_permute:
        x1d = dp_swap(tie(z1d, act), 2)
        z3d = dp_swap(tie(down_own, z2d, act), 12)
        x2d = dp_swap(tie(z2d, act), 2)
        up_ready = [act, z2d]
    *down_grad, grad_b_down = weight_grad(
        tie(experts_two, *up_ready), slots, 0, cots, act, ffn_chunk, n_out, e_count, items
    )
    experts_late = tie(experts_two, grad_b_down)
    if by_permute:
        x3d = dp_swap(tie(z3d, x1d, grad_b_down), 2)
        down_pieces = [down_own, z1d, z2d, z3d, x0d, x1d, x2d, x3d]

        def near(parts, core_slot, *others):
            return dp_swap(tie(parts[2 * core_slot + 1], *others), 2)

        def middle(parts, core_slot, got, *others):
            keep, got = tie(parts[2 * core_slot], got, *others), tie(got, *others)
            both = keep[2:4].astype(F32) + got[2:4].astype(F32)
            return keep, got, dp_swap(both.astype(BF), 8)

        def last(state, *others):
            keep, got, mid = state
            mid = tie(mid, *others)
            part = keep[1].astype(F32) + got[1].astype(F32) + mid[1].astype(F32)
            return keep, got, mid, dp_swap(part.astype(BF), 4)

        def total(state):
            keep, got, mid, end = state
            return (
                keep[0].astype(F32)
                + got[0].astype(F32)
                + mid[0].astype(F32)
                + end.astype(F32)
            )

        dn1 = near(down_grad, 1, x3d)
        experts_late = tie(experts_two, x3d, grad_b_down)
    db_two, du, grad_b_up = experts_back(
        experts_late, ffn_off, cots, slope, up_pieces, down_pieces
    )
    db = [add_low(db_two[n], partner(db_two[items + n])) for n in range(items)]
    db_theirs = [peer(v) for v in db]
    experts_late = tie(experts_two, *db)
    if by_permute:
        dm1 = middle(down_grad, 1, dn1, *db)
        dn0 = near(down_grad, 0, *db, dn1)
        experts_late = tie(experts_two, dn1, *db)
    *up_grad, _ = weight_grad(
        experts_late, slots, 0, b_two, du, ffn_chunk, n_out, e_count, 0
    )

    dh, dy, dqkv, da, da_theirs, so_far = [], [], [], [], [], []
    lens = tie(text_len, up_grad[0])
    for n in range(items):
        dh_n, dy_n, dqkv_n, da_n, *so_far = attend_back(
            n, lens, db[n], db_theirs[n], h, cot, tok, qkv, attn_w, out_w, vectors, so_far, scale
        )
        dh.append(dh_n)
        dy.append(dy_n)
        dqkv.append(dqkv_n)
        da.append(da_n)
        da_theirs.append(peer(da_n))
        seen = so_far[1]
        waits = [seen] + da_theirs[:n]
        if by_permute and n == 0:
            waits = waits + [dm1[2], dn0]
            de1 = last(dm1, seen)
            dm0 = middle(down_grad, 0, dn0, seen)
            un1 = near(up_grad, 1, seen, dn0)
        if by_permute and n == 1:
            waits = waits + [de1[3]]
        if by_permute and n == 2:
            waits = waits + [dm0[2], un1]
            de0 = last(dm0, seen)
            um1 = middle(up_grad, 1, un1, seen)
            un0 = near(up_grad, 0, seen, un1)
        lens = tie(text_len, *waits)
    sums, bias_sums = so_far
    attn_parts = attn_grad(tie(slots, *waits), 0, a, dqkv, dy, ctx, attn_chunk, n_out)

    first_norm = sums[3:5]
    first_norm_theirs = peer(first_norm)
    waits = [attn_parts[0], da_theirs[-1], first_norm_theirs]
    up_pair = jnp.zeros((2, e_count, hidden), F32)
    up_pair = lax.dynamic_update_slice_in_dim(up_pair, grad_b_up[None], core, 0)
    small = jnp.concatenate(
        [
            (first_norm + first_norm_theirs).reshape(-1),
            sums[0:3].reshape(-1),
            grad_b_down.reshape(-1),
            up_pair.reshape(-1),
            bias_sums.reshape(-1),
        ]
    ).reshape(-1, LANES)
    steps = list(masks)

    def add_step(*others):
        nonlocal small
        small = tie(small, *others)
        got = swap(small, "dp", dp, steps.pop(0))
        small = small + got
        return got

    got = add_step(attn_parts[0])
    if by_permute:
        send = add_low(attn_parts[1], partner(attn_parts[3]))
        keep = add_low(attn_parts[0], partner(attn_parts[2]))
        an = near([keep, send], 0)
        waits = waits + [de0[3]]
    z_own, z_other = experts_down(
        tie(experts_two, *waits), ffn_off, act, down_pieces, rows, items
    )
    z = add_low(z_own, partner(z_other))
    z_theirs = peer(z)
    waits = [z, got]
    if by_permute:
        ue1 = last(um1, z)
        um0 = middle(up_grad, 0, un0, z)
        down_other = total(tie(de1, z))
        down_got = partner(down_other)
        down_mine = total(tie(de0, z))
        waits = waits + [um1[2], un0]
    grad_tokens = None
    got = add_step(z)
    for n in range(items):
        vec = tie(vectors, *waits)
        grad_tokens = token_grad(
            n, dh[n], da[n], da_theirs[n], tok, vec, seq, grad_tokens
        )
        waits = [grad_tokens, got]
        if n < items - 1:
            got = add_step(grad_tokens)
    if by_permute:
        am = middle([keep, send], 0, an, grad_tokens)
        up_other = total(tie(ue1, grad_tokens))
        up_got = partner(up_other)
        waits = waits + [an, up_other, down_got]
    output = finish_output(tie(experts, *waits), h, z, z_theirs, b_down, seq)

    if by_permute:

        def joined(own, got):
            first = core == 0
            return jnp.concatenate(
                [jnp.where(first, own, got), jnp.where(first, got, own)], axis=-1
            )

        grad_w_down = joined(down_mine, down_got)
        ae = last(am, output)
        ue0 = last(um0, output)
        grad_attn = total(ae)
        grad_w_up = joined(total(ue0), up_got)
        grad_w_qkv, grad_w_out = grad_attn[:3], grad_attn[3]
    else:

        def finish(chunk):
            whole = jnp.zeros((e_count, width, 2 * hidden), BF)
            whole = lax.dynamic_update_slice_in_dim(whole, chunk[0], core * hidden, 2)
            return lax.psum_scatter(whole, "dp", scatter_dimension=1, tiled=True).astype(F32)

        grad_w_down, grad_w_up = finish(down_grad[0]), finish(up_grad[0])
        grad_attn = lax.psum_scatter(attn_parts[0][0], "dp", scatter_dimension=1, tiled=True)
        grad_w_qkv, grad_w_out = grad_attn[:3].astype(F32), grad_attn[3].astype(F32)

    while steps:
        add_step()
    small = small.reshape(-1)
    at = 0

    def take(*shape):
        nonlocal at
        n = math.prod(shape)
        piece = small[at : at + n].reshape(shape)
        at += n
        return piece

    norm_one, norm_two, grad_b_out = take(2, width), take(2, width), take(width)
    total_down = take(e_count, width)
    total_up = jnp.moveaxis(take(2, e_count, hidden), 0, 1).reshape(e_count, 2 * hidden)
    total_qv = take(2, cols)
    return (
        output,
        grad_tokens,
        grad_w_qkv,
        grad_w_out,
        grad_w_up,
        grad_w_down,
        total_qv,
        grad_b_out,
        total_up,
        total_down,
        jnp.concatenate([norm_one, norm_two], axis=0),
    )


def solution(mesh):
    body = functools.partial(per_device, dp=mesh.shape["dp"], rep=mesh.shape["rep"])
    return jax.shard_map(
        body,
        mesh=mesh,
        in_specs=(
            P("dp", None, None),
            P("dp"),
            P("dp", None),
            P(),
            P(),
            P(None, "dp", "rep"),
            P(None, "rep"),
            P("dp", "rep"),
            P(),
            P(),
            P(),
            P(None, "dp", "rep"),
            P(None, "rep"),
            P(None, "dp", "rep"),
            P(),
            P("dp", None, None),
        ),
        out_specs=(
            P("dp", None, None),
            P("dp", None, None),
            P(None, "dp", "rep"),
            P("dp", "rep"),
            P(None, "dp", "rep"),
            P(None, "dp", "rep"),
            P(None, "rep"),
            P(),
            P(None, "rep"),
            P(),
            P(),
        ),
        check_vma=False,
    )
```

```python
import functools
import math

import jax
import jax.numpy as jnp
from jax import lax
from jax.experimental import pallas as pl
from jax.experimental.pallas import tpu as pltpu
from jax.sharding import PartitionSpec as P

HDIM = 64
IMG = 197
EPSILON = 1e-05
ROOT_HALF = 0.7071067811865476
INV_ROOT_TAU = 0.3989422804014327
SUB = 16
LANES = 128
BF = jnp.bfloat16
F32 = jnp.float32

NN = (((1,), (0,)), ((), ()))
NT = (((1,), (1,)), ((), ()))
TN = (((0,), (0,)), ((), ()))


def up_to(n, m):
    return -(-n // m) * m


def dot(a, b, dims):
    return lax.dot_general(a, b, dims, preferred_element_type=F32)


def full(shape):
    zeros = (0,) * len(shape)
    return pl.BlockSpec(shape, lambda *_: zeros)


def per_item(shape):
    zeros = (0,) * (len(shape) - 1)
    return pl.BlockSpec(shape, lambda i, *_: (i,) + zeros)


ANY = pl.BlockSpec(memory_space=pl.ANY)


def params():
    return pltpu.CompilerParams(vmem_limit_bytes=60 * 1024 * 1024)


SHORT = pl.CostEstimate(flops=1, transcendentals=0, bytes_accessed=1)


def normed(v):
    centred = v - jnp.mean(v, axis=-1, keepdims=True)
    var = jnp.mean(centred * centred, axis=-1, keepdims=True)
    spread = lax.rsqrt(var + EPSILON)
    return centred * spread, spread


def norm_back(grad, hat, spread, gain):
    scaled = grad * gain
    return spread * (
        scaled
        - jnp.mean(scaled, axis=-1, keepdims=True)
        - hat * jnp.mean(scaled * hat, axis=-1, keepdims=True)
    )


def run_copies(copies, *, start=False, wait=False):
    for c in copies:
        if start:
            c.start()
        if wait:
            c.wait()


def place_copies(off_ref, pieces, dest, sems, plane=0):
    copies = []
    for n, piece in enumerate(pieces):
        subs, _, rows, _ = piece.shape
        for j in range(subs):
            at = off_ref[n * subs + j]
            copies.append(
                pltpu.make_async_copy(
                    piece.at[j, plane : plane + dest.shape[0]],
                    dest.at[:, pl.ds(pl.multiple_of(at, SUB), rows), :],
                    sems.at[n * subs + j],
                )
            )
    return copies


def k_proj(off_ref, tok_ref, vec_ref, bias_ref, *rest):
    a_ref, qkv_ref, w_ref, wo_ref, sems, out_sems = rest[-6:]
    pieces = rest[:-6]
    first = pl.program_id(0) == 0

    @pl.when(first)
    def _():
        run_copies(place_copies(off_ref, pieces, w_ref, sems), start=True)
        run_copies(place_copies(off_ref, pieces, wo_ref, out_sems, 3), start=True)

    hat, _ = normed(tok_ref[0].astype(F32))
    a_ref[0] = (hat * vec_ref[0:1, :] + vec_ref[1:2, :]).astype(BF)

    @pl.when(first)
    def _():
        run_copies(place_copies(off_ref, pieces, w_ref, sems), wait=True)
        run_copies(place_copies(off_ref, pieces, wo_ref, out_sems, 3), wait=True)

    a = a_ref[0]
    for t in range(3):
        qkv_ref[t, 0] = (dot(a, w_ref[t], NN) + bias_ref[t : t + 1, :]).astype(BF)


def project(tokens, vectors, bias, pieces, offsets):
    items, rows, width = tokens.shape
    cols = pieces[0].shape[3]
    count = len(pieces) * pieces[0].shape[0]
    grid_spec = pltpu.PrefetchScalarGridSpec(
        num_scalar_prefetch=1,
        grid=(items,),
        in_specs=[
            per_item((1, rows, width)),
            full(vectors.shape),
            full((3, cols)),
        ]
        + [ANY] * len(pieces),
        out_specs=[
            per_item((1, rows, width)),
            pl.BlockSpec((3, 1, rows, cols), lambda i, *_: (0, i, 0, 0)),
            full((3, width, cols)),
            full((1, width, cols)),
        ],
        scratch_shapes=[pltpu.SemaphoreType.DMA((count,)), pltpu.SemaphoreType.DMA((count,))],
    )
    return pl.pallas_call(
        k_proj,
        grid_spec=grid_spec,
        out_shape=[
            jax.ShapeDtypeStruct((items, rows, width), BF),
            jax.ShapeDtypeStruct((3, items, rows, cols), BF),
            jax.ShapeDtypeStruct((3, width, cols), BF),
            jax.ShapeDtypeStruct((1, width, cols), BF),
        ],
        compiler_params=params(),
        cost_estimate=SHORT,
        name="project",
    )(offsets, tokens, vectors, bias, *pieces)


def k_attend(len_ref, q_ref, k_ref, v_ref, c_ref, *, scale):
    rows, width = c_ref.shape[1:]
    length = len_ref[pl.program_id(0)]
    valid = lax.broadcasted_iota(jnp.int32, (1, rows), 1) < IMG + length
    low = lax.broadcasted_iota(jnp.int32, (1, LANES), 1) < HDIM
    for pair in range(width // LANES):
        cols = slice(pair * LANES, (pair + 1) * LANES)
        q, k, v = q_ref[0, 0, :, cols], k_ref[0, 0, :, cols], v_ref[0, 0, :, cols]
        both = []
        for side in (low, ~low):
            s = dot(q * side.astype(BF), k, NT) * scale
            s = jnp.where(valid, s, -1e30)
            e = jnp.exp(s - jnp.max(s, axis=-1, keepdims=True))
            p = (e / jnp.sum(e, axis=-1, keepdims=True)).astype(BF)
            both.append(dot(p, v, NN))
        c_ref[0, :, cols] = jnp.where(low, both[0], both[1]).astype(BF)


def qkv_specs(rows, cols):
    return [pl.BlockSpec((1, 1, rows, cols), lambda i, *_, t=t: (t, i, 0, 0)) for t in range(3)]


def attend(text_len, qkv, scale):
    _, items, rows, cols = qkv.shape
    grid_spec = pltpu.PrefetchScalarGridSpec(
        num_scalar_prefetch=1,
        grid=(items,),
        in_specs=qkv_specs(rows, cols),
        out_specs=per_item((1, rows, cols)),
    )
    return pl.pallas_call(
        functools.partial(k_attend, scale=scale),
        grid_spec=grid_spec,
        out_shape=jax.ShapeDtypeStruct((items, rows, cols), BF),
        compiler_params=params(),
        cost_estimate=SHORT,
        name="attend",
    )(text_len, qkv, qkv, qkv)


def k_residual(tok_ref, cm_ref, cp_ref, wm_ref, wp_ref, vec_ref, h_ref, b_ref):
    y = dot(cm_ref[0], wm_ref[0], NT) + dot(cp_ref[0], wp_ref[0], NT)
    h = tok_ref[0].astype(F32) + (y + vec_ref[2:3, :])
    h_ref[0] = h
    hat, _ = normed(h)
    b_ref[0] = (hat * vec_ref[3:4, :] + vec_ref[4:5, :]).astype(BF)


def residual(tokens, mine, theirs, w_mine, w_theirs, vectors):
    items, rows, width = tokens.shape
    cols = mine.shape[2]
    return pl.pallas_call(
        k_residual,
        grid=(items,),
        in_specs=[
            per_item((1, rows, width)),
            per_item((1, rows, cols)),
            per_item((1, rows, cols)),
            full((1, width, cols)),
            full((1, width, cols)),
            full(vectors.shape),
        ],
        out_specs=[per_item((1, rows, width))] * 2,
        out_shape=[
            jax.ShapeDtypeStruct(tokens.shape, F32),
            jax.ShapeDtypeStruct(tokens.shape, BF),
        ],
        compiler_params=params(),
        cost_estimate=SHORT,
        name="residual",
    )(tokens, mine, theirs, w_mine, w_theirs, vectors)


def segments(rows):
    head = up_to(IMG, SUB)
    tail = IMG // SUB * SUB
    return (0, head), (tail, rows - tail), head


def segment_masks(rows):
    (a0, an), (b0, bn), _ = segments(rows)
    in_a = lax.broadcasted_iota(jnp.int32, (an, 1), 0) + a0 < IMG
    in_b = lax.broadcasted_iota(jnp.int32, (bn, 1), 0) + b0 >= IMG
    return in_a, in_b


def masked_parts(g_ref, i):
    rows = g_ref.shape[1]
    (a0, an), (b0, bn), _ = segments(rows)
    in_a, in_b = segment_masks(rows)
    g_a = jnp.where(in_a, g_ref[i, a0 : a0 + an, :].astype(F32), 0.0)
    g_b = jnp.where(in_b, g_ref[i, b0 : b0 + bn, :].astype(F32), 0.0)
    return g_a, g_b


def item_copies(refs, dest, sems):
    copies = []
    for ref in refs:
        if len(ref.shape) == 2:
            copies.append(
                pltpu.make_async_copy(ref, dest.at[len(copies)], sems.at[len(copies)])
            )
        else:
            for j in range(ref.shape[0]):
                copies.append(
                    pltpu.make_async_copy(ref.at[j], dest.at[len(copies)], sems.at[len(copies)])
                )
    return copies


def wait_item(copies, i):
    for n, c in enumerate(copies):

        @pl.when(i == n)
        def _(c=c):
            c.wait()


def write_chunks(slot_ref, base, acc, stage, outs, sems):
    count, _, rows, _ = stage.shape
    for c in range(count):
        stage[slot_ref[base + c]] = acc[:, c * rows : (c + 1) * rows, :].astype(BF)
    per = count // len(outs)
    copies = [
        pltpu.make_async_copy(stage.at[n * per : (n + 1) * per], out, sems.at[n])
        for n, out in enumerate(outs)
    ]
    run_copies(copies, start=True)
    run_copies(copies, wait=True)


def k_up(e_ref, off_ref, bias_ref, *rest, n_left):
    b_refs, pieces = rest[:n_left], rest[n_left:-6]
    act_ref, slope_ref, b_s, w_s, b_sem, w_sem = rest[-6:]
    i = pl.program_id(0)
    b_copies = item_copies(b_refs, b_s, b_sem)

    @pl.when(i == 0)
    def _():
        run_copies(b_copies[:1], start=True)
        w_copies = place_copies(off_ref, pieces, w_s, w_sem)
        run_copies(w_copies, start=True)
        run_copies(b_copies[1:], start=True)
        run_copies(w_copies, wait=True)

    wait_item(b_copies, i)
    seg_a, seg_b, _ = segments(b_s.shape[1])
    at = 0
    for which, (lo, n) in zip((0, 1), (seg_a, seg_b)):
        e = e_ref[which, i]
        u = dot(b_s[i, lo : lo + n, :], w_s[e], NN) + bias_ref[pl.ds(e, 1), :]
        cdf = 0.5 * (1.0 + lax.erf(u * ROOT_HALF))
        act_ref[0, at : at + n, :] = (u * cdf).astype(BF)
        slope_ref[0, at : at + n, :] = (cdf + u * jnp.exp(-0.5 * u * u) * INV_ROOT_TAU).astype(BF)
        at += n


def experts_up(experts, offsets, b, bias, pieces):
    items = experts.shape[1]
    rows, width = b[0].shape[-2:]
    e_count, _, hidden = pieces[0].shape[1:]
    count = len(pieces) * pieces[0].shape[0]
    (_, an), (_, bn), _ = segments(rows)
    grid_spec = pltpu.PrefetchScalarGridSpec(
        num_scalar_prefetch=2,
        grid=(items,),
        in_specs=[full((e_count, hidden))] + [ANY] * (len(b) + len(pieces)),
        out_specs=[per_item((1, an + bn, hidden))] * 2,
        scratch_shapes=[
            pltpu.VMEM((items, rows, width), BF),
            pltpu.VMEM((e_count, width, hidden), BF),
            pltpu.SemaphoreType.DMA((items,)),
            pltpu.SemaphoreType.DMA((count,)),
        ],
    )
    return pl.pallas_call(
        functools.partial(k_up, n_left=len(b)),
        grid_spec=grid_spec,
        out_shape=[jax.ShapeDtypeStruct((items, an + bn, hidden), BF)] * 2,
        compiler_params=params(),
        cost_estimate=SHORT,
        name="experts_up",
    )(experts, offsets, bias, *b, *pieces)


def k_weight_grad(e_ref, slot_ref, right_ref, *rest, n_left, n_out, base, own):
    lefts = rest[:n_left]
    outs = rest[n_left : n_left + n_out]
    left_s, dw_s, stage, left_sem, out_sem = rest[-5:]
    sums_ref = rest[n_left + n_out]
    i = pl.program_id(0)
    copies = item_copies(lefts, left_s, left_sem)

    @pl.when(i == 0)
    def _():
        run_copies(copies, start=True)
        dw_s[...] = jnp.zeros_like(dw_s)
        sums_ref[...] = jnp.zeros_like(sums_ref)

    wait_item(copies, i)
    at = 0
    for which, left in zip((0, 1), masked_parts(left_s, i)):
        e = e_ref[which, i]
        n = left.shape[0]
        dw_s[e] += dot(left.astype(BF), right_ref[0, at : at + n, :], TN)

        @pl.when(i < own)
        def _(left=left, e=e):
            sums_ref[pl.ds(e, 1), :] += jnp.sum(left, axis=0, keepdims=True)

        at += n

    @pl.when(i == pl.num_programs(0) - 1)
    def _():
        write_chunks(slot_ref, base, dw_s, stage, outs, out_sem)


def weight_grad(experts, slots, base, left, right, chunk, n_out, e_count, own):
    items, seg_rows, hidden = right.shape
    rows, width = left[0].shape[-2:]
    count = chunk[0] * n_out
    grid_spec = pltpu.PrefetchScalarGridSpec(
        num_scalar_prefetch=2,
        grid=(items,),
        in_specs=[per_item((1, seg_rows, hidden))] + [ANY] * len(left),
        out_specs=[ANY] * n_out + [full((e_count, width))],
        scratch_shapes=[
            pltpu.VMEM((items, rows, width), BF),
            pltpu.VMEM((e_count, width, hidden), F32),
            pltpu.VMEM((count,) + chunk[1:], BF),
            pltpu.SemaphoreType.DMA((items,)),
            pltpu.SemaphoreType.DMA((n_out,)),
        ],
    )
    return pl.pallas_call(
        functools.partial(
            k_weight_grad, n_left=len(left), n_out=n_out, base=base, own=own
        ),
        grid_spec=grid_spec,
        out_shape=[jax.ShapeDtypeStruct(chunk, BF)] * n_out
        + [jax.ShapeDtypeStruct((e_count, width), F32)],
        compiler_params=params(),
        cost_estimate=SHORT,
        name="weight_grad",
    )(experts, slots, right, *left)


def store_joined(ref, first, middle, second, tail, head):
    ref[0, :tail, :] = first[:tail].astype(BF)
    ref[0, tail:head, :] = middle.astype(BF)
    ref[0, head:, :] = second[head - tail :].astype(BF)


def k_back(e_ref, off_ref, slope_ref, *rest, n_left, n_up, own):
    g_s, w_up, w_down, sem_g, sem_up, sem_down = rest[-6:]
    do_ref, dp_ref, du_ref, gbu_ref = rest[-10:-6]
    lefts, ups, downs = rest[:n_left], rest[n_left : n_left + n_up], rest[n_left + n_up : -10]
    i = pl.program_id(0)
    copies = item_copies(lefts, g_s, sem_g)

    @pl.when(i == 0)
    def _():
        w_copies = place_copies(off_ref, downs, w_down, sem_down)
        run_copies(copies[:1] + w_copies, start=True)
        more = place_copies(off_ref, ups, w_up, sem_up)
        run_copies(more + copies[1:], start=True)
        gbu_ref[...] = jnp.zeros_like(gbu_ref)
        run_copies(w_copies + more, wait=True)

    wait_item(copies, i)
    rows = g_s.shape[1]
    seg_a, seg_b, head = segments(rows)
    tail = seg_b[0]
    at = 0
    both = []
    for which, g in zip((0, 1), masked_parts(g_s, i)):
        e = e_ref[which, i]
        n = g.shape[0]
        dact = dot(g.astype(BF), w_down[e], NN)
        du = (dact * slope_ref[0, at : at + n, :].astype(F32)).astype(BF)
        du_ref[0, at : at + n, :] = du
        gbu_ref[pl.ds(e, 1), :] += jnp.sum(du.astype(F32), axis=0, keepdims=True)
        both.append(dot(du, w_up[e], NT))
        at += n
    middle = both[0][tail:] + both[1][: head - tail]
    for cond, db_ref in ((i < own, do_ref), (i >= own, dp_ref)):

        @pl.when(cond)
        def _(db_ref=db_ref):
            store_joined(db_ref, both[0], middle, both[1], tail, head)


def own_and_other(rows, width, own):
    block = (1, rows, width)
    return [
        pl.BlockSpec(block, lambda i, *_: (jnp.minimum(i, own - 1), 0, 0)),
        pl.BlockSpec(block, lambda i, *_: (jnp.maximum(i - own, 0), 0, 0)),
    ]


def experts_back(experts, offsets, left, slope, ups, downs, own):
    rows, width = left[0].shape[-2:]
    e_count, _, hidden = ups[0].shape[1:]
    count = len(ups) * ups[0].shape[0]
    items, seg_rows, _ = slope.shape
    grid_spec = pltpu.PrefetchScalarGridSpec(
        num_scalar_prefetch=2,
        grid=(items,),
        in_specs=[per_item((1, seg_rows, hidden))]
        + [ANY] * (len(left) + len(ups) + len(downs)),
        out_specs=own_and_other(rows, width, own)
        + [per_item((1, seg_rows, hidden)), full((e_count, hidden))],
        scratch_shapes=[
            pltpu.VMEM((items, rows, width), BF),
            pltpu.VMEM((e_count, width, hidden), BF),
            pltpu.VMEM((e_count, width, hidden), BF),
            pltpu.SemaphoreType.DMA((items,)),
            pltpu.SemaphoreType.DMA((count,)),
            pltpu.SemaphoreType.DMA((count,)),
        ],
    )
    return pl.pallas_call(
        functools.partial(k_back, n_left=len(left), n_up=len(ups), own=own),
        grid_spec=grid_spec,
        out_shape=[
            jax.ShapeDtypeStruct((own, rows, width), BF),
            jax.ShapeDtypeStruct((items - own, rows, width), BF),
            jax.ShapeDtypeStruct((items, seg_rows, hidden), BF),
            jax.ShapeDtypeStruct((e_count, hidden), F32),
        ],
        compiler_params=params(),
        cost_estimate=SHORT,
        name="experts_back",
    )(experts, offsets, slope, *left, *ups, *downs)


def k_down(e_ref, off_ref, act_ref, *rest, own):
    zo_ref, zp_ref, w_down, sems = rest[-4:]
    pieces = rest[:-4]
    i = pl.program_id(0)

    @pl.when(i == 0)
    def _():
        copies = place_copies(off_ref, pieces, w_down, sems)
        run_copies(copies, start=True)
        run_copies(copies, wait=True)

    rows = zo_ref.shape[1]
    seg_a, seg_b, head = segments(rows)
    tail = seg_b[0]
    z_a = dot(act_ref[0, : seg_a[1], :], w_down[e_ref[0, i]], NT)
    z_b = dot(act_ref[0, seg_a[1] :, :], w_down[e_ref[1, i]], NT)
    image = lax.broadcasted_iota(jnp.int32, (head - tail, 1), 0) + tail < IMG
    middle = jnp.where(image, z_a[tail:], z_b[: head - tail])
    for cond, z_ref in ((i < own, zo_ref), (i >= own, zp_ref)):

        @pl.when(cond)
        def _(z_ref=z_ref):
            store_joined(z_ref, z_a, middle, z_b, tail, head)


def experts_down(experts, offsets, act, pieces, rows, own):
    items, seg_rows, hidden = act.shape
    e_count = pieces[0].shape[1]
    width = sum(p.shape[0] * p.shape[2] for p in pieces)
    count = len(pieces) * pieces[0].shape[0]
    grid_spec = pltpu.PrefetchScalarGridSpec(
        num_scalar_prefetch=2,
        grid=(items,),
        in_specs=[per_item((1, seg_rows, hidden))] + [ANY] * len(pieces),
        out_specs=own_and_other(rows, width, own),
        scratch_shapes=[
            pltpu.VMEM((e_count, width, hidden), BF),
            pltpu.SemaphoreType.DMA((count,)),
        ],
    )
    return pl.pallas_call(
        functools.partial(k_down, own=own),
        grid_spec=grid_spec,
        out_shape=[
            jax.ShapeDtypeStruct((own, rows, width), BF),
            jax.ShapeDtypeStruct((items - own, rows, width), BF),
        ],
        compiler_params=params(),
        cost_estimate=SHORT,
        name="experts_down",
    )(experts, offsets, act, *pieces)


def k_output(e_ref, h_ref, zm_ref, zp_ref, bias_ref, o_ref):
    i = pl.program_id(0)
    rows, keep = h_ref.shape[1], o_ref.shape[1]
    image = lax.broadcasted_iota(jnp.int32, (rows, 1), 0) < IMG
    bias = jnp.where(image, bias_ref[pl.ds(e_ref[0, i], 1), :], bias_ref[pl.ds(e_ref[1, i], 1), :])
    out = h_ref[0] + ((zm_ref[0].astype(F32) + zp_ref[0].astype(F32)) + bias)
    o_ref[0] = out[:keep].astype(BF)


def finish_output(experts, h, mine, theirs, bias, keep):
    items, rows, width = h.shape
    grid_spec = pltpu.PrefetchScalarGridSpec(
        num_scalar_prefetch=1,
        grid=(items,),
        in_specs=[per_item((1, rows, width))] * 3 + [full(bias.shape)],
        out_specs=per_item((1, keep, width)),
    )
    return pl.pallas_call(
        k_output,
        grid_spec=grid_spec,
        out_shape=jax.ShapeDtypeStruct((items, keep, width), BF),
        compiler_params=params(),
        cost_estimate=SHORT,
        name="finish_output",
    )(experts, h, mine, theirs, bias)


def k_attend_back(
    len_ref, dm_ref, dp_ref, h_ref, g_ref, tok_ref, q_ref, k_ref, v_ref, w_ref, wo_ref, vec_ref,
    dh_ref, dy_ref, dqkv_ref, da_ref, sums_ref, bias_ref, *, scale,
):
    rows, width = dh_ref.shape[1:]
    cols = q_ref.shape[3]
    i = pl.program_id(0)

    @pl.when(i == 0)
    def _():
        sums_ref[...] = jnp.zeros_like(sums_ref)
        bias_ref[...] = jnp.zeros_like(bias_ref)

    def add_rows(ref, at, value):
        ref[at : at + 1, :] += jnp.sum(value, axis=0, keepdims=True)

    db = dm_ref[0].astype(F32) + dp_ref[0].astype(F32)
    hat, spread = normed(h_ref[0])
    dh = g_ref[0].astype(F32) + norm_back(db, hat, spread, vec_ref[3:4, :])
    dh_ref[0] = dh
    dy = dh.astype(BF)
    dy_ref[0] = dy
    add_rows(sums_ref, 0, db * hat)
    add_rows(sums_ref, 1, db)
    add_rows(sums_ref, 2, dy.astype(F32))
    dctx = dot(dy, wo_ref[0], NN).astype(BF)
    valid = lax.broadcasted_iota(jnp.int32, (rows, 1), 0) < IMG + len_ref[i]
    low = lax.broadcasted_iota(jnp.int32, (1, LANES), 1) < HDIM
    for pair in range(cols // LANES):
        at = slice(pair * LANES, (pair + 1) * LANES)
        q, k, v = q_ref[0, 0, :, at], k_ref[0, 0, :, at], v_ref[0, 0, :, at]
        dc = dctx[:, at]
        parts = []
        for side in (low, ~low):
            only = side.astype(BF)
            s = dot(k * only, q, NT) * scale
            s = jnp.where(valid, s, -1e30)
            e = jnp.exp(s - jnp.max(s, axis=0, keepdims=True))
            p = e / jnp.sum(e, axis=0, keepdims=True)
            dp = dot(v * only, dc, NT)
            ds = (p * (dp - jnp.sum(p * dp, axis=0, keepdims=True))).astype(BF)
            parts.append((dot(ds, k, TN), dot(ds, q, NN), dot(p.astype(BF), dc, NN)))
        dqkv_ref[0, 0, :, at] = (jnp.where(low, parts[0][0], parts[1][0]) * scale).astype(BF)
        dqkv_ref[0, 1, :, at] = (jnp.where(low, parts[0][1], parts[1][1]) * scale).astype(BF)
        dqkv_ref[0, 2, :, at] = jnp.where(low, parts[0][2], parts[1][2]).astype(BF)
    da = dot(dqkv_ref[0, 0], w_ref[0], NT)
    da += dot(dqkv_ref[0, 1], w_ref[1], NT)
    da += dot(dqkv_ref[0, 2], w_ref[2], NT)
    add_rows(bias_ref, 0, dqkv_ref[0, 0].astype(F32))
    add_rows(bias_ref, 1, dqkv_ref[0, 2].astype(F32))
    hat, _ = normed(tok_ref[0].astype(F32))
    add_rows(sums_ref, 3, da * hat)
    add_rows(sums_ref, 4, da)
    da_ref[0] = da.astype(BF)


def attend_back(text_len, mine, theirs, h, g, tokens, qkv, weights, w_out, vectors, scale):
    items, rows, width = h.shape
    cols = qkv.shape[3]
    block = per_item((1, rows, width))
    grid_spec = pltpu.PrefetchScalarGridSpec(
        num_scalar_prefetch=1,
        grid=(items,),
        in_specs=[block] * 5
        + qkv_specs(rows, cols)
        + [full(weights.shape), full(w_out.shape), full(vectors.shape)],
        out_specs=[
            block,
            block,
            per_item((1, 3, rows, cols)),
            block,
            full((5, width)),
            full((2, cols)),
        ],
    )
    return pl.pallas_call(
        functools.partial(k_attend_back, scale=scale),
        grid_spec=grid_spec,
        out_shape=[
            jax.ShapeDtypeStruct((items, rows, width), F32),
            jax.ShapeDtypeStruct((items, rows, width), BF),
            jax.ShapeDtypeStruct((items, 3, rows, cols), BF),
            jax.ShapeDtypeStruct((items, rows, width), BF),
            jax.ShapeDtypeStruct((5, width), F32),
            jax.ShapeDtypeStruct((2, cols), F32),
        ],
        compiler_params=params(),
        cost_estimate=SHORT,
        name="attend_back",
    )(text_len, mine, theirs, h, g, tokens, qkv, qkv, qkv, weights, w_out, vectors)


def k_attn_grad(slot_ref, a_ref, d_ref, y_ref, c_ref, *rest, base):
    acc, stage, sems = rest[-3:]
    outs = rest[:-3]
    i = pl.program_id(0)

    @pl.when(i == 0)
    def _():
        acc[...] = jnp.zeros_like(acc)

    for t in range(4):
        left, right = (a_ref[0], d_ref[0, t]) if t < 3 else (y_ref[0], c_ref[0])
        acc[t] += dot(left, right, TN)

    @pl.when(i == pl.num_programs(0) - 1)
    def _():
        write_chunks(slot_ref, base, acc, stage, outs, sems)


def attn_grad(slots, base, a, dqkv, dy, ctx, chunk, n_out):
    items, rows, width = a.shape
    cols = ctx.shape[2]
    grid_spec = pltpu.PrefetchScalarGridSpec(
        num_scalar_prefetch=1,
        grid=(items,),
        in_specs=[
            per_item((1, rows, width)),
            per_item((1, 3, rows, cols)),
            per_item((1, rows, width)),
            per_item((1, rows, cols)),
        ],
        out_specs=[ANY] * n_out,
        scratch_shapes=[
            pltpu.VMEM((4, width, cols), F32),
            pltpu.VMEM((chunk[0] * n_out,) + chunk[1:], BF),
            pltpu.SemaphoreType.DMA((n_out,)),
        ],
    )
    return pl.pallas_call(
        functools.partial(k_attn_grad, base=base),
        grid_spec=grid_spec,
        out_shape=[jax.ShapeDtypeStruct(chunk, BF)] * n_out,
        compiler_params=params(),
        cost_estimate=SHORT,
        name="attn_grad",
    )(slots, a, dqkv, dy, ctx)


def k_token_grad(dh_ref, dm_ref, dp_ref, tok_ref, vec_ref, o_ref):
    keep = o_ref.shape[1]
    da = dm_ref[0].astype(F32) + dp_ref[0].astype(F32)
    hat, spread = normed(tok_ref[0].astype(F32))
    out = dh_ref[0] + norm_back(da, hat, spread, vec_ref[0:1, :])
    o_ref[0] = out[:keep]


def token_grad(dh, mine, theirs, tokens, vectors, keep):
    items, rows, width = dh.shape
    return pl.pallas_call(
        k_token_grad,
        grid=(items,),
        in_specs=[per_item((1, rows, width))] * 4 + [full(vectors.shape)],
        out_specs=per_item((1, keep, width)),
        out_shape=jax.ShapeDtypeStruct((items, keep, width), F32),
        compiler_params=params(),
        cost_estimate=SHORT,
        name="token_grad",
    )(dh, mine, theirs, tokens, vectors)


def swap(value, axis, size, mask):
    return lax.ppermute(value, axis, [(i, i ^ mask) for i in range(size)])


def tie(value, *others):
    return lax.optimization_barrier((value,) + others)[0]


def add_low(a, b):
    return (a.astype(F32) + b.astype(F32)).astype(BF)


def per_device(
    tokens, text_len, routes, attn_gain, attn_shift, w_qkv, b_qv, w_out, b_out, ffn_gain, ffn_shift,
    w_up, b_up, w_down, b_down, cotangent, *, dp, rep,
):
    items, seq, width = tokens.shape
    rows = up_to(seq, SUB)
    share = w_qkv.shape[1]
    cols = w_qkv.shape[2]
    hidden = w_up.shape[2] // 2
    e_count = w_up.shape[0]
    scale = 1.0 / math.sqrt(HDIM)
    me = lax.axis_index("dp")
    core = me % 2
    by_permute = dp == 16 and share % SUB == 0
    masks = [m for m in (1, 2, 4, 8, 16, 32, 64, 128) if m < dp]

    def peer(value):
        return lax.ppermute(value, "rep", [(i, i ^ 1) for i in range(rep)])

    def partner(value):
        return swap(value, "dp", dp, 1)

    def dp_swap(value, mask):
        return swap(value, "dp", dp, mask)

    def halves(w):
        mine = lax.dynamic_slice_in_dim(w, core * hidden, hidden, 2)
        other = lax.dynamic_slice_in_dim(w, (1 - core) * hidden, hidden, 2)
        return mine, other

    attn_shard = jnp.concatenate([w_qkv, w_out[None]], axis=0)
    vectors = jnp.stack([attn_gain, attn_shift, b_out, ffn_gain, ffn_shift])
    pad = ((0, 0), (0, rows - seq), (0, 0))
    tok = jnp.pad(tokens, pad)
    bias = jnp.stack([b_qv[0], jnp.zeros_like(b_qv[0]), b_qv[1]])
    experts = jnp.stack([routes[:, 0], routes[:, seq - 1]]).astype(jnp.int32)
    b_up_mine = lax.dynamic_slice_in_dim(b_up, core * hidden, hidden, 1)
    cot_partner = partner(cotangent)
    tok_tied = tie(tok, cot_partner)

    if by_permute:
        here = me.astype(jnp.int32)
        own_attn = attn_shard[None]
        z8a, z4a = dp_swap(own_attn, 8), dp_swap(own_attn, 4)
        za = [own_attn, z4a, z8a, dp_swap(z8a, 4)]
        xa = [dp_swap(p, 2) for p in za]
        attn_pieces = za + xa + [partner(p) for p in za + xa]
        rel = [0, 4, 8, 12]
        rel = rel + [r ^ 2 for r in rel]
        attn_off = (here ^ jnp.array(rel + [r ^ 1 for r in rel], jnp.int32)) * share
        rel = [r ^ j for r in rel for j in (0, 1)]
        ffn_off = (here ^ jnp.array(rel, jnp.int32)) * share
        mine, other = halves(w_up)
        up_own = jnp.stack([mine, partner(other)])
        mine, other = halves(w_down)
        down_own = jnp.stack([mine, partner(other)])
        ids = jnp.arange(dp, dtype=jnp.int32) ^ here
        slots = (
            (ids & 1) * (dp // 2)
            + (ids & 2) // 2 * (dp // 4)
            + (ids & 4) // 4 * (dp // 8)
            + (ids & 8) // 8
        )
        n_out = 4
        ffn_chunk, attn_chunk = (dp // 4, e_count, share, hidden), (dp // 4, 4, share, cols)

        up_own = tie(up_own, *za)
        z8u, z4u = dp_swap(up_own, 8), dp_swap(up_own, 4)
        x0u = dp_swap(tie(up_own, *xa), 2)
        x0d = dp_swap(tie(down_own, *xa), 2)
    else:
        attn_pieces = [lax.all_gather(attn_shard, "dp", axis=1, tiled=True)[None]]
        gathered = lax.all_gather(w_up, "dp", axis=1, tiled=True)
        up_pieces = [halves(gathered)[0][None]]
        gathered = lax.all_gather(w_down, "dp", axis=1, tiled=True)
        down_pieces = [halves(gathered)[0][None]]
        attn_off = ffn_off = slots = jnp.zeros((1,), jnp.int32)
        n_out = 1
        ffn_chunk, attn_chunk = (1, e_count, width, hidden), (1, 4, width, cols)

    a, qkv, attn_w, out_w = project(tok_tied, vectors, bias, attn_pieces, attn_off)
    half = width // 2
    out_mine = lax.dynamic_slice_in_dim(out_w, core * half, half, 1)
    stage = [out_w]
    if by_permute:
        stage = stage + [z4u, z8u, x0u, x0d]
        z12u = dp_swap(tie(z8u, *stage), 4)
        x1u = dp_swap(tie(z4u, *stage), 2)
    out_half = peer(tie(out_mine, *stage))
    experts_partner = partner(tie(experts, *stage))
    ctx = attend(tie(text_len, *stage), qkv, scale)
    stage = [ctx, out_half, experts_partner]
    if by_permute:
        stage = stage + [z12u, x1u]
        x2u = dp_swap(tie(z8u, *stage), 2)
        x3u = dp_swap(tie(z12u, *stage), 2)
        z8d, z4d = (dp_swap(tie(down_own, *stage), r) for r in (8, 4))
    ctx_theirs = peer(tie(ctx, *stage))
    out_other = partner(tie(out_half, *stage))
    out_theirs = jnp.where(
        core == 0,
        jnp.concatenate([out_half, out_other], axis=1),
        jnp.concatenate([out_other, out_half], axis=1),
    )
    cots = [jnp.pad(tie(v, *stage), pad) for v in (cotangent, cot_partner)]
    experts_two = jnp.concatenate([experts, experts_partner], axis=1)
    stage = [*cots, ctx]
    if by_permute:
        stage = stage + [x2u]
    h, b = residual(tok, ctx, ctx_theirs, out_w, out_theirs, tie(vectors, *stage))
    stage = [h]
    if by_permute:
        stage = stage + [x3u, z8d, z4d]
        x1d = dp_swap(tie(z4d, *stage), 2)
        x2d = dp_swap(tie(z8d, *stage), 2)
        z12d = dp_swap(tie(z8d, *stage), 4)
        up_pieces = [up_own, z4u, z8u, z12u, x0u, x1u, x2u, x3u]
    b_two = [b, partner(tie(b, *stage))]

    act, slope = experts_up(tie(experts_two, *stage), ffn_off, b_two, b_up_mine, up_pieces)
    stage = [act]
    if by_permute:
        stage = stage + [x1d, z12d, x2d]
        x3d = dp_swap(tie(z12d, *stage), 2)
    *down_grad, grad_b_down = weight_grad(
        tie(experts_two, *stage), slots, 0, cots, act, ffn_chunk, n_out, e_count, items
    )
    stage = [grad_b_down]
    if by_permute:
        down_pieces = [down_own, z4d, z8d, z12d, x0d, x1d, x2d, x3d]

        def near(parts, core_slot, *others):
            return dp_swap(tie(parts[2 * core_slot + 1], *others), 2)

        def middle(parts, core_slot, got, *others):
            keep, got = tie(parts[2 * core_slot], got, *others), tie(got, *others)
            both = keep[2:4].astype(F32) + got[2:4].astype(F32)
            return keep, got, dp_swap(both.astype(BF), 4)

        def last(state, *others):
            keep, got, mid = state
            mid = tie(mid, *others)
            part = keep[1].astype(F32) + got[1].astype(F32) + mid[1].astype(F32)
            return keep, got, mid, dp_swap(part.astype(BF), 8)

        def total(state):
            keep, got, mid, end = state
            return (
                keep[0].astype(F32)
                + got[0].astype(F32)
                + mid[0].astype(F32)
                + end.astype(F32)
            )

        stage = stage + [x3d]
        dn1 = near(down_grad, 1, *stage)
    db_own, db_other, du, grad_b_up = experts_back(
        tie(experts_two, *stage), ffn_off, cots, slope, up_pieces, down_pieces, items
    )
    db = add_low(db_own, partner(db_other))
    stage = [db]
    if by_permute:
        stage = stage + [dn1]
        dm1 = middle(down_grad, 1, dn1, *stage)
        dn0 = near(down_grad, 0, *stage)
    db_theirs = peer(tie(db, *stage))
    *up_grad, _ = weight_grad(
        tie(experts_two, *stage), slots, 0, b_two, du, ffn_chunk, n_out, e_count, 0
    )
    stage = [up_grad[0]]
    if by_permute:
        stage = stage + [dm1[2]]
        un1 = near(up_grad, 1, *stage)
        de1 = last(dm1, *stage)
    z_own, z_other = experts_down(
        tie(experts_two, *stage), ffn_off, act, down_pieces, rows, items
    )
    stage = [z_own, db_theirs]
    if by_permute:
        stage = stage + [dn0, de1[3]]
        dm0 = middle(down_grad, 0, dn0, *stage)
        un0 = near(up_grad, 0, *stage)
    z = add_low(z_own, partner(tie(z_other, *stage)))
    z_theirs = peer(z)

    dh, dy, dqkv, da, sums, bias_sums = attend_back(
        tie(text_len, z), db, db_theirs, h, cots[0], tok, qkv, attn_w, out_w, vectors, scale
    )
    stage = [bias_sums, z_theirs]
    if by_permute:
        stage = stage + [dm0[2], un1]
        um1 = middle(up_grad, 1, un1, *stage)
        de0 = last(dm0, *stage)
    da_theirs = peer(tie(da, *stage))
    first_norm = tie(sums[3:5], *stage)
    first_norm_theirs = peer(first_norm)
    attn_parts = attn_grad(tie(slots, *stage), 0, a, dqkv, dy, ctx, attn_chunk, n_out)

    stage = [attn_parts[0], first_norm_theirs]
    up_pair = jnp.zeros((2, e_count, hidden), F32)
    up_pair = lax.dynamic_update_slice_in_dim(up_pair, grad_b_up[None], core, 0)
    small = jnp.concatenate(
        [
            (first_norm + first_norm_theirs).reshape(-1),
            sums[0:3].reshape(-1),
            grad_b_down.reshape(-1),
            up_pair.reshape(-1),
            bias_sums.reshape(-1),
        ]
    ).reshape(-1, LANES)
    steps = list(masks)

    def add_step(*others):
        nonlocal small
        small = tie(small, *others)
        got = swap(small, "dp", dp, steps.pop(0))
        small = small + got
        return got

    if by_permute:
        send = add_low(attn_parts[1], partner(attn_parts[3]))
        keep = add_low(attn_parts[0], partner(attn_parts[2]))
        stage = stage + [um1[2], de0[3], un0]
        an = near([keep, send], 0, *stage)
        ue1 = last(um1, *stage)
        um0 = middle(up_grad, 0, un0, *stage)
        down_other = total(tie(de1, *stage))
        down_got = partner(down_other)
    got = add_step(*stage)
    output = finish_output(tie(experts, *stage), h, z, z_theirs, b_down, seq)
    stage = [output, got]
    if by_permute:
        stage = stage + [down_got]
        down_mine = total(tie(de0, *stage))
    got = add_step(*stage)
    grad_tokens = token_grad(dh, da, da_theirs, tok, tie(vectors, *stage), seq)
    stage = [grad_tokens, got]
    if by_permute:
        stage = stage + [um0[2], ue1[3]]
        ue0 = last(um0, *stage)
        up_other = total(tie(ue1, *stage))
        up_got = partner(up_other)
    got = add_step(*stage)

    if by_permute:

        def joined(own, got):
            whole = jnp.zeros((e_count, share, 2 * hidden), F32)
            whole = lax.dynamic_update_slice_in_dim(whole, got, (1 - core) * hidden, 2)
            return lax.dynamic_update_slice_in_dim(whole, own, core * hidden, 2)

        am = middle([keep, send], 0, an, up_other)
        grad_w_down = joined(tie(down_mine, am[0]), down_got)
        ae = last(am, grad_w_down)
        grad_w_up = joined(total(ue0), up_got)
        grad_attn = total(tie(ae, grad_w_up))
        grad_w_qkv, grad_w_out = grad_attn[:3], grad_attn[3]
    else:

        def finish(chunk):
            whole = jnp.zeros((e_count, width, 2 * hidden), BF)
            whole = lax.dynamic_update_slice_in_dim(whole, chunk[0], core * hidden, 2)
            return lax.psum_scatter(whole, "dp", scatter_dimension=1, tiled=True).astype(F32)

        grad_w_down, grad_w_up = finish(down_grad[0]), finish(up_grad[0])
        grad_attn = lax.psum_scatter(attn_parts[0][0], "dp", scatter_dimension=1, tiled=True)
        grad_w_qkv, grad_w_out = grad_attn[:3].astype(F32), grad_attn[3].astype(F32)

    while steps:
        add_step()
    small = small.reshape(-1)
    at = 0

    def take(*shape):
        nonlocal at
        n = math.prod(shape)
        piece = small[at : at + n].reshape(shape)
        at += n
        return piece

    norm_one, norm_two, grad_b_out = take(2, width), take(2, width), take(width)
    total_down = take(e_count, width)
    total_up = jnp.moveaxis(take(2, e_count, hidden), 0, 1).reshape(e_count, 2 * hidden)
    total_qv = take(2, cols)
    return (
        output,
        grad_tokens,
        grad_w_qkv,
        grad_w_out,
        grad_w_up,
        grad_w_down,
        total_qv,
        grad_b_out,
        total_up,
        total_down,
        jnp.concatenate([norm_one, norm_two], axis=0),
    )


def solution(mesh):
    body = functools.partial(per_device, dp=mesh.shape["dp"], rep=mesh.shape["rep"])
    return jax.shard_map(
        body,
        mesh=mesh,
        in_specs=(
            P("dp", None, None),
            P("dp"),
            P("dp", None),
            P(),
            P(),
            P(None, "dp", "rep"),
            P(None, "rep"),
            P("dp", "rep"),
            P(),
            P(),
            P(),
            P(None, "dp", "rep"),
            P(None, "rep"),
            P(None, "dp", "rep"),
            P(),
            P("dp", None, None),
        ),
        out_specs=(
            P("dp", None, None),
            P("dp", None, None),
            P(None, "dp", "rep"),
            P("dp", "rep"),
            P(None, "dp", "rep"),
            P(None, "dp", "rep"),
            P(None, "rep"),
            P(),
            P(None, "rep"),
            P(),
            P(),
        ),
        check_vma=False,
    )
```

```python
import functools
import math

import jax
import jax.numpy as jnp
from jax import lax
from jax.experimental import pallas as pl
from jax.experimental.pallas import tpu as pltpu
from jax.sharding import PartitionSpec as P

HDIM = 64
IMG = 197
EPSILON = 1e-05
ROOT_HALF = 0.7071067811865476
INV_ROOT_TAU = 0.3989422804014327
SUB = 16
LANES = 128
BF = jnp.bfloat16
F32 = jnp.float32

NN = (((1,), (0,)), ((), ()))
NT = (((1,), (1,)), ((), ()))
TN = (((0,), (0,)), ((), ()))


def up_to(n, m):
    return -(-n // m) * m


def dot(a, b, dims):
    return lax.dot_general(a, b, dims, preferred_element_type=F32)


def full(shape):
    zeros = (0,) * len(shape)
    return pl.BlockSpec(shape, lambda *_: zeros)


def per_item(shape):
    zeros = (0,) * (len(shape) - 1)
    return pl.BlockSpec(shape, lambda i, *_: (i,) + zeros)


ANY = pl.BlockSpec(memory_space=pl.ANY)


def params():
    return pltpu.CompilerParams(vmem_limit_bytes=60 * 1024 * 1024)


SHORT = pl.CostEstimate(flops=1, transcendentals=0, bytes_accessed=1)


def normed(v):
    centred = v - jnp.mean(v, axis=-1, keepdims=True)
    var = jnp.mean(centred * centred, axis=-1, keepdims=True)
    spread = lax.rsqrt(var + EPSILON)
    return centred * spread, spread


def norm_back(grad, hat, spread, gain):
    scaled = grad * gain
    return spread * (
        scaled
        - jnp.mean(scaled, axis=-1, keepdims=True)
        - hat * jnp.mean(scaled * hat, axis=-1, keepdims=True)
    )


def run_copies(copies, *, start=False, wait=False):
    for c in copies:
        if start:
            c.start()
        if wait:
            c.wait()


def place_copies(off_ref, pieces, dest, sems, plane=0):
    copies = []
    for n, piece in enumerate(pieces):
        subs, _, rows, _ = piece.shape
        for j in range(subs):
            at = off_ref[n * subs + j]
            copies.append(
                pltpu.make_async_copy(
                    piece.at[j, plane : plane + dest.shape[0]],
                    dest.at[:, pl.ds(pl.multiple_of(at, SUB), rows), :],
                    sems.at[n * subs + j],
                )
            )
    return copies


def k_proj(off_ref, tok_ref, vec_ref, bias_ref, *rest):
    a_ref, qkv_ref, w_ref, wo_ref, sems, out_sems = rest[-6:]
    pieces = rest[:-6]
    first = pl.program_id(0) == 0

    @pl.when(first)
    def _():
        run_copies(place_copies(off_ref, pieces, w_ref, sems), start=True)
        run_copies(place_copies(off_ref, pieces, wo_ref, out_sems, 3), start=True)

    hat, _ = normed(tok_ref[0].astype(F32))
    a_ref[0] = (hat * vec_ref[0:1, :] + vec_ref[1:2, :]).astype(BF)

    @pl.when(first)
    def _():
        run_copies(place_copies(off_ref, pieces, w_ref, sems), wait=True)
        run_copies(place_copies(off_ref, pieces, wo_ref, out_sems, 3), wait=True)

    a = a_ref[0]
    for t in range(3):
        qkv_ref[t, 0] = (dot(a, w_ref[t], NN) + bias_ref[t : t + 1, :]).astype(BF)


def project(tokens, vectors, bias, pieces, offsets):
    items, rows, width = tokens.shape
    cols = pieces[0].shape[3]
    count = len(pieces) * pieces[0].shape[0]
    grid_spec = pltpu.PrefetchScalarGridSpec(
        num_scalar_prefetch=1,
        grid=(items,),
        in_specs=[
            per_item((1, rows, width)),
            full(vectors.shape),
            full((3, cols)),
        ]
        + [ANY] * len(pieces),
        out_specs=[
            per_item((1, rows, width)),
            pl.BlockSpec((3, 1, rows, cols), lambda i, *_: (0, i, 0, 0)),
            full((3, width, cols)),
            full((1, width, cols)),
        ],
        scratch_shapes=[pltpu.SemaphoreType.DMA((count,)), pltpu.SemaphoreType.DMA((count,))],
    )
    return pl.pallas_call(
        k_proj,
        grid_spec=grid_spec,
        out_shape=[
            jax.ShapeDtypeStruct((items, rows, width), BF),
            jax.ShapeDtypeStruct((3, items, rows, cols), BF),
            jax.ShapeDtypeStruct((3, width, cols), BF),
            jax.ShapeDtypeStruct((1, width, cols), BF),
        ],
        compiler_params=params(),
        cost_estimate=SHORT,
        name="project",
    )(offsets, tokens, vectors, bias, *pieces)


def k_attend(len_ref, q_ref, k_ref, v_ref, c_ref, *, scale):
    rows, width = c_ref.shape[1:]
    length = len_ref[pl.program_id(0)]
    valid = lax.broadcasted_iota(jnp.int32, (1, rows), 1) < IMG + length
    low = lax.broadcasted_iota(jnp.int32, (1, LANES), 1) < HDIM
    for pair in range(width // LANES):
        cols = slice(pair * LANES, (pair + 1) * LANES)
        q, k, v = q_ref[0, 0, :, cols], k_ref[0, 0, :, cols], v_ref[0, 0, :, cols]
        both = []
        for side in (low, ~low):
            s = dot(q * side.astype(BF), k, NT) * scale
            s = jnp.where(valid, s, -1e30)
            e = jnp.exp(s - jnp.max(s, axis=-1, keepdims=True))
            p = (e / jnp.sum(e, axis=-1, keepdims=True)).astype(BF)
            both.append(dot(p, v, NN))
        c_ref[0, :, cols] = jnp.where(low, both[0], both[1]).astype(BF)


def qkv_specs(rows, cols):
    return [pl.BlockSpec((1, 1, rows, cols), lambda i, *_, t=t: (t, i, 0, 0)) for t in range(3)]


def attend(text_len, qkv, scale):
    _, items, rows, cols = qkv.shape
    grid_spec = pltpu.PrefetchScalarGridSpec(
        num_scalar_prefetch=1,
        grid=(items,),
        in_specs=qkv_specs(rows, cols),
        out_specs=per_item((1, rows, cols)),
    )
    return pl.pallas_call(
        functools.partial(k_attend, scale=scale),
        grid_spec=grid_spec,
        out_shape=jax.ShapeDtypeStruct((items, rows, cols), BF),
        compiler_params=params(),
        cost_estimate=SHORT,
        name="attend",
    )(text_len, qkv, qkv, qkv)


def k_residual(tok_ref, cm_ref, cp_ref, wm_ref, wp_ref, vec_ref, h_ref, b_ref):
    y = dot(cm_ref[0], wm_ref[0], NT) + dot(cp_ref[0], wp_ref[0], NT)
    h = tok_ref[0].astype(F32) + (y + vec_ref[2:3, :])
    h_ref[0] = h
    hat, _ = normed(h)
    b_ref[0] = (hat * vec_ref[3:4, :] + vec_ref[4:5, :]).astype(BF)


def residual(tokens, mine, theirs, w_mine, w_theirs, vectors):
    items, rows, width = tokens.shape
    cols = mine.shape[2]
    return pl.pallas_call(
        k_residual,
        grid=(items,),
        in_specs=[
            per_item((1, rows, width)),
            per_item((1, rows, cols)),
            per_item((1, rows, cols)),
            full((1, width, cols)),
            full((1, width, cols)),
            full(vectors.shape),
        ],
        out_specs=[per_item((1, rows, width))] * 2,
        out_shape=[
            jax.ShapeDtypeStruct(tokens.shape, F32),
            jax.ShapeDtypeStruct(tokens.shape, BF),
        ],
        compiler_params=params(),
        cost_estimate=SHORT,
        name="residual",
    )(tokens, mine, theirs, w_mine, w_theirs, vectors)


def segments(rows):
    head = up_to(IMG, SUB)
    tail = IMG // SUB * SUB
    return (0, head), (tail, rows - tail), head


def segment_masks(rows):
    (a0, an), (b0, bn), _ = segments(rows)
    in_a = lax.broadcasted_iota(jnp.int32, (an, 1), 0) + a0 < IMG
    in_b = lax.broadcasted_iota(jnp.int32, (bn, 1), 0) + b0 >= IMG
    return in_a, in_b


def masked_parts(g_ref, i):
    rows = g_ref.shape[1]
    (a0, an), (b0, bn), _ = segments(rows)
    in_a, in_b = segment_masks(rows)
    g_a = jnp.where(in_a, g_ref[i, a0 : a0 + an, :].astype(F32), 0.0)
    g_b = jnp.where(in_b, g_ref[i, b0 : b0 + bn, :].astype(F32), 0.0)
    return g_a, g_b


def item_copies(refs, dest, sems):
    copies = []
    for ref in refs:
        if len(ref.shape) == 2:
            copies.append(
                pltpu.make_async_copy(ref, dest.at[len(copies)], sems.at[len(copies)])
            )
        else:
            for j in range(ref.shape[0]):
                copies.append(
                    pltpu.make_async_copy(ref.at[j], dest.at[len(copies)], sems.at[len(copies)])
                )
    return copies


def wait_item(copies, i):
    for n, c in enumerate(copies):

        @pl.when(i == n)
        def _(c=c):
            c.wait()


def write_chunks(slot_ref, base, acc, stage, outs, sems):
    count, _, rows, _ = stage.shape
    for c in range(count):
        stage[slot_ref[base + c]] = acc[:, c * rows : (c + 1) * rows, :].astype(BF)
    per = count // len(outs)
    copies = [
        pltpu.make_async_copy(stage.at[n * per : (n + 1) * per], out, sems.at[n])
        for n, out in enumerate(outs)
    ]
    run_copies(copies, start=True)
    run_copies(copies, wait=True)


def k_up(e_ref, off_ref, bias_ref, *rest, n_left):
    b_refs, pieces = rest[:n_left], rest[n_left:-6]
    act_ref, slope_ref, b_s, w_s, b_sem, w_sem = rest[-6:]
    i = pl.program_id(0)
    b_copies = item_copies(b_refs, b_s, b_sem)

    @pl.when(i == 0)
    def _():
        run_copies(b_copies[:1], start=True)
        w_copies = place_copies(off_ref, pieces, w_s, w_sem)
        run_copies(w_copies, start=True)
        run_copies(b_copies[1:], start=True)
        run_copies(w_copies, wait=True)

    wait_item(b_copies, i)
    seg_a, seg_b, _ = segments(b_s.shape[1])
    at = 0
    for which, (lo, n) in zip((0, 1), (seg_a, seg_b)):
        e = e_ref[which, i]
        u = dot(b_s[i, lo : lo + n, :], w_s[e], NN) + bias_ref[pl.ds(e, 1), :]
        cdf = 0.5 * (1.0 + lax.erf(u * ROOT_HALF))
        act_ref[0, at : at + n, :] = (u * cdf).astype(BF)
        slope_ref[0, at : at + n, :] = (cdf + u * jnp.exp(-0.5 * u * u) * INV_ROOT_TAU).astype(BF)
        at += n


def experts_up(experts, offsets, b, bias, pieces):
    items = experts.shape[1]
    rows, width = b[0].shape[-2:]
    e_count, _, hidden = pieces[0].shape[1:]
    count = len(pieces) * pieces[0].shape[0]
    (_, an), (_, bn), _ = segments(rows)
    grid_spec = pltpu.PrefetchScalarGridSpec(
        num_scalar_prefetch=2,
        grid=(items,),
        in_specs=[full((e_count, hidden))] + [ANY] * (len(b) + len(pieces)),
        out_specs=[per_item((1, an + bn, hidden))] * 2,
        scratch_shapes=[
            pltpu.VMEM((items, rows, width), BF),
            pltpu.VMEM((e_count, width, hidden), BF),
            pltpu.SemaphoreType.DMA((items,)),
            pltpu.SemaphoreType.DMA((count,)),
        ],
    )
    return pl.pallas_call(
        functools.partial(k_up, n_left=len(b)),
        grid_spec=grid_spec,
        out_shape=[jax.ShapeDtypeStruct((items, an + bn, hidden), BF)] * 2,
        compiler_params=params(),
        cost_estimate=SHORT,
        name="experts_up",
    )(experts, offsets, bias, *b, *pieces)


def k_weight_grad(e_ref, slot_ref, right_ref, *rest, n_left, n_out, base, own):
    lefts = rest[:n_left]
    outs = rest[n_left : n_left + n_out]
    left_s, dw_s, stage, left_sem, out_sem = rest[-5:]
    sums_ref = rest[n_left + n_out]
    i = pl.program_id(0)
    copies = item_copies(lefts, left_s, left_sem)

    @pl.when(i == 0)
    def _():
        run_copies(copies, start=True)
        dw_s[...] = jnp.zeros_like(dw_s)
        sums_ref[...] = jnp.zeros_like(sums_ref)

    wait_item(copies, i)
    at = 0
    for which, left in zip((0, 1), masked_parts(left_s, i)):
        e = e_ref[which, i]
        n = left.shape[0]
        dw_s[e] += dot(left.astype(BF), right_ref[0, at : at + n, :], TN)

        @pl.when(i < own)
        def _(left=left, e=e):
            sums_ref[pl.ds(e, 1), :] += jnp.sum(left, axis=0, keepdims=True)

        at += n

    @pl.when(i == pl.num_programs(0) - 1)
    def _():
        write_chunks(slot_ref, base, dw_s, stage, outs, out_sem)


def weight_grad(experts, slots, base, left, right, chunk, n_out, e_count, own):
    items, seg_rows, hidden = right.shape
    rows, width = left[0].shape[-2:]
    count = chunk[0] * n_out
    grid_spec = pltpu.PrefetchScalarGridSpec(
        num_scalar_prefetch=2,
        grid=(items,),
        in_specs=[per_item((1, seg_rows, hidden))] + [ANY] * len(left),
        out_specs=[ANY] * n_out + [full((e_count, width))],
        scratch_shapes=[
            pltpu.VMEM((items, rows, width), BF),
            pltpu.VMEM((e_count, width, hidden), F32),
            pltpu.VMEM((count,) + chunk[1:], BF),
            pltpu.SemaphoreType.DMA((items,)),
            pltpu.SemaphoreType.DMA((n_out,)),
        ],
    )
    return pl.pallas_call(
        functools.partial(
            k_weight_grad, n_left=len(left), n_out=n_out, base=base, own=own
        ),
        grid_spec=grid_spec,
        out_shape=[jax.ShapeDtypeStruct(chunk, BF)] * n_out
        + [jax.ShapeDtypeStruct((e_count, width), F32)],
        compiler_params=params(),
        cost_estimate=SHORT,
        name="weight_grad",
    )(experts, slots, right, *left)


def store_joined(ref, first, middle, second, tail, head):
    ref[0, :tail, :] = first[:tail].astype(BF)
    ref[0, tail:head, :] = middle.astype(BF)
    ref[0, head:, :] = second[head - tail :].astype(BF)


def k_back(e_ref, off_ref, slope_ref, *rest, n_left, n_up, own):
    g_s, w_up, w_down, sem_g, sem_up, sem_down = rest[-6:]
    do_ref, dp_ref, du_ref, gbu_ref = rest[-10:-6]
    lefts, ups, downs = rest[:n_left], rest[n_left : n_left + n_up], rest[n_left + n_up : -10]
    i = pl.program_id(0)
    copies = item_copies(lefts, g_s, sem_g)

    @pl.when(i == 0)
    def _():
        w_copies = place_copies(off_ref, downs, w_down, sem_down)
        run_copies(copies[:1] + w_copies, start=True)
        more = place_copies(off_ref, ups, w_up, sem_up)
        run_copies(more + copies[1:], start=True)
        gbu_ref[...] = jnp.zeros_like(gbu_ref)
        run_copies(w_copies + more, wait=True)

    wait_item(copies, i)
    rows = g_s.shape[1]
    seg_a, seg_b, head = segments(rows)
    tail = seg_b[0]
    at = 0
    both = []
    for which, g in zip((0, 1), masked_parts(g_s, i)):
        e = e_ref[which, i]
        n = g.shape[0]
        dact = dot(g.astype(BF), w_down[e], NN)
        du = (dact * slope_ref[0, at : at + n, :].astype(F32)).astype(BF)
        du_ref[0, at : at + n, :] = du
        gbu_ref[pl.ds(e, 1), :] += jnp.sum(du.astype(F32), axis=0, keepdims=True)
        both.append(dot(du, w_up[e], NT))
        at += n
    middle = both[0][tail:] + both[1][: head - tail]
    for cond, db_ref in ((i < own, do_ref), (i >= own, dp_ref)):

        @pl.when(cond)
        def _(db_ref=db_ref):
            store_joined(db_ref, both[0], middle, both[1], tail, head)


def own_and_other(rows, width, own):
    block = (1, rows, width)
    return [
        pl.BlockSpec(block, lambda i, *_: (jnp.minimum(i, own - 1), 0, 0)),
        pl.BlockSpec(block, lambda i, *_: (jnp.maximum(i - own, 0), 0, 0)),
    ]


def experts_back(experts, offsets, left, slope, ups, downs, own):
    rows, width = left[0].shape[-2:]
    e_count, _, hidden = ups[0].shape[1:]
    count = len(ups) * ups[0].shape[0]
    items, seg_rows, _ = slope.shape
    grid_spec = pltpu.PrefetchScalarGridSpec(
        num_scalar_prefetch=2,
        grid=(items,),
        in_specs=[per_item((1, seg_rows, hidden))]
        + [ANY] * (len(left) + len(ups) + len(downs)),
        out_specs=own_and_other(rows, width, own)
        + [per_item((1, seg_rows, hidden)), full((e_count, hidden))],
        scratch_shapes=[
            pltpu.VMEM((items, rows, width), BF),
            pltpu.VMEM((e_count, width, hidden), BF),
            pltpu.VMEM((e_count, width, hidden), BF),
            pltpu.SemaphoreType.DMA((items,)),
            pltpu.SemaphoreType.DMA((count,)),
            pltpu.SemaphoreType.DMA((count,)),
        ],
    )
    return pl.pallas_call(
        functools.partial(k_back, n_left=len(left), n_up=len(ups), own=own),
        grid_spec=grid_spec,
        out_shape=[
            jax.ShapeDtypeStruct((own, rows, width), BF),
            jax.ShapeDtypeStruct((items - own, rows, width), BF),
            jax.ShapeDtypeStruct((items, seg_rows, hidden), BF),
            jax.ShapeDtypeStruct((e_count, hidden), F32),
        ],
        compiler_params=params(),
        cost_estimate=SHORT,
        name="experts_back",
    )(experts, offsets, slope, *left, *ups, *downs)


def k_down(e_ref, off_ref, act_ref, *rest, own):
    zo_ref, zp_ref, w_down, sems = rest[-4:]
    pieces = rest[:-4]
    i = pl.program_id(0)

    @pl.when(i == 0)
    def _():
        copies = place_copies(off_ref, pieces, w_down, sems)
        run_copies(copies, start=True)
        run_copies(copies, wait=True)

    rows = zo_ref.shape[1]
    seg_a, seg_b, head = segments(rows)
    tail = seg_b[0]
    z_a = dot(act_ref[0, : seg_a[1], :], w_down[e_ref[0, i]], NT)
    z_b = dot(act_ref[0, seg_a[1] :, :], w_down[e_ref[1, i]], NT)
    image = lax.broadcasted_iota(jnp.int32, (head - tail, 1), 0) + tail < IMG
    middle = jnp.where(image, z_a[tail:], z_b[: head - tail])
    for cond, z_ref in ((i < own, zo_ref), (i >= own, zp_ref)):

        @pl.when(cond)
        def _(z_ref=z_ref):
            store_joined(z_ref, z_a, middle, z_b, tail, head)


def experts_down(experts, offsets, act, pieces, rows, own):
    items, seg_rows, hidden = act.shape
    e_count = pieces[0].shape[1]
    width = sum(p.shape[0] * p.shape[2] for p in pieces)
    count = len(pieces) * pieces[0].shape[0]
    grid_spec = pltpu.PrefetchScalarGridSpec(
        num_scalar_prefetch=2,
        grid=(items,),
        in_specs=[per_item((1, seg_rows, hidden))] + [ANY] * len(pieces),
        out_specs=own_and_other(rows, width, own),
        scratch_shapes=[
            pltpu.VMEM((e_count, width, hidden), BF),
            pltpu.SemaphoreType.DMA((count,)),
        ],
    )
    return pl.pallas_call(
        functools.partial(k_down, own=own),
        grid_spec=grid_spec,
        out_shape=[
            jax.ShapeDtypeStruct((own, rows, width), BF),
            jax.ShapeDtypeStruct((items - own, rows, width), BF),
        ],
        compiler_params=params(),
        cost_estimate=SHORT,
        name="experts_down",
    )(experts, offsets, act, *pieces)


def k_output(e_ref, h_ref, zm_ref, zp_ref, bias_ref, o_ref):
    i = pl.program_id(0)
    rows, keep = h_ref.shape[1], o_ref.shape[1]
    image = lax.broadcasted_iota(jnp.int32, (rows, 1), 0) < IMG
    bias = jnp.where(image, bias_ref[pl.ds(e_ref[0, i], 1), :], bias_ref[pl.ds(e_ref[1, i], 1), :])
    out = h_ref[0] + ((zm_ref[0].astype(F32) + zp_ref[0].astype(F32)) + bias)
    o_ref[0] = out[:keep].astype(BF)


def finish_output(experts, h, mine, theirs, bias, keep):
    items, rows, width = h.shape
    grid_spec = pltpu.PrefetchScalarGridSpec(
        num_scalar_prefetch=1,
        grid=(items,),
        in_specs=[per_item((1, rows, width))] * 3 + [full(bias.shape)],
        out_specs=per_item((1, keep, width)),
    )
    return pl.pallas_call(
        k_output,
        grid_spec=grid_spec,
        out_shape=jax.ShapeDtypeStruct((items, keep, width), BF),
        compiler_params=params(),
        cost_estimate=SHORT,
        name="finish_output",
    )(experts, h, mine, theirs, bias)


def k_attend_back(
    len_ref, slot_ref, dm_ref, dp_ref, h_ref, g_ref, tok_ref, a_ref, c_ref, q_ref, k_ref, v_ref,
    w_ref, wo_ref, vec_ref, dh_ref, da_ref, one_ref, two_ref, bias_ref, *rest, scale,
):
    dqkv, acc, stage, sems = rest[-4:]
    outs = rest[:-4]
    rows, width = dh_ref.shape[1:]
    cols = q_ref.shape[3]
    i = pl.program_id(0)

    @pl.when(i == 0)
    def _():
        one_ref[...] = jnp.zeros_like(one_ref)
        two_ref[...] = jnp.zeros_like(two_ref)
        bias_ref[...] = jnp.zeros_like(bias_ref)
        acc[...] = jnp.zeros_like(acc)

    def add_rows(ref, at, value):
        ref[at : at + 1, :] += jnp.sum(value, axis=0, keepdims=True)

    db = dm_ref[0].astype(F32) + dp_ref[0].astype(F32)
    hat, spread = normed(h_ref[0])
    dh = g_ref[0].astype(F32) + norm_back(db, hat, spread, vec_ref[3:4, :])
    dh_ref[0] = dh
    dy = dh.astype(BF)
    add_rows(two_ref, 0, db * hat)
    add_rows(two_ref, 1, db)
    add_rows(two_ref, 2, dy.astype(F32))
    dctx = dot(dy, wo_ref[0], NN).astype(BF)
    valid = lax.broadcasted_iota(jnp.int32, (rows, 1), 0) < IMG + len_ref[i]
    low = lax.broadcasted_iota(jnp.int32, (1, LANES), 1) < HDIM
    for pair in range(cols // LANES):
        at = slice(pair * LANES, (pair + 1) * LANES)
        q, k, v = q_ref[0, 0, :, at], k_ref[0, 0, :, at], v_ref[0, 0, :, at]
        dc = dctx[:, at]
        parts = []
        for side in (low, ~low):
            only = side.astype(BF)
            s = dot(k * only, q, NT) * scale
            s = jnp.where(valid, s, -1e30)
            e = jnp.exp(s - jnp.max(s, axis=0, keepdims=True))
            p = e / jnp.sum(e, axis=0, keepdims=True)
            dp = dot(v * only, dc, NT)
            ds = (p * (dp - jnp.sum(p * dp, axis=0, keepdims=True))).astype(BF)
            parts.append((dot(ds, k, TN), dot(ds, q, NN), dot(p.astype(BF), dc, NN)))
        dqkv[0, :, at] = (jnp.where(low, parts[0][0], parts[1][0]) * scale).astype(BF)
        dqkv[1, :, at] = (jnp.where(low, parts[0][1], parts[1][1]) * scale).astype(BF)
        dqkv[2, :, at] = jnp.where(low, parts[0][2], parts[1][2]).astype(BF)
    da = dot(dqkv[0], w_ref[0], NT)
    da += dot(dqkv[1], w_ref[1], NT)
    da += dot(dqkv[2], w_ref[2], NT)
    add_rows(bias_ref, 0, dqkv[0].astype(F32))
    add_rows(bias_ref, 1, dqkv[2].astype(F32))
    hat, _ = normed(tok_ref[0].astype(F32))
    add_rows(one_ref, 0, da * hat)
    add_rows(one_ref, 1, da)
    da_ref[0] = da.astype(BF)
    for t in range(3):
        acc[t] += dot(a_ref[0], dqkv[t], TN)
    acc[3] += dot(dy, c_ref[0], TN)

    @pl.when(i == pl.num_programs(0) - 1)
    def _():
        write_chunks(slot_ref, 0, acc, stage, outs, sems)


def attend_back(
    text_len, slots, mine, theirs, h, g, tokens, a, ctx, qkv, weights, w_out, vectors, chunk, n_out, scale
):
    items, rows, width = h.shape
    cols = qkv.shape[3]
    block = per_item((1, rows, width))
    grid_spec = pltpu.PrefetchScalarGridSpec(
        num_scalar_prefetch=2,
        grid=(items,),
        in_specs=[block] * 6
        + [per_item((1, rows, cols))]
        + qkv_specs(rows, cols)
        + [full(weights.shape), full(w_out.shape), full(vectors.shape)],
        out_specs=[block, block, full((2, width)), full((3, width)), full((2, cols))]
        + [ANY] * n_out,
        scratch_shapes=[
            pltpu.VMEM((3, rows, cols), BF),
            pltpu.VMEM((4, width, cols), F32),
            pltpu.VMEM((chunk[0] * n_out,) + chunk[1:], BF),
            pltpu.SemaphoreType.DMA((n_out,)),
        ],
    )
    return pl.pallas_call(
        functools.partial(k_attend_back, scale=scale),
        grid_spec=grid_spec,
        out_shape=[
            jax.ShapeDtypeStruct((items, rows, width), F32),
            jax.ShapeDtypeStruct((items, rows, width), BF),
            jax.ShapeDtypeStruct((2, width), F32),
            jax.ShapeDtypeStruct((3, width), F32),
            jax.ShapeDtypeStruct((2, cols), F32),
        ]
        + [jax.ShapeDtypeStruct(chunk, BF)] * n_out,
        compiler_params=params(),
        cost_estimate=SHORT,
        name="attend_back",
    )(text_len, slots, mine, theirs, h, g, tokens, a, ctx, qkv, qkv, qkv, weights, w_out, vectors)


def k_token_grad(dh_ref, dm_ref, dp_ref, tok_ref, vec_ref, o_ref):
    keep = o_ref.shape[1]
    da = dm_ref[0].astype(F32) + dp_ref[0].astype(F32)
    hat, spread = normed(tok_ref[0].astype(F32))
    out = dh_ref[0] + norm_back(da, hat, spread, vec_ref[0:1, :])
    o_ref[0] = out[:keep]


def token_grad(dh, mine, theirs, tokens, vectors, keep):
    items, rows, width = dh.shape
    return pl.pallas_call(
        k_token_grad,
        grid=(items,),
        in_specs=[per_item((1, rows, width))] * 4 + [full(vectors.shape)],
        out_specs=per_item((1, keep, width)),
        out_shape=jax.ShapeDtypeStruct((items, keep, width), F32),
        compiler_params=params(),
        cost_estimate=SHORT,
        name="token_grad",
    )(dh, mine, theirs, tokens, vectors)


def swap(value, axis, size, mask):
    return lax.ppermute(value, axis, [(i, i ^ mask) for i in range(size)])


def tie(value, *others):
    return lax.optimization_barrier((value,) + others)[0]


def add_low(a, b):
    return (a.astype(F32) + b.astype(F32)).astype(BF)


def per_device(
    tokens, text_len, routes, attn_gain, attn_shift, w_qkv, b_qv, w_out, b_out, ffn_gain, ffn_shift,
    w_up, b_up, w_down, b_down, cotangent, *, dp, rep,
):
    items, seq, width = tokens.shape
    rows = up_to(seq, SUB)
    share = w_qkv.shape[1]
    cols = w_qkv.shape[2]
    hidden = w_up.shape[2] // 2
    e_count = w_up.shape[0]
    scale = 1.0 / math.sqrt(HDIM)
    me = lax.axis_index("dp")
    core = me % 2
    by_permute = dp == 16 and share % SUB == 0
    masks = [m for m in (1, 128, 64, 32, 16, 8, 4, 2) if m < dp]

    def peer(value):
        return lax.ppermute(value, "rep", [(i, i ^ 1) for i in range(rep)])

    def partner(value):
        return swap(value, "dp", dp, 1)

    def dp_swap(value, mask):
        return swap(value, "dp", dp, mask)

    def halves(w):
        mine = lax.dynamic_slice_in_dim(w, core * hidden, hidden, 2)
        other = lax.dynamic_slice_in_dim(w, (1 - core) * hidden, hidden, 2)
        return mine, other

    attn_shard = jnp.concatenate([w_qkv, w_out[None]], axis=0)
    vectors = jnp.stack([attn_gain, attn_shift, b_out, ffn_gain, ffn_shift])
    pad = ((0, 0), (0, rows - seq), (0, 0))
    tok = jnp.pad(tokens, pad)
    bias = jnp.stack([b_qv[0], jnp.zeros_like(b_qv[0]), b_qv[1]])
    experts = jnp.stack([routes[:, 0], routes[:, seq - 1]]).astype(jnp.int32)
    b_up_mine = lax.dynamic_slice_in_dim(b_up, core * hidden, hidden, 1)
    cot_partner = partner(cotangent)
    tok_tied = tie(tok, cot_partner)

    if by_permute:
        here = me.astype(jnp.int32)
        own_attn = attn_shard[None]
        z8a, z4a = dp_swap(own_attn, 8), dp_swap(own_attn, 4)
        za = [own_attn, z4a, z8a, dp_swap(z8a, 4)]
        xa = [dp_swap(p, 2) for p in za]
        attn_pieces = za + xa + [partner(p) for p in za + xa]
        rel = [0, 4, 8, 12]
        rel = rel + [r ^ 2 for r in rel]
        attn_off = (here ^ jnp.array(rel + [r ^ 1 for r in rel], jnp.int32)) * share
        rel = [r ^ j for r in rel for j in (0, 1)]
        ffn_off = (here ^ jnp.array(rel, jnp.int32)) * share
        mine, other = halves(w_up)
        up_own = jnp.stack([mine, partner(other)])
        mine, other = halves(w_down)
        down_own = jnp.stack([mine, partner(other)])
        ids = jnp.arange(dp, dtype=jnp.int32) ^ here
        slots = (
            (ids & 1) * (dp // 2)
            + (ids & 2) // 2 * (dp // 4)
            + (ids & 4) // 4 * (dp // 8)
            + (ids & 8) // 8
        )
        n_out = 4
        ffn_chunk, attn_chunk = (dp // 4, e_count, share, hidden), (dp // 4, 4, share, cols)

        up_own = tie(up_own, *za)
        z8u, z4u = dp_swap(up_own, 8), dp_swap(up_own, 4)
        x0u = dp_swap(tie(up_own, *xa), 2)
        x0d = dp_swap(tie(down_own, *xa), 2)
    else:
        attn_pieces = [lax.all_gather(attn_shard, "dp", axis=1, tiled=True)[None]]
        gathered = lax.all_gather(w_up, "dp", axis=1, tiled=True)
        up_pieces = [halves(gathered)[0][None]]
        gathered = lax.all_gather(w_down, "dp", axis=1, tiled=True)
        down_pieces = [halves(gathered)[0][None]]
        attn_off = ffn_off = slots = jnp.zeros((1,), jnp.int32)
        n_out = 1
        ffn_chunk, attn_chunk = (1, e_count, width, hidden), (1, 4, width, cols)

    a, qkv, attn_w, out_w = project(tok_tied, vectors, bias, attn_pieces, attn_off)
    half = width // 2
    out_mine = lax.dynamic_slice_in_dim(out_w, core * half, half, 1)
    stage = [out_w]
    if by_permute:
        stage = stage + [z4u, z8u, x0u, x0d]
        z12u = dp_swap(tie(z8u, *stage), 4)
        x1u = dp_swap(tie(z4u, *stage), 2)
    out_half = peer(tie(out_mine, *stage))
    experts_partner = partner(tie(experts, *stage))
    ctx = attend(tie(text_len, *stage), qkv, scale)
    stage = [ctx, out_half, experts_partner]
    if by_permute:
        stage = stage + [z12u, x1u]
        x2u = dp_swap(tie(z8u, *stage), 2)
        x3u = dp_swap(tie(z12u, *stage), 2)
        z8d, z4d = (dp_swap(tie(down_own, *stage), r) for r in (8, 4))
    ctx_theirs = peer(tie(ctx, *stage))
    out_other = partner(tie(out_half, *stage))
    out_theirs = jnp.where(
        core == 0,
        jnp.concatenate([out_half, out_other], axis=1),
        jnp.concatenate([out_other, out_half], axis=1),
    )
    cots = [jnp.pad(tie(v, *stage), pad) for v in (cotangent, cot_partner)]
    experts_two = jnp.concatenate([experts, experts_partner], axis=1)
    stage = [*cots, ctx]
    if by_permute:
        stage = stage + [x2u]
    h, b = residual(tok, ctx, ctx_theirs, out_w, out_theirs, tie(vectors, *stage))
    stage = [h]
    if by_permute:
        stage = stage + [x3u, z8d, z4d]
        x1d = dp_swap(tie(z4d, *stage), 2)
        x2d = dp_swap(tie(z8d, *stage), 2)
        z12d = dp_swap(tie(z8d, *stage), 4)
        up_pieces = [up_own, z4u, z8u, z12u, x0u, x1u, x2u, x3u]
    b_two = [b, partner(tie(b, *stage))]

    act, slope = experts_up(tie(experts_two, *stage), ffn_off, b_two, b_up_mine, up_pieces)
    stage = [act]
    if by_permute:
        stage = stage + [x1d, z12d, x2d]
        x3d = dp_swap(tie(z12d, *stage), 2)
    *down_grad, grad_b_down = weight_grad(
        tie(experts_two, *stage), slots, 0, cots, act, ffn_chunk, n_out, e_count, items
    )
    stage = [grad_b_down]
    if by_permute:
        down_pieces = [down_own, z4d, z8d, z12d, x0d, x1d, x2d, x3d]

        def near(parts, core_slot, *others):
            return dp_swap(tie(parts[2 * core_slot + 1], *others), 2)

        def middle(parts, core_slot, got, *others):
            keep, got = tie(parts[2 * core_slot], got, *others), tie(got, *others)
            both = keep[2:4].astype(F32) + got[2:4].astype(F32)
            return keep, got, both.astype(BF)

        def last(state, mid, *others):
            keep, got, _ = state
            mid = tie(mid, *others)
            part = keep[1].astype(F32) + got[1].astype(F32) + mid[1].astype(F32)
            return keep, got, mid, part.astype(BF)

        def total(state, end, *others, planes=slice(None)):
            keep, got, mid, _ = state
            end = tie(end, *others)
            return (
                keep[0, planes].astype(F32)
                + got[0, planes].astype(F32)
                + mid[0, planes].astype(F32)
                + end[planes].astype(F32)
            )

        stage = stage + [x3d]
        dn1 = near(down_grad, 1, *stage)
    db_own, db_other, du, grad_b_up = experts_back(
        tie(experts_two, *stage), ffn_off, cots, slope, up_pieces, down_pieces, items
    )
    stage = [du]
    if by_permute:
        d1 = middle(down_grad, 1, dn1, du)
        stage = [d1[2]]
    db = add_low(db_own, partner(tie(db_other, *stage)))
    stage = stage + [db]
    if by_permute:
        df1 = dp_swap(tie(d1[2], *stage), 4)
        dn0 = near(down_grad, 0, *stage)
    db_theirs = peer(tie(db, *stage))
    *up_grad, _ = weight_grad(
        tie(experts_two, *stage), slots, 0, b_two, du, ffn_chunk, n_out, e_count, 0
    )
    stage = [up_grad[0]]
    if by_permute:
        stage = stage + [df1]
        un1 = near(up_grad, 1, *stage)
        d1 = last(d1, df1, *stage)
        dg1 = dp_swap(d1[3], 8)
    z_own, z_other = experts_down(
        tie(experts_two, *stage), ffn_off, act, down_pieces, rows, items
    )
    stage = [z_own, db_theirs]
    if by_permute:
        d0 = middle(down_grad, 0, dn0, *stage)
        stage = stage + [d0[2], dg1]
    z = add_low(z_own, partner(tie(z_other, *stage)))
    stage = stage + [z]
    z_theirs = peer(tie(z, *stage))
    if by_permute:
        df0 = dp_swap(tie(d0[2], *stage), 4)
        un0 = near(up_grad, 0, *stage)

    dh, da, norm_one, norm_two, bias_sums, *attn_parts = attend_back(
        tie(text_len, *stage), slots, db, db_theirs, h, cots[0], tok, a, ctx, qkv, attn_w, out_w, vectors,
        attn_chunk, n_out, scale,
    )
    stage = [bias_sums, z_theirs]
    if by_permute:
        u1 = middle(up_grad, 1, un1, *stage)
        stage = stage + [u1[2], df0]
        uf1 = dp_swap(tie(u1[2], *stage), 4)
        d0 = last(d0, df0, *stage)
        dg0 = dp_swap(d0[3], 8)
    da_theirs = peer(tie(da, bias_sums, z_theirs))
    norm_one_theirs = peer(tie(norm_one, *stage))
    attn_parts = [tie(v, *stage) for v in attn_parts]

    up_pair = jnp.zeros((2, e_count, hidden), F32)
    up_pair = lax.dynamic_update_slice_in_dim(up_pair, grad_b_up[None], core, 0)
    small = jnp.concatenate(
        [
            norm_one + norm_one_theirs,
            norm_two,
            grad_b_down,
            up_pair.reshape(-1, width),
            bias_sums.reshape(-1, width),
        ]
    )
    steps = list(masks)

    def add_step(*others):
        nonlocal small
        small = tie(small, *others)
        got = swap(small, "dp", dp, steps.pop(0))
        small = small + got
        return got

    stage = [norm_one_theirs]
    if by_permute:
        u0 = middle(up_grad, 0, un0, *stage)
        stage = stage + [u0[2]]
        send = add_low(tie(attn_parts[1], *stage), partner(attn_parts[3]))
        keep = add_low(tie(attn_parts[0], *stage), partner(attn_parts[2]))
        an = near([keep, send], 0, *stage)
        uf0 = dp_swap(tie(u0[2], *stage), 4)
        stage = stage + [keep, send]
    got = add_step(*stage)
    output = finish_output(tie(experts, *stage), h, z, z_theirs, b_down, seq)
    stage = [output, got]
    if by_permute:
        stage = stage + [uf1, dg0]
        u1 = last(u1, uf1, *stage)
        ug1 = dp_swap(u1[3], 8)
        stage = [u1[3], got]
        got = add_step(*stage)
        down_other = total(d1, dg1, *stage)
        down_got = partner(down_other)
        u0 = last(u0, uf0, *stage)
        ug0 = dp_swap(u0[3], 8)
        stage = [u0[3], down_other, da_theirs]
        a0 = middle([keep, send], 0, an, *stage)
        stage = stage + [a0[2]]
        af = dp_swap(tie(a0[2], *stage), 4)
        down_mine = total(d0, dg0, *stage)
        stage = stage + [down_mine]
    else:
        got = add_step(*stage)
    stage = [got, *stage]
    grad_tokens = token_grad(dh, da, da_theirs, tok, tie(vectors, *stage), seq)
    stage = [grad_tokens]
    got = add_step(*stage)
    if by_permute:
        up_other = total(u1, ug1, *stage)
        up_got = partner(up_other)
        a0 = last(a0, af, up_other, *stage)
        stage = stage + [a0[3], got]
        got = add_step(*stage)

    if by_permute:

        def joined(own, got):
            whole = jnp.zeros((e_count, share, 2 * hidden), F32)
            whole = lax.dynamic_update_slice_in_dim(whole, got, (1 - core) * hidden, 2)
            return lax.dynamic_update_slice_in_dim(whole, own, core * hidden, 2)

        ag = dp_swap(a0[3], 8)
        grad_w_down = joined(tie(down_mine, a0[3]), down_got)
        grad_w_up = joined(total(u0, ug0, a0[3]), up_got)
        ag = tie(ag, grad_w_up)
        grad_w_qkv = total(a0, ag, planes=slice(0, 3))
        grad_w_out = total(a0, ag, planes=3)
    else:

        def finish(chunk):
            whole = jnp.zeros((e_count, width, 2 * hidden), BF)
            whole = lax.dynamic_update_slice_in_dim(whole, chunk[0], core * hidden, 2)
            return lax.psum_scatter(whole, "dp", scatter_dimension=1, tiled=True).astype(F32)

        grad_w_down, grad_w_up = finish(down_grad[0]), finish(up_grad[0])
        grad_attn = lax.psum_scatter(attn_parts[0][0], "dp", scatter_dimension=1, tiled=True)
        grad_w_qkv, grad_w_out = grad_attn[:3].astype(F32), grad_attn[3].astype(F32)

    while steps:
        add_step()
    at = 5 + e_count
    end = at + e_count * hidden // width
    total_up = jnp.concatenate(
        [small[n : n + end - at].reshape(e_count, hidden) for n in (at, end)], axis=1
    )
    total_qv = small[2 * end - at :].reshape(2, cols)
    return (
        output,
        grad_tokens,
        grad_w_qkv,
        grad_w_out,
        grad_w_up,
        grad_w_down,
        total_qv,
        small[4],
        total_up,
        small[5:at],
        small[:4],
    )


def solution(mesh):
    body = functools.partial(per_device, dp=mesh.shape["dp"], rep=mesh.shape["rep"])
    return jax.shard_map(
        body,
        mesh=mesh,
        in_specs=(
            P("dp", None, None),
            P("dp"),
            P("dp", None),
            P(),
            P(),
            P(None, "dp", "rep"),
            P(None, "rep"),
            P("dp", "rep"),
            P(),
            P(),
            P(),
            P(None, "dp", "rep"),
            P(None, "rep"),
            P(None, "dp", "rep"),
            P(),
            P("dp", None, None),
        ),
        out_specs=(
            P("dp", None, None),
            P("dp", None, None),
            P(None, "dp", "rep"),
            P("dp", "rep"),
            P(None, "dp", "rep"),
            P(None, "dp", "rep"),
            P(None, "rep"),
            P(),
            P(None, "rep"),
            P(),
            P(),
        ),
        check_vma=False,
    )
```

```python
import functools
import math

import jax
import jax.numpy as jnp
from jax import lax
from jax.experimental import pallas as pl
from jax.experimental.pallas import tpu as pltpu
from jax.sharding import PartitionSpec as P

HDIM = 64
IMG = 197
EPSILON = 1e-05
ROOT_HALF = 0.7071067811865476
INV_ROOT_TAU = 0.3989422804014327
SUB = 16
LANES = 128
BF = jnp.bfloat16
F32 = jnp.float32

NN = (((1,), (0,)), ((), ()))
NT = (((1,), (1,)), ((), ()))
TN = (((0,), (0,)), ((), ()))


def up_to(n, m):
    return -(-n // m) * m


def dot(a, b, dims):
    return lax.dot_general(a, b, dims, preferred_element_type=F32)


def full(shape):
    zeros = (0,) * len(shape)
    return pl.BlockSpec(shape, lambda *_: zeros)


def per_item(shape):
    zeros = (0,) * (len(shape) - 1)
    return pl.BlockSpec(shape, lambda i, *_: (i,) + zeros)


ANY = pl.BlockSpec(memory_space=pl.ANY)


def params():
    return pltpu.CompilerParams(vmem_limit_bytes=60 * 1024 * 1024)


SHORT = pl.CostEstimate(flops=1, transcendentals=0, bytes_accessed=1)


def normed(v):
    centred = v - jnp.mean(v, axis=-1, keepdims=True)
    var = jnp.mean(centred * centred, axis=-1, keepdims=True)
    spread = lax.rsqrt(var + EPSILON)
    return centred * spread, spread


def norm_back(grad, hat, spread, gain):
    scaled = grad * gain
    return spread * (
        scaled
        - jnp.mean(scaled, axis=-1, keepdims=True)
        - hat * jnp.mean(scaled * hat, axis=-1, keepdims=True)
    )


def run_copies(copies, *, start=False, wait=False):
    for c in copies:
        if start:
            c.start()
        if wait:
            c.wait()


def place_copies(off_ref, pieces, dest, sems, plane=0):
    copies = []
    for n, piece in enumerate(pieces):
        subs, _, rows, _ = piece.shape
        for j in range(subs):
            at = off_ref[n * subs + j]
            copies.append(
                pltpu.make_async_copy(
                    piece.at[j, plane : plane + dest.shape[0]],
                    dest.at[:, pl.ds(pl.multiple_of(at, SUB), rows), :],
                    sems.at[n * subs + j],
                )
            )
    return copies


def k_proj(off_ref, tok_ref, vec_ref, bias_ref, *rest):
    a_ref, qkv_ref, w_ref, wo_ref, sems, out_sems = rest[-6:]
    pieces = rest[:-6]
    first = pl.program_id(0) == 0

    @pl.when(first)
    def _():
        run_copies(place_copies(off_ref, pieces, w_ref, sems), start=True)
        run_copies(place_copies(off_ref, pieces, wo_ref, out_sems, 3), start=True)

    hat, _ = normed(tok_ref[0].astype(F32))
    a_ref[0] = (hat * vec_ref[0:1, :] + vec_ref[1:2, :]).astype(BF)

    @pl.when(first)
    def _():
        run_copies(place_copies(off_ref, pieces, w_ref, sems), wait=True)
        run_copies(place_copies(off_ref, pieces, wo_ref, out_sems, 3), wait=True)

    a = a_ref[0]
    for t in range(3):
        qkv_ref[t, 0] = (dot(a, w_ref[t], NN) + bias_ref[t : t + 1, :]).astype(BF)


def project(tokens, vectors, bias, pieces, offsets):
    items, rows, width = tokens.shape
    cols = pieces[0].shape[3]
    count = len(pieces) * pieces[0].shape[0]
    grid_spec = pltpu.PrefetchScalarGridSpec(
        num_scalar_prefetch=1,
        grid=(items,),
        in_specs=[
            per_item((1, rows, width)),
            full(vectors.shape),
            full((3, cols)),
        ]
        + [ANY] * len(pieces),
        out_specs=[
            per_item((1, rows, width)),
            pl.BlockSpec((3, 1, rows, cols), lambda i, *_: (0, i, 0, 0)),
            full((3, width, cols)),
            full((1, width, cols)),
        ],
        scratch_shapes=[pltpu.SemaphoreType.DMA((count,)), pltpu.SemaphoreType.DMA((count,))],
    )
    return pl.pallas_call(
        k_proj,
        grid_spec=grid_spec,
        out_shape=[
            jax.ShapeDtypeStruct((items, rows, width), BF),
            jax.ShapeDtypeStruct((3, items, rows, cols), BF),
            jax.ShapeDtypeStruct((3, width, cols), BF),
            jax.ShapeDtypeStruct((1, width, cols), BF),
        ],
        compiler_params=params(),
        cost_estimate=SHORT,
        name="project",
    )(offsets, tokens, vectors, bias, *pieces)


def k_attend(len_ref, q_ref, k_ref, v_ref, c_ref, *, scale):
    rows, width = c_ref.shape[1:]
    length = len_ref[pl.program_id(0)]
    valid = lax.broadcasted_iota(jnp.int32, (1, rows), 1) < IMG + length
    low = lax.broadcasted_iota(jnp.int32, (1, LANES), 1) < HDIM
    for pair in range(width // LANES):
        cols = slice(pair * LANES, (pair + 1) * LANES)
        q, k, v = q_ref[0, 0, :, cols], k_ref[0, 0, :, cols], v_ref[0, 0, :, cols]
        both = []
        for side in (low, ~low):
            s = dot(q * side.astype(BF), k, NT) * scale
            s = jnp.where(valid, s, -1e30)
            e = jnp.exp(s - jnp.max(s, axis=-1, keepdims=True))
            p = (e / jnp.sum(e, axis=-1, keepdims=True)).astype(BF)
            both.append(dot(p, v, NN))
        c_ref[0, :, cols] = jnp.where(low, both[0], both[1]).astype(BF)


def qkv_specs(rows, cols):
    return [pl.BlockSpec((1, 1, rows, cols), lambda i, *_, t=t: (t, i, 0, 0)) for t in range(3)]


def attend(text_len, qkv, scale):
    _, items, rows, cols = qkv.shape
    grid_spec = pltpu.PrefetchScalarGridSpec(
        num_scalar_prefetch=1,
        grid=(items,),
        in_specs=qkv_specs(rows, cols),
        out_specs=per_item((1, rows, cols)),
    )
    return pl.pallas_call(
        functools.partial(k_attend, scale=scale),
        grid_spec=grid_spec,
        out_shape=jax.ShapeDtypeStruct((items, rows, cols), BF),
        compiler_params=params(),
        cost_estimate=SHORT,
        name="attend",
    )(text_len, qkv, qkv, qkv)


def k_residual(tok_ref, cm_ref, cp_ref, wm_ref, wp_ref, vec_ref, h_ref, b_ref):
    y = dot(cm_ref[0], wm_ref[0], NT) + dot(cp_ref[0], wp_ref[0], NT)
    h = tok_ref[0].astype(F32) + (y + vec_ref[2:3, :])
    h_ref[0] = h
    hat, _ = normed(h)
    b_ref[0] = (hat * vec_ref[3:4, :] + vec_ref[4:5, :]).astype(BF)


def residual(tokens, mine, theirs, w_mine, w_theirs, vectors):
    items, rows, width = tokens.shape
    cols = mine.shape[2]
    return pl.pallas_call(
        k_residual,
        grid=(items,),
        in_specs=[
            per_item((1, rows, width)),
            per_item((1, rows, cols)),
            per_item((1, rows, cols)),
            full((1, width, cols)),
            full((1, width, cols)),
            full(vectors.shape),
        ],
        out_specs=[per_item((1, rows, width))] * 2,
        out_shape=[
            jax.ShapeDtypeStruct(tokens.shape, F32),
            jax.ShapeDtypeStruct(tokens.shape, BF),
        ],
        compiler_params=params(),
        cost_estimate=SHORT,
        name="residual",
    )(tokens, mine, theirs, w_mine, w_theirs, vectors)


def segments(rows):
    head = up_to(IMG, SUB)
    tail = IMG // SUB * SUB
    return (0, head), (tail, rows - tail), head


def segment_masks(rows):
    (a0, an), (b0, bn), _ = segments(rows)
    in_a = lax.broadcasted_iota(jnp.int32, (an, 1), 0) + a0 < IMG
    in_b = lax.broadcasted_iota(jnp.int32, (bn, 1), 0) + b0 >= IMG
    return in_a, in_b


def masked_parts(g_ref, i):
    rows = g_ref.shape[1]
    (a0, an), (b0, bn), _ = segments(rows)
    in_a, in_b = segment_masks(rows)
    g_a = jnp.where(in_a, g_ref[i, a0 : a0 + an, :].astype(F32), 0.0)
    g_b = jnp.where(in_b, g_ref[i, b0 : b0 + bn, :].astype(F32), 0.0)
    return g_a, g_b


def item_copies(refs, dest, sems):
    copies = []
    for ref in refs:
        if len(ref.shape) == 2:
            copies.append(
                pltpu.make_async_copy(ref, dest.at[len(copies)], sems.at[len(copies)])
            )
        else:
            for j in range(ref.shape[0]):
                copies.append(
                    pltpu.make_async_copy(ref.at[j], dest.at[len(copies)], sems.at[len(copies)])
                )
    return copies


def wait_item(copies, i):
    for n, c in enumerate(copies):

        @pl.when(i == n)
        def _(c=c):
            c.wait()


def write_chunks(slot_ref, base, acc, stage, outs, sems):
    count, _, rows, _ = stage.shape
    for c in range(count):
        stage[slot_ref[base + c]] = acc[:, c * rows : (c + 1) * rows, :].astype(BF)
    per = count // len(outs)
    copies = [
        pltpu.make_async_copy(stage.at[n * per : (n + 1) * per], out, sems.at[n])
        for n, out in enumerate(outs)
    ]
    run_copies(copies, start=True)
    run_copies(copies, wait=True)


def k_up(e_ref, off_ref, bias_ref, *rest, n_left):
    b_refs, pieces = rest[:n_left], rest[n_left:-6]
    act_ref, slope_ref, b_s, w_s, b_sem, w_sem = rest[-6:]
    i = pl.program_id(0)
    b_copies = item_copies(b_refs, b_s, b_sem)

    @pl.when(i == 0)
    def _():
        run_copies(b_copies[:1], start=True)
        w_copies = place_copies(off_ref, pieces, w_s, w_sem)
        run_copies(w_copies, start=True)
        run_copies(b_copies[1:], start=True)
        run_copies(w_copies, wait=True)

    wait_item(b_copies, i)
    seg_a, seg_b, _ = segments(b_s.shape[1])
    at = 0
    for which, (lo, n) in zip((0, 1), (seg_a, seg_b)):
        e = e_ref[which, i]
        u = dot(b_s[i, lo : lo + n, :], w_s[e], NN) + bias_ref[pl.ds(e, 1), :]
        cdf = 0.5 * (1.0 + lax.erf(u * ROOT_HALF))
        act_ref[0, at : at + n, :] = (u * cdf).astype(BF)
        slope_ref[0, at : at + n, :] = (cdf + u * jnp.exp(-0.5 * u * u) * INV_ROOT_TAU).astype(BF)
        at += n


def experts_up(experts, offsets, b, bias, pieces):
    items = experts.shape[1]
    rows, width = b[0].shape[-2:]
    e_count, _, hidden = pieces[0].shape[1:]
    count = len(pieces) * pieces[0].shape[0]
    (_, an), (_, bn), _ = segments(rows)
    grid_spec = pltpu.PrefetchScalarGridSpec(
        num_scalar_prefetch=2,
        grid=(items,),
        in_specs=[full((e_count, hidden))] + [ANY] * (len(b) + len(pieces)),
        out_specs=[per_item((1, an + bn, hidden))] * 2,
        scratch_shapes=[
            pltpu.VMEM((items, rows, width), BF),
            pltpu.VMEM((e_count, width, hidden), BF),
            pltpu.SemaphoreType.DMA((items,)),
            pltpu.SemaphoreType.DMA((count,)),
        ],
    )
    return pl.pallas_call(
        functools.partial(k_up, n_left=len(b)),
        grid_spec=grid_spec,
        out_shape=[jax.ShapeDtypeStruct((items, an + bn, hidden), BF)] * 2,
        compiler_params=params(),
        cost_estimate=SHORT,
        name="experts_up",
    )(experts, offsets, bias, *b, *pieces)


def k_weight_grad(e_ref, slot_ref, right_ref, *rest, n_left, n_out, base, own):
    lefts = rest[:n_left]
    outs = rest[n_left : n_left + n_out]
    left_s, dw_s, stage, left_sem, out_sem = rest[-5:]
    sums_ref = rest[n_left + n_out]
    i = pl.program_id(0)
    copies = item_copies(lefts, left_s, left_sem)

    @pl.when(i == 0)
    def _():
        run_copies(copies, start=True)
        dw_s[...] = jnp.zeros_like(dw_s)
        sums_ref[...] = jnp.zeros_like(sums_ref)

    wait_item(copies, i)
    at = 0
    for which, left in zip((0, 1), masked_parts(left_s, i)):
        e = e_ref[which, i]
        n = left.shape[0]
        dw_s[e] += dot(left.astype(BF), right_ref[0, at : at + n, :], TN)

        @pl.when(i < own)
        def _(left=left, e=e):
            sums_ref[pl.ds(e, 1), :] += jnp.sum(left, axis=0, keepdims=True)

        at += n

    @pl.when(i == pl.num_programs(0) - 1)
    def _():
        write_chunks(slot_ref, base, dw_s, stage, outs, out_sem)


def weight_grad(experts, slots, base, left, right, chunk, n_out, e_count, own):
    items, seg_rows, hidden = right.shape
    rows, width = left[0].shape[-2:]
    count = chunk[0] * n_out
    grid_spec = pltpu.PrefetchScalarGridSpec(
        num_scalar_prefetch=2,
        grid=(items,),
        in_specs=[per_item((1, seg_rows, hidden))] + [ANY] * len(left),
        out_specs=[ANY] * n_out + [full((e_count, width))],
        scratch_shapes=[
            pltpu.VMEM((items, rows, width), BF),
            pltpu.VMEM((e_count, width, hidden), F32),
            pltpu.VMEM((count,) + chunk[1:], BF),
            pltpu.SemaphoreType.DMA((items,)),
            pltpu.SemaphoreType.DMA((n_out,)),
        ],
    )
    return pl.pallas_call(
        functools.partial(
            k_weight_grad, n_left=len(left), n_out=n_out, base=base, own=own
        ),
        grid_spec=grid_spec,
        out_shape=[jax.ShapeDtypeStruct(chunk, BF)] * n_out
        + [jax.ShapeDtypeStruct((e_count, width), F32)],
        compiler_params=params(),
        cost_estimate=SHORT,
        name="weight_grad",
    )(experts, slots, right, *left)


def store_joined(ref, first, middle, second, tail, head):
    ref[0, :tail, :] = first[:tail].astype(BF)
    ref[0, tail:head, :] = middle.astype(BF)
    ref[0, head:, :] = second[head - tail :].astype(BF)


def k_back(e_ref, off_ref, slope_ref, *rest, n_left, n_up, own):
    g_s, w_up, w_down, sem_g, sem_up, sem_down = rest[-6:]
    do_ref, dp_ref, du_ref, gbu_ref = rest[-10:-6]
    lefts, ups, downs = rest[:n_left], rest[n_left : n_left + n_up], rest[n_left + n_up : -10]
    i = pl.program_id(0)
    copies = item_copies(lefts, g_s, sem_g)

    @pl.when(i == 0)
    def _():
        w_copies = place_copies(off_ref, downs, w_down, sem_down)
        run_copies(copies[:1] + w_copies, start=True)
        more = place_copies(off_ref, ups, w_up, sem_up)
        run_copies(more + copies[1:], start=True)
        gbu_ref[...] = jnp.zeros_like(gbu_ref)
        run_copies(w_copies + more, wait=True)

    wait_item(copies, i)
    rows = g_s.shape[1]
    seg_a, seg_b, head = segments(rows)
    tail = seg_b[0]
    at = 0
    both = []
    for which, g in zip((0, 1), masked_parts(g_s, i)):
        e = e_ref[which, i]
        n = g.shape[0]
        dact = dot(g.astype(BF), w_down[e], NN)
        du = (dact * slope_ref[0, at : at + n, :].astype(F32)).astype(BF)
        du_ref[0, at : at + n, :] = du
        gbu_ref[pl.ds(e, 1), :] += jnp.sum(du.astype(F32), axis=0, keepdims=True)
        both.append(dot(du, w_up[e], NT))
        at += n
    middle = both[0][tail:] + both[1][: head - tail]
    for cond, db_ref in ((i < own, do_ref), (i >= own, dp_ref)):

        @pl.when(cond)
        def _(db_ref=db_ref):
            store_joined(db_ref, both[0], middle, both[1], tail, head)


def own_and_other(rows, width, own):
    block = (1, rows, width)
    return [
        pl.BlockSpec(block, lambda i, *_: (jnp.minimum(i, own - 1), 0, 0)),
        pl.BlockSpec(block, lambda i, *_: (jnp.maximum(i - own, 0), 0, 0)),
    ]


def experts_back(experts, offsets, left, slope, ups, downs, own):
    rows, width = left[0].shape[-2:]
    e_count, _, hidden = ups[0].shape[1:]
    count = len(ups) * ups[0].shape[0]
    items, seg_rows, _ = slope.shape
    grid_spec = pltpu.PrefetchScalarGridSpec(
        num_scalar_prefetch=2,
        grid=(items,),
        in_specs=[per_item((1, seg_rows, hidden))]
        + [ANY] * (len(left) + len(ups) + len(downs)),
        out_specs=own_and_other(rows, width, own)
        + [per_item((1, seg_rows, hidden)), full((e_count, hidden))],
        scratch_shapes=[
            pltpu.VMEM((items, rows, width), BF),
            pltpu.VMEM((e_count, width, hidden), BF),
            pltpu.VMEM((e_count, width, hidden), BF),
            pltpu.SemaphoreType.DMA((items,)),
            pltpu.SemaphoreType.DMA((count,)),
            pltpu.SemaphoreType.DMA((count,)),
        ],
    )
    return pl.pallas_call(
        functools.partial(k_back, n_left=len(left), n_up=len(ups), own=own),
        grid_spec=grid_spec,
        out_shape=[
            jax.ShapeDtypeStruct((own, rows, width), BF),
            jax.ShapeDtypeStruct((items - own, rows, width), BF),
            jax.ShapeDtypeStruct((items, seg_rows, hidden), BF),
            jax.ShapeDtypeStruct((e_count, hidden), F32),
        ],
        compiler_params=params(),
        cost_estimate=SHORT,
        name="experts_back",
    )(experts, offsets, slope, *left, *ups, *downs)


def k_down(e_ref, off_ref, act_ref, *rest, own):
    zo_ref, zp_ref, w_down, sems = rest[-4:]
    pieces = rest[:-4]
    i = pl.program_id(0)

    @pl.when(i == 0)
    def _():
        copies = place_copies(off_ref, pieces, w_down, sems)
        run_copies(copies, start=True)
        run_copies(copies, wait=True)

    rows = zo_ref.shape[1]
    seg_a, seg_b, head = segments(rows)
    tail = seg_b[0]
    z_a = dot(act_ref[0, : seg_a[1], :], w_down[e_ref[0, i]], NT)
    z_b = dot(act_ref[0, seg_a[1] :, :], w_down[e_ref[1, i]], NT)
    image = lax.broadcasted_iota(jnp.int32, (head - tail, 1), 0) + tail < IMG
    middle = jnp.where(image, z_a[tail:], z_b[: head - tail])
    for cond, z_ref in ((i < own, zo_ref), (i >= own, zp_ref)):

        @pl.when(cond)
        def _(z_ref=z_ref):
            store_joined(z_ref, z_a, middle, z_b, tail, head)


def experts_down(experts, offsets, act, pieces, rows, own):
    items, seg_rows, hidden = act.shape
    e_count = pieces[0].shape[1]
    width = sum(p.shape[0] * p.shape[2] for p in pieces)
    count = len(pieces) * pieces[0].shape[0]
    grid_spec = pltpu.PrefetchScalarGridSpec(
        num_scalar_prefetch=2,
        grid=(items,),
        in_specs=[per_item((1, seg_rows, hidden))] + [ANY] * len(pieces),
        out_specs=own_and_other(rows, width, own),
        scratch_shapes=[
            pltpu.VMEM((e_count, width, hidden), BF),
            pltpu.SemaphoreType.DMA((count,)),
        ],
    )
    return pl.pallas_call(
        functools.partial(k_down, own=own),
        grid_spec=grid_spec,
        out_shape=[
            jax.ShapeDtypeStruct((own, rows, width), BF),
            jax.ShapeDtypeStruct((items - own, rows, width), BF),
        ],
        compiler_params=params(),
        cost_estimate=SHORT,
        name="experts_down",
    )(experts, offsets, act, *pieces)


def k_output(e_ref, h_ref, zm_ref, zp_ref, bias_ref, o_ref):
    i = pl.program_id(0)
    rows, keep = h_ref.shape[1], o_ref.shape[1]
    image = lax.broadcasted_iota(jnp.int32, (rows, 1), 0) < IMG
    bias = jnp.where(image, bias_ref[pl.ds(e_ref[0, i], 1), :], bias_ref[pl.ds(e_ref[1, i], 1), :])
    out = h_ref[0] + ((zm_ref[0].astype(F32) + zp_ref[0].astype(F32)) + bias)
    o_ref[0] = out[:keep].astype(BF)


def finish_output(experts, h, mine, theirs, bias, keep):
    items, rows, width = h.shape
    grid_spec = pltpu.PrefetchScalarGridSpec(
        num_scalar_prefetch=1,
        grid=(items,),
        in_specs=[per_item((1, rows, width))] * 3 + [full(bias.shape)],
        out_specs=per_item((1, keep, width)),
    )
    return pl.pallas_call(
        k_output,
        grid_spec=grid_spec,
        out_shape=jax.ShapeDtypeStruct((items, keep, width), BF),
        compiler_params=params(),
        cost_estimate=SHORT,
        name="finish_output",
    )(experts, h, mine, theirs, bias)


def k_attend_back(
    len_ref, slot_ref, dm_ref, dp_ref, h_ref, g_ref, tok_ref, a_ref, c_ref, q_ref, k_ref, v_ref,
    w_ref, wo_ref, vec_ref, dh_ref, da_ref, one_ref, two_ref, bias_ref, *rest, scale,
):
    dqkv, acc, stage, sems = rest[-4:]
    outs = rest[:-4]
    rows, width = dh_ref.shape[1:]
    cols = q_ref.shape[3]
    i = pl.program_id(0)

    @pl.when(i == 0)
    def _():
        one_ref[...] = jnp.zeros_like(one_ref)
        two_ref[...] = jnp.zeros_like(two_ref)
        bias_ref[...] = jnp.zeros_like(bias_ref)
        acc[...] = jnp.zeros_like(acc)

    def add_rows(ref, at, value):
        ref[at : at + 1, :] += jnp.sum(value, axis=0, keepdims=True)

    db = dm_ref[0].astype(F32) + dp_ref[0].astype(F32)
    hat, spread = normed(h_ref[0])
    dh = g_ref[0].astype(F32) + norm_back(db, hat, spread, vec_ref[3:4, :])
    dh_ref[0] = dh
    dy = dh.astype(BF)
    add_rows(two_ref, 0, db * hat)
    add_rows(two_ref, 1, db)
    add_rows(two_ref, 2, dy.astype(F32))
    dctx = dot(dy, wo_ref[0], NN).astype(BF)
    valid = lax.broadcasted_iota(jnp.int32, (rows, 1), 0) < IMG + len_ref[i]
    low = lax.broadcasted_iota(jnp.int32, (1, LANES), 1) < HDIM
    for pair in range(cols // LANES):
        at = slice(pair * LANES, (pair + 1) * LANES)
        q, k, v = q_ref[0, 0, :, at], k_ref[0, 0, :, at], v_ref[0, 0, :, at]
        dc = dctx[:, at]
        parts = []
        for side in (low, ~low):
            only = side.astype(BF)
            s = dot(k * only, q, NT) * scale
            s = jnp.where(valid, s, -1e30)
            e = jnp.exp(s - jnp.max(s, axis=0, keepdims=True))
            p = e / jnp.sum(e, axis=0, keepdims=True)
            dp = dot(v * only, dc, NT)
            ds = (p * (dp - jnp.sum(p * dp, axis=0, keepdims=True))).astype(BF)
            parts.append((dot(ds, k, TN), dot(ds, q, NN), dot(p.astype(BF), dc, NN)))
        dqkv[0, :, at] = (jnp.where(low, parts[0][0], parts[1][0]) * scale).astype(BF)
        dqkv[1, :, at] = (jnp.where(low, parts[0][1], parts[1][1]) * scale).astype(BF)
        dqkv[2, :, at] = jnp.where(low, parts[0][2], parts[1][2]).astype(BF)
    da = dot(dqkv[0], w_ref[0], NT)
    da += dot(dqkv[1], w_ref[1], NT)
    da += dot(dqkv[2], w_ref[2], NT)
    add_rows(bias_ref, 0, dqkv[0].astype(F32))
    add_rows(bias_ref, 1, dqkv[2].astype(F32))
    hat, _ = normed(tok_ref[0].astype(F32))
    add_rows(one_ref, 0, da * hat)
    add_rows(one_ref, 1, da)
    da_ref[0] = da.astype(BF)
    for t in range(3):
        acc[t] += dot(a_ref[0], dqkv[t], TN)
    acc[3] += dot(dy, c_ref[0], TN)

    @pl.when(i == pl.num_programs(0) - 1)
    def _():
        write_chunks(slot_ref, 0, acc, stage, outs, sems)


def attend_back(
    text_len, slots, mine, theirs, h, g, tokens, a, ctx, qkv, weights, w_out, vectors, chunk, n_out, scale
):
    items, rows, width = h.shape
    cols = qkv.shape[3]
    block = per_item((1, rows, width))
    grid_spec = pltpu.PrefetchScalarGridSpec(
        num_scalar_prefetch=2,
        grid=(items,),
        in_specs=[block] * 6
        + [per_item((1, rows, cols))]
        + qkv_specs(rows, cols)
        + [full(weights.shape), full(w_out.shape), full(vectors.shape)],
        out_specs=[block, block, full((2, width)), full((3, width)), full((2, cols))]
        + [ANY] * n_out,
        scratch_shapes=[
            pltpu.VMEM((3, rows, cols), BF),
            pltpu.VMEM((4, width, cols), F32),
            pltpu.VMEM((chunk[0] * n_out,) + chunk[1:], BF),
            pltpu.SemaphoreType.DMA((n_out,)),
        ],
    )
    return pl.pallas_call(
        functools.partial(k_attend_back, scale=scale),
        grid_spec=grid_spec,
        out_shape=[
            jax.ShapeDtypeStruct((items, rows, width), F32),
            jax.ShapeDtypeStruct((items, rows, width), BF),
            jax.ShapeDtypeStruct((2, width), F32),
            jax.ShapeDtypeStruct((3, width), F32),
            jax.ShapeDtypeStruct((2, cols), F32),
        ]
        + [jax.ShapeDtypeStruct(chunk, BF)] * n_out,
        compiler_params=params(),
        cost_estimate=SHORT,
        name="attend_back",
    )(text_len, slots, mine, theirs, h, g, tokens, a, ctx, qkv, qkv, qkv, weights, w_out, vectors)


def k_token_grad(dh_ref, dm_ref, dp_ref, tok_ref, vec_ref, o_ref):
    keep = o_ref.shape[1]
    da = dm_ref[0].astype(F32) + dp_ref[0].astype(F32)
    hat, spread = normed(tok_ref[0].astype(F32))
    out = dh_ref[0] + norm_back(da, hat, spread, vec_ref[0:1, :])
    o_ref[0] = out[:keep]


def token_grad(dh, mine, theirs, tokens, vectors, keep):
    items, rows, width = dh.shape
    return pl.pallas_call(
        k_token_grad,
        grid=(items,),
        in_specs=[per_item((1, rows, width))] * 4 + [full(vectors.shape)],
        out_specs=per_item((1, keep, width)),
        out_shape=jax.ShapeDtypeStruct((items, keep, width), F32),
        compiler_params=params(),
        cost_estimate=SHORT,
        name="token_grad",
    )(dh, mine, theirs, tokens, vectors)


def swap(value, axis, size, mask):
    return lax.ppermute(value, axis, [(i, i ^ mask) for i in range(size)])


def tie(value, *others):
    return lax.optimization_barrier((value,) + others)[0]


def add_low(a, b):
    return (a.astype(F32) + b.astype(F32)).astype(BF)


def per_device(
    tokens, text_len, routes, attn_gain, attn_shift, w_qkv, b_qv, w_out, b_out, ffn_gain, ffn_shift,
    w_up, b_up, w_down, b_down, cotangent, *, dp, rep,
):
    items, seq, width = tokens.shape
    rows = up_to(seq, SUB)
    share = w_qkv.shape[1]
    cols = w_qkv.shape[2]
    hidden = w_up.shape[2] // 2
    e_count = w_up.shape[0]
    scale = 1.0 / math.sqrt(HDIM)
    me = lax.axis_index("dp")
    core = me % 2
    by_permute = dp == 16 and share % SUB == 0
    masks = [m for m in (1, 128, 64, 32, 16, 8, 4, 2) if m < dp]

    def peer(value):
        return lax.ppermute(value, "rep", [(i, i ^ 1) for i in range(rep)])

    def partner(value):
        return swap(value, "dp", dp, 1)

    def dp_swap(value, mask):
        return swap(value, "dp", dp, mask)

    def halves(w):
        mine = lax.dynamic_slice_in_dim(w, core * hidden, hidden, 2)
        other = lax.dynamic_slice_in_dim(w, (1 - core) * hidden, hidden, 2)
        return mine, other

    attn_shard = jnp.concatenate([w_qkv, w_out[None]], axis=0)
    vectors = jnp.stack([attn_gain, attn_shift, b_out, ffn_gain, ffn_shift])
    pad = ((0, 0), (0, rows - seq), (0, 0))
    tok = jnp.pad(tokens, pad)
    bias = jnp.stack([b_qv[0], jnp.zeros_like(b_qv[0]), b_qv[1]])
    experts = jnp.stack([routes[:, 0], routes[:, seq - 1]]).astype(jnp.int32)
    b_up_mine = lax.dynamic_slice_in_dim(b_up, core * hidden, hidden, 1)
    cot_partner = partner(cotangent)
    tok_tied = tie(tok, cot_partner)

    if by_permute:
        here = me.astype(jnp.int32)
        own_attn = attn_shard[None]
        z8a, z4a = dp_swap(own_attn, 8), dp_swap(own_attn, 4)
        za = [own_attn, z4a, z8a, dp_swap(z8a, 4)]
        xa = [dp_swap(p, 2) for p in za]
        attn_pieces = za + xa + [partner(p) for p in za + xa]
        rel = [0, 4, 8, 12]
        rel = rel + [r ^ 2 for r in rel]
        attn_off = (here ^ jnp.array(rel + [r ^ 1 for r in rel], jnp.int32)) * share
        rel = jnp.array([r ^ j for r in rel for j in (0, 1)], jnp.int32)
        ffn_off = (here ^ rel) * share
        mine, other = halves(w_up)
        up_own = jnp.stack([mine, partner(other)])
        mine, other = halves(w_down)
        down_own = jnp.stack([mine, partner(other)])
        ids = jnp.arange(dp, dtype=jnp.int32) ^ here
        slots = (
            (ids & 1) * (dp // 2)
            + (ids & 2) // 2 * (dp // 4)
            + (ids & 4) // 4 * (dp // 8)
            + (ids & 8) // 8
        )
        n_out = 4
        ffn_chunk, attn_chunk = (dp // 4, e_count, share, hidden), (dp // 4, 4, share, cols)

        up_own = tie(up_own, *za)
        z8u, z4u = dp_swap(up_own, 8), dp_swap(up_own, 4)
        x0u = dp_swap(tie(up_own, *xa), 2)
        x0d = dp_swap(tie(down_own, *xa), 2)
    else:
        attn_pieces = [lax.all_gather(attn_shard, "dp", axis=1, tiled=True)[None]]
        gathered = lax.all_gather(w_up, "dp", axis=1, tiled=True)
        up_pieces = [halves(gathered)[0][None]]
        gathered = lax.all_gather(w_down, "dp", axis=1, tiled=True)
        down_pieces = [halves(gathered)[0][None]]
        attn_off = ffn_off = slots = jnp.zeros((1,), jnp.int32)
        n_out = 1
        ffn_chunk, attn_chunk = (1, e_count, width, hidden), (1, 4, width, cols)

    a, qkv, attn_w, out_w = project(tok_tied, vectors, bias, attn_pieces, attn_off)
    half = width // 2
    out_mine = lax.dynamic_slice_in_dim(out_w, core * half, half, 1)
    stage = [out_w]
    if by_permute:
        stage = stage + [z4u, z8u, x0u, x0d]
        z12u = dp_swap(tie(z8u, *stage), 4)
        x1u = dp_swap(tie(z4u, *stage), 2)
    out_half = peer(tie(out_mine, *stage))
    experts_partner = partner(tie(experts, *stage))
    ctx = attend(tie(text_len, *stage), qkv, scale)
    stage = [ctx, out_half, experts_partner]
    if by_permute:
        stage = stage + [z12u, x1u]
        x2u = dp_swap(tie(z8u, *stage), 2)
        x3u = dp_swap(tie(z12u, *stage), 2)
        z8d, z4d = (dp_swap(tie(down_own, *stage), r) for r in (8, 4))
    ctx_theirs = peer(tie(ctx, *stage))
    out_other = partner(tie(out_half, *stage))
    out_theirs = jnp.where(
        core == 0,
        jnp.concatenate([out_half, out_other], axis=1),
        jnp.concatenate([out_other, out_half], axis=1),
    )
    cots = [jnp.pad(tie(v, *stage), pad) for v in (cotangent, cot_partner)]
    experts_two = jnp.concatenate([experts, experts_partner], axis=1)
    stage = [*cots, ctx]
    if by_permute:
        stage = stage + [x2u]
    h, b = residual(tok, ctx, ctx_theirs, out_w, out_theirs, tie(vectors, *stage))
    stage = [h]
    if by_permute:
        stage = stage + [x3u, z8d, z4d]
        x1d = dp_swap(tie(z4d, *stage), 2)
        x2d = dp_swap(tie(z8d, *stage), 2)
        z12d = dp_swap(tie(z8d, *stage), 4)
        up_pieces = [up_own, z4u, z8u, z12u, x0u, x1u, x2u, x3u]
    b_two = [b, partner(tie(b, *stage))]

    act, slope = experts_up(tie(experts_two, *stage), ffn_off, b_two, b_up_mine, up_pieces)
    stage = [act]
    if by_permute:
        stage = stage + [x1d, z12d]
        x3d = dp_swap(tie(z12d, *stage), 2)
    *down_grad, grad_b_down = weight_grad(
        tie(experts_two, *stage), slots, 0, cots, act, ffn_chunk, n_out, e_count, items
    )
    stage = [grad_b_down]
    if by_permute:
        down_pieces = [down_own, z4d, z8d, z12d, x0d, x1d, x2d, x3d]

        def near(parts, core_slot, *others):
            return dp_swap(tie(parts[2 * core_slot + 1], *others), 2)

        def middle(parts, core_slot, got, *others):
            keep, got = tie(parts[2 * core_slot], got, *others), tie(got, *others)
            both = keep[2:4].astype(F32) + got[2:4].astype(F32)
            return keep, got, both.astype(BF)

        def last(state, mid, *others):
            keep, got, _ = state
            mid = tie(mid, *others)
            part = keep[1].astype(F32) + got[1].astype(F32) + mid[1].astype(F32)
            return keep, got, mid, part.astype(BF)

        def total(state, end, *others, planes=slice(None)):
            keep, got, mid, _ = state
            end = tie(end, *others)
            return (
                keep[0, planes].astype(F32)
                + got[0, planes].astype(F32)
                + mid[0, planes].astype(F32)
                + end[planes].astype(F32)
            )

        ffn_off = (tie(here, x2d, *stage) ^ rel) * share
        stage = stage + [tie(x3d, ffn_off)]
        dn1 = near(down_grad, 1, *stage)
    db_own, db_other, du, grad_b_up = experts_back(
        tie(experts_two, *stage), ffn_off, cots, slope, up_pieces, down_pieces, items
    )
    stage = [du]
    if by_permute:
        d1 = middle(down_grad, 1, dn1, du)
        stage = [d1[2]]
    db = add_low(db_own, partner(tie(db_other, *stage)))
    stage = stage + [db]
    if by_permute:
        df1 = dp_swap(tie(d1[2], *stage), 4)
        dn0 = near(down_grad, 0, *stage)
    db_theirs = peer(tie(db, *stage))
    *up_grad, _ = weight_grad(
        tie(experts_two, *stage), slots, 0, b_two, du, ffn_chunk, n_out, e_count, 0
    )
    stage = [up_grad[0]]
    if by_permute:
        stage = stage + [df1]
        un1 = near(up_grad, 1, *stage)
        d1 = last(d1, df1, *stage)
        dg1 = dp_swap(d1[3], 8)
    z_own, z_other = experts_down(
        tie(experts_two, *stage), ffn_off, act, down_pieces, rows, items
    )
    stage = [z_own, db_theirs]
    if by_permute:
        d0 = middle(down_grad, 0, dn0, *stage)
        stage = stage + [d0[2], dg1]
    z = add_low(z_own, partner(tie(z_other, *stage)))
    stage = stage + [z]
    z_theirs = peer(tie(z, *stage))
    if by_permute:
        df0 = dp_swap(tie(d0[2], *stage), 4)
        un0 = near(up_grad, 0, *stage)

    dh, da, norm_one, norm_two, bias_sums, *attn_parts = attend_back(
        tie(text_len, *stage), slots, db, db_theirs, h, cots[0], tok, a, ctx, qkv, attn_w, out_w, vectors,
        attn_chunk, n_out, scale,
    )
    stage = [bias_sums, z_theirs]
    if by_permute:
        u1 = middle(up_grad, 1, un1, *stage)
        stage = stage + [u1[2], df0]
        uf1 = dp_swap(tie(u1[2], *stage), 4)
        d0 = last(d0, df0, *stage)
        dg0 = dp_swap(d0[3], 8)
    da_theirs = peer(tie(da, bias_sums, z_theirs))
    norm_one_theirs = peer(tie(norm_one, *stage))
    attn_parts = [tie(v, *stage) for v in attn_parts]

    up_pair = jnp.zeros((2, e_count, hidden), F32)
    up_pair = lax.dynamic_update_slice_in_dim(up_pair, grad_b_up[None], core, 0)
    small = jnp.concatenate(
        [
            norm_one + norm_one_theirs,
            norm_two,
            grad_b_down,
            up_pair.reshape(-1, width),
            bias_sums.reshape(-1, width),
        ]
    )
    steps = list(masks)

    def add_step(*others):
        nonlocal small
        small = tie(small, *others)
        got = swap(small, "dp", dp, steps.pop(0))
        small = small + got
        return got

    stage = [norm_one_theirs]
    if by_permute:
        u0 = middle(up_grad, 0, un0, *stage)
        stage = stage + [u0[2]]
        send = add_low(tie(attn_parts[1], *stage), partner(attn_parts[3]))
        keep = add_low(tie(attn_parts[0], *stage), partner(attn_parts[2]))
        an = near([keep, send], 0, *stage)
        uf0 = dp_swap(tie(u0[2], *stage), 4)
        stage = stage + [keep, send]
    got = add_step(*stage)
    output = finish_output(tie(experts, *stage), h, z, z_theirs, b_down, seq)
    stage = [output, got]
    if by_permute:
        stage = stage + [uf1, dg0]
        u1 = last(u1, uf1, *stage)
        ug1 = dp_swap(u1[3], 8)
        stage = [u1[3], got]
        got = add_step(*stage)
        down_other = total(d1, dg1, *stage)
        down_got = partner(down_other)
        u0 = last(u0, uf0, *stage)
        ug0 = dp_swap(u0[3], 8)
        stage = [u0[3], down_other, da_theirs]
        a0 = middle([keep, send], 0, an, *stage)
        stage = stage + [a0[2]]
        af = dp_swap(tie(a0[2], *stage), 4)
        down_mine = total(d0, dg0, *stage)
        stage = stage + [down_mine]
    else:
        got = add_step(*stage)
    stage = [got, *stage]
    grad_tokens = token_grad(dh, da, da_theirs, tok, tie(vectors, *stage), seq)
    stage = [grad_tokens]
    got = add_step(*stage)
    if by_permute:
        up_other = total(u1, ug1, *stage)
        up_got = partner(up_other)
        a0 = last(a0, af, up_other, *stage)
        stage = stage + [a0[3], got]
        got = add_step(*stage)

    if by_permute:

        def joined(own, got):
            whole = jnp.zeros((e_count, share, 2 * hidden), F32)
            whole = lax.dynamic_update_slice_in_dim(whole, got, (1 - core) * hidden, 2)
            return lax.dynamic_update_slice_in_dim(whole, own, core * hidden, 2)

        ag = dp_swap(a0[3], 8)
        grad_w_down = joined(tie(down_mine, a0[3]), down_got)
        grad_w_up = joined(total(u0, ug0, a0[3]), up_got)
        ag = tie(ag, grad_w_up)
        grad_w_qkv = total(a0, ag, planes=slice(0, 3))
        grad_w_out = total(a0, ag, planes=3)
    else:

        def finish(chunk):
            whole = jnp.zeros((e_count, width, 2 * hidden), BF)
            whole = lax.dynamic_update_slice_in_dim(whole, chunk[0], core * hidden, 2)
            return lax.psum_scatter(whole, "dp", scatter_dimension=1, tiled=True).astype(F32)

        grad_w_down, grad_w_up = finish(down_grad[0]), finish(up_grad[0])
        grad_attn = lax.psum_scatter(attn_parts[0][0], "dp", scatter_dimension=1, tiled=True)
        grad_w_qkv, grad_w_out = grad_attn[:3].astype(F32), grad_attn[3].astype(F32)

    while steps:
        add_step()
    at = 5 + e_count
    end = at + e_count * hidden // width
    total_up = jnp.concatenate(
        [small[n : n + end - at].reshape(e_count, hidden) for n in (at, end)], axis=1
    )
    total_qv = small[2 * end - at :].reshape(2, cols)
    return (
        output,
        grad_tokens,
        grad_w_qkv,
        grad_w_out,
        grad_w_up,
        grad_w_down,
        total_qv,
        small[4],
        total_up,
        small[5:at],
        small[:4],
    )


def solution(mesh):
    body = functools.partial(per_device, dp=mesh.shape["dp"], rep=mesh.shape["rep"])
    return jax.shard_map(
        body,
        mesh=mesh,
        in_specs=(
            P("dp", None, None),
            P("dp"),
            P("dp", None),
            P(),
            P(),
            P(None, "dp", "rep"),
            P(None, "rep"),
            P("dp", "rep"),
            P(),
            P(),
            P(),
            P(None, "dp", "rep"),
            P(None, "rep"),
            P(None, "dp", "rep"),
            P(),
            P("dp", None, None),
        ),
        out_specs=(
            P("dp", None, None),
            P("dp", None, None),
            P(None, "dp", "rep"),
            P("dp", "rep"),
            P(None, "dp", "rep"),
            P(None, "dp", "rep"),
            P(None, "rep"),
            P(),
            P(None, "rep"),
            P(),
            P(),
        ),
        check_vma=False,
    )
```

```python
import functools
import math

import jax
import jax.numpy as jnp
from jax import lax
from jax.experimental import pallas as pl
from jax.experimental.pallas import tpu as pltpu
from jax.sharding import PartitionSpec as P

HDIM = 64
IMG = 197
EPSILON = 1e-05
ROOT_HALF = 0.7071067811865476
INV_ROOT_TAU = 0.3989422804014327
SUB = 16
LANES = 128
BF = jnp.bfloat16
F32 = jnp.float32

NN = (((1,), (0,)), ((), ()))
NT = (((1,), (1,)), ((), ()))
TN = (((0,), (0,)), ((), ()))


def up_to(n, m):
    return -(-n // m) * m


def dot(a, b, dims):
    return lax.dot_general(a, b, dims, preferred_element_type=F32)


def full(shape):
    zeros = (0,) * len(shape)
    return pl.BlockSpec(shape, lambda *_: zeros)


def per_item(shape):
    zeros = (0,) * (len(shape) - 1)
    return pl.BlockSpec(shape, lambda i, *_: (i,) + zeros)


ANY = pl.BlockSpec(memory_space=pl.ANY)


def params():
    return pltpu.CompilerParams(vmem_limit_bytes=60 * 1024 * 1024)


SHORT = pl.CostEstimate(flops=1, transcendentals=0, bytes_accessed=1)


def normed(v):
    centred = v - jnp.mean(v, axis=-1, keepdims=True)
    var = jnp.mean(centred * centred, axis=-1, keepdims=True)
    spread = lax.rsqrt(var + EPSILON)
    return centred * spread, spread


def norm_back(grad, hat, spread, gain):
    scaled = grad * gain
    return spread * (
        scaled
        - jnp.mean(scaled, axis=-1, keepdims=True)
        - hat * jnp.mean(scaled * hat, axis=-1, keepdims=True)
    )


def run_copies(copies, *, start=False, wait=False):
    for c in copies:
        if start:
            c.start()
        if wait:
            c.wait()


def place_copies(off_ref, pieces, dest, sems, plane=0):
    copies = []
    for n, piece in enumerate(pieces):
        subs, _, rows, _ = piece.shape
        for j in range(subs):
            at = off_ref[n * subs + j]
            copies.append(
                pltpu.make_async_copy(
                    piece.at[j, plane : plane + dest.shape[0]],
                    dest.at[:, pl.ds(pl.multiple_of(at, SUB), rows), :],
                    sems.at[n * subs + j],
                )
            )
    return copies


def k_proj(off_ref, tok_ref, vec_ref, bias_ref, *rest):
    a_ref, qkv_ref, w_ref, wo_ref, sems, out_sems = rest[-6:]
    pieces = rest[:-6]
    first = pl.program_id(0) == 0

    @pl.when(first)
    def _():
        run_copies(place_copies(off_ref, pieces, w_ref, sems), start=True)
        run_copies(place_copies(off_ref, pieces, wo_ref, out_sems, 3), start=True)

    hat, _ = normed(tok_ref[0].astype(F32))
    a_ref[0] = (hat * vec_ref[0:1, :] + vec_ref[1:2, :]).astype(BF)

    @pl.when(first)
    def _():
        run_copies(place_copies(off_ref, pieces, w_ref, sems), wait=True)
        run_copies(place_copies(off_ref, pieces, wo_ref, out_sems, 3), wait=True)

    a = a_ref[0]
    for t in range(3):
        qkv_ref[t, 0] = (dot(a, w_ref[t], NN) + bias_ref[t : t + 1, :]).astype(BF)


def project(tokens, vectors, bias, pieces, offsets):
    items, rows, width = tokens.shape
    cols = pieces[0].shape[3]
    count = len(pieces) * pieces[0].shape[0]
    grid_spec = pltpu.PrefetchScalarGridSpec(
        num_scalar_prefetch=1,
        grid=(items,),
        in_specs=[
            per_item((1, rows, width)),
            full(vectors.shape),
            full((3, cols)),
        ]
        + [ANY] * len(pieces),
        out_specs=[
            per_item((1, rows, width)),
            pl.BlockSpec((3, 1, rows, cols), lambda i, *_: (0, i, 0, 0)),
            full((3, width, cols)),
            full((1, width, cols)),
        ],
        scratch_shapes=[pltpu.SemaphoreType.DMA((count,)), pltpu.SemaphoreType.DMA((count,))],
    )
    return pl.pallas_call(
        k_proj,
        grid_spec=grid_spec,
        out_shape=[
            jax.ShapeDtypeStruct((items, rows, width), BF),
            jax.ShapeDtypeStruct((3, items, rows, cols), BF),
            jax.ShapeDtypeStruct((3, width, cols), BF),
            jax.ShapeDtypeStruct((1, width, cols), BF),
        ],
        compiler_params=params(),
        cost_estimate=SHORT,
        name="project",
    )(offsets, tokens, vectors, bias, *pieces)


def k_attend(len_ref, q_ref, k_ref, v_ref, c_ref, *, scale):
    rows, width = c_ref.shape[1:]
    length = len_ref[pl.program_id(0)]
    valid = lax.broadcasted_iota(jnp.int32, (1, rows), 1) < IMG + length
    low = lax.broadcasted_iota(jnp.int32, (1, LANES), 1) < HDIM
    for pair in range(width // LANES):
        cols = slice(pair * LANES, (pair + 1) * LANES)
        q, k, v = q_ref[0, 0, :, cols], k_ref[0, 0, :, cols], v_ref[0, 0, :, cols]
        both = []
        for side in (low, ~low):
            s = dot(q * side.astype(BF), k, NT) * scale
            s = jnp.where(valid, s, -1e30)
            e = jnp.exp(s - jnp.max(s, axis=-1, keepdims=True))
            p = (e / jnp.sum(e, axis=-1, keepdims=True)).astype(BF)
            both.append(dot(p, v, NN))
        c_ref[0, :, cols] = jnp.where(low, both[0], both[1]).astype(BF)


def qkv_specs(rows, cols):
    return [pl.BlockSpec((1, 1, rows, cols), lambda i, *_, t=t: (t, i, 0, 0)) for t in range(3)]


def attend(text_len, qkv, scale):
    _, items, rows, cols = qkv.shape
    grid_spec = pltpu.PrefetchScalarGridSpec(
        num_scalar_prefetch=1,
        grid=(items,),
        in_specs=qkv_specs(rows, cols),
        out_specs=per_item((1, rows, cols)),
    )
    return pl.pallas_call(
        functools.partial(k_attend, scale=scale),
        grid_spec=grid_spec,
        out_shape=jax.ShapeDtypeStruct((items, rows, cols), BF),
        compiler_params=params(),
        cost_estimate=SHORT,
        name="attend",
    )(text_len, qkv, qkv, qkv)


def k_residual(tok_ref, cm_ref, cp_ref, wm_ref, wp_ref, vec_ref, h_ref, b_ref):
    y = dot(cm_ref[0], wm_ref[0], NT) + dot(cp_ref[0], wp_ref[0], NT)
    h = tok_ref[0].astype(F32) + (y + vec_ref[2:3, :])
    h_ref[0] = h
    hat, _ = normed(h)
    b_ref[0] = (hat * vec_ref[3:4, :] + vec_ref[4:5, :]).astype(BF)


def residual(tokens, mine, theirs, w_mine, w_theirs, vectors):
    items, rows, width = tokens.shape
    cols = mine.shape[2]
    return pl.pallas_call(
        k_residual,
        grid=(items,),
        in_specs=[
            per_item((1, rows, width)),
            per_item((1, rows, cols)),
            per_item((1, rows, cols)),
            full((1, width, cols)),
            full((1, width, cols)),
            full(vectors.shape),
        ],
        out_specs=[per_item((1, rows, width))] * 2,
        out_shape=[
            jax.ShapeDtypeStruct(tokens.shape, F32),
            jax.ShapeDtypeStruct(tokens.shape, BF),
        ],
        compiler_params=params(),
        cost_estimate=SHORT,
        name="residual",
    )(tokens, mine, theirs, w_mine, w_theirs, vectors)


def segments(rows):
    head = up_to(IMG, SUB)
    tail = IMG // SUB * SUB
    return (0, head), (tail, rows - tail), head


def segment_masks(rows):
    (a0, an), (b0, bn), _ = segments(rows)
    in_a = lax.broadcasted_iota(jnp.int32, (an, 1), 0) + a0 < IMG
    in_b = lax.broadcasted_iota(jnp.int32, (bn, 1), 0) + b0 >= IMG
    return in_a, in_b


def masked_parts(g_ref, i):
    rows = g_ref.shape[1]
    (a0, an), (b0, bn), _ = segments(rows)
    in_a, in_b = segment_masks(rows)
    g_a = jnp.where(in_a, g_ref[i, a0 : a0 + an, :].astype(F32), 0.0)
    g_b = jnp.where(in_b, g_ref[i, b0 : b0 + bn, :].astype(F32), 0.0)
    return g_a, g_b


def item_copies(refs, dest, sems):
    copies = []
    for ref in refs:
        if len(ref.shape) == 2:
            copies.append(
                pltpu.make_async_copy(ref, dest.at[len(copies)], sems.at[len(copies)])
            )
        else:
            for j in range(ref.shape[0]):
                copies.append(
                    pltpu.make_async_copy(ref.at[j], dest.at[len(copies)], sems.at[len(copies)])
                )
    return copies


def wait_item(copies, i):
    for n, c in enumerate(copies):

        @pl.when(i == n)
        def _(c=c):
            c.wait()


def write_chunks(slot_ref, base, acc, stage, outs, sems):
    count, _, rows, _ = stage.shape
    for c in range(count):
        stage[slot_ref[base + c]] = acc[:, c * rows : (c + 1) * rows, :].astype(BF)
    per = count // len(outs)
    copies = [
        pltpu.make_async_copy(stage.at[n * per : (n + 1) * per], out, sems.at[n])
        for n, out in enumerate(outs)
    ]
    run_copies(copies, start=True)
    run_copies(copies, wait=True)


def k_up(e_ref, off_ref, bias_ref, *rest, n_left):
    b_refs, pieces = rest[:n_left], rest[n_left:-6]
    act_ref, slope_ref, b_s, w_s, b_sem, w_sem = rest[-6:]
    i = pl.program_id(0)
    b_copies = item_copies(b_refs, b_s, b_sem)

    @pl.when(i == 0)
    def _():
        run_copies(b_copies[:1], start=True)
        w_copies = place_copies(off_ref, pieces, w_s, w_sem)
        run_copies(w_copies, start=True)
        run_copies(b_copies[1:], start=True)
        run_copies(w_copies, wait=True)

    wait_item(b_copies, i)
    seg_a, seg_b, _ = segments(b_s.shape[1])
    at = 0
    for which, (lo, n) in zip((0, 1), (seg_a, seg_b)):
        e = e_ref[which, i]
        u = dot(b_s[i, lo : lo + n, :], w_s[e], NN) + bias_ref[pl.ds(e, 1), :]
        cdf = 0.5 * (1.0 + lax.erf(u * ROOT_HALF))
        act_ref[0, at : at + n, :] = (u * cdf).astype(BF)
        slope_ref[0, at : at + n, :] = (cdf + u * jnp.exp(-0.5 * u * u) * INV_ROOT_TAU).astype(BF)
        at += n


def experts_up(experts, offsets, b, bias, pieces):
    items = experts.shape[1]
    rows, width = b[0].shape[-2:]
    e_count, _, hidden = pieces[0].shape[1:]
    count = len(pieces) * pieces[0].shape[0]
    (_, an), (_, bn), _ = segments(rows)
    grid_spec = pltpu.PrefetchScalarGridSpec(
        num_scalar_prefetch=2,
        grid=(items,),
        in_specs=[full((e_count, hidden))] + [ANY] * (len(b) + len(pieces)),
        out_specs=[per_item((1, an + bn, hidden))] * 2,
        scratch_shapes=[
            pltpu.VMEM((items, rows, width), BF),
            pltpu.VMEM((e_count, width, hidden), BF),
            pltpu.SemaphoreType.DMA((items,)),
            pltpu.SemaphoreType.DMA((count,)),
        ],
    )
    return pl.pallas_call(
        functools.partial(k_up, n_left=len(b)),
        grid_spec=grid_spec,
        out_shape=[jax.ShapeDtypeStruct((items, an + bn, hidden), BF)] * 2,
        compiler_params=params(),
        cost_estimate=SHORT,
        name="experts_up",
    )(experts, offsets, bias, *b, *pieces)


def k_weight_grad(e_ref, slot_ref, right_ref, *rest, n_left, n_out, base, own):
    lefts = rest[:n_left]
    outs = rest[n_left : n_left + n_out]
    left_s, dw_s, stage, left_sem, out_sem = rest[-5:]
    sums_ref = rest[n_left + n_out]
    i = pl.program_id(0)
    copies = item_copies(lefts, left_s, left_sem)

    @pl.when(i == 0)
    def _():
        run_copies(copies, start=True)
        dw_s[...] = jnp.zeros_like(dw_s)
        sums_ref[...] = jnp.zeros_like(sums_ref)

    wait_item(copies, i)
    at = 0
    for which, left in zip((0, 1), masked_parts(left_s, i)):
        e = e_ref[which, i]
        n = left.shape[0]
        dw_s[e] += dot(left.astype(BF), right_ref[0, at : at + n, :], TN)

        @pl.when(i < own)
        def _(left=left, e=e):
            sums_ref[pl.ds(e, 1), :] += jnp.sum(left, axis=0, keepdims=True)

        at += n

    @pl.when(i == pl.num_programs(0) - 1)
    def _():
        write_chunks(slot_ref, base, dw_s, stage, outs, out_sem)


def weight_grad(experts, slots, base, left, right, chunk, n_out, e_count, own):
    items, seg_rows, hidden = right.shape
    rows, width = left[0].shape[-2:]
    count = chunk[0] * n_out
    grid_spec = pltpu.PrefetchScalarGridSpec(
        num_scalar_prefetch=2,
        grid=(items,),
        in_specs=[per_item((1, seg_rows, hidden))] + [ANY] * len(left),
        out_specs=[ANY] * n_out + [full((e_count, width))],
        scratch_shapes=[
            pltpu.VMEM((items, rows, width), BF),
            pltpu.VMEM((e_count, width, hidden), F32),
            pltpu.VMEM((count,) + chunk[1:], BF),
            pltpu.SemaphoreType.DMA((items,)),
            pltpu.SemaphoreType.DMA((n_out,)),
        ],
    )
    return pl.pallas_call(
        functools.partial(
            k_weight_grad, n_left=len(left), n_out=n_out, base=base, own=own
        ),
        grid_spec=grid_spec,
        out_shape=[jax.ShapeDtypeStruct(chunk, BF)] * n_out
        + [jax.ShapeDtypeStruct((e_count, width), F32)],
        compiler_params=params(),
        cost_estimate=SHORT,
        name="weight_grad",
    )(experts, slots, right, *left)


def store_joined(ref, first, middle, second, tail, head):
    ref[0, :tail, :] = first[:tail].astype(BF)
    ref[0, tail:head, :] = middle.astype(BF)
    ref[0, head:, :] = second[head - tail :].astype(BF)


def k_back(e_ref, off_ref, slope_ref, *rest, n_left, n_up, own):
    g_s, w_up, w_down, sem_g, sem_up, sem_down = rest[-6:]
    do_ref, dp_ref, du_ref, gbu_ref = rest[-10:-6]
    lefts, ups, downs = rest[:n_left], rest[n_left : n_left + n_up], rest[n_left + n_up : -10]
    i = pl.program_id(0)
    copies = item_copies(lefts, g_s, sem_g)

    @pl.when(i == 0)
    def _():
        w_copies = place_copies(off_ref, downs, w_down, sem_down)
        run_copies(copies[:1] + w_copies, start=True)
        more = place_copies(off_ref, ups, w_up, sem_up)
        run_copies(more + copies[1:], start=True)
        gbu_ref[...] = jnp.zeros_like(gbu_ref)
        run_copies(w_copies + more, wait=True)

    wait_item(copies, i)
    rows = g_s.shape[1]
    seg_a, seg_b, head = segments(rows)
    tail = seg_b[0]
    at = 0
    both = []
    for which, g in zip((0, 1), masked_parts(g_s, i)):
        e = e_ref[which, i]
        n = g.shape[0]
        dact = dot(g.astype(BF), w_down[e], NN)
        du = (dact * slope_ref[0, at : at + n, :].astype(F32)).astype(BF)
        du_ref[0, at : at + n, :] = du
        gbu_ref[pl.ds(e, 1), :] += jnp.sum(du.astype(F32), axis=0, keepdims=True)
        both.append(dot(du, w_up[e], NT))
        at += n
    middle = both[0][tail:] + both[1][: head - tail]
    for cond, db_ref in ((i < own, do_ref), (i >= own, dp_ref)):

        @pl.when(cond)
        def _(db_ref=db_ref):
            store_joined(db_ref, both[0], middle, both[1], tail, head)


def own_and_other(rows, width, own):
    block = (1, rows, width)
    return [
        pl.BlockSpec(block, lambda i, *_: (jnp.minimum(i, own - 1), 0, 0)),
        pl.BlockSpec(block, lambda i, *_: (jnp.maximum(i - own, 0), 0, 0)),
    ]


def experts_back(experts, offsets, left, slope, ups, downs, own):
    rows, width = left[0].shape[-2:]
    e_count, _, hidden = ups[0].shape[1:]
    count = len(ups) * ups[0].shape[0]
    items, seg_rows, _ = slope.shape
    grid_spec = pltpu.PrefetchScalarGridSpec(
        num_scalar_prefetch=2,
        grid=(items,),
        in_specs=[per_item((1, seg_rows, hidden))]
        + [ANY] * (len(left) + len(ups) + len(downs)),
        out_specs=own_and_other(rows, width, own)
        + [per_item((1, seg_rows, hidden)), full((e_count, hidden))],
        scratch_shapes=[
            pltpu.VMEM((items, rows, width), BF),
            pltpu.VMEM((e_count, width, hidden), BF),
            pltpu.VMEM((e_count, width, hidden), BF),
            pltpu.SemaphoreType.DMA((items,)),
            pltpu.SemaphoreType.DMA((count,)),
            pltpu.SemaphoreType.DMA((count,)),
        ],
    )
    return pl.pallas_call(
        functools.partial(k_back, n_left=len(left), n_up=len(ups), own=own),
        grid_spec=grid_spec,
        out_shape=[
            jax.ShapeDtypeStruct((own, rows, width), BF),
            jax.ShapeDtypeStruct((items - own, rows, width), BF),
            jax.ShapeDtypeStruct((items, seg_rows, hidden), BF),
            jax.ShapeDtypeStruct((e_count, hidden), F32),
        ],
        compiler_params=params(),
        cost_estimate=SHORT,
        name="experts_back",
    )(experts, offsets, slope, *left, *ups, *downs)


def k_down(e_ref, off_ref, act_ref, *rest, own):
    zo_ref, zp_ref, w_down, sems = rest[-4:]
    pieces = rest[:-4]
    i = pl.program_id(0)

    @pl.when(i == 0)
    def _():
        copies = place_copies(off_ref, pieces, w_down, sems)
        run_copies(copies, start=True)
        run_copies(copies, wait=True)

    rows = zo_ref.shape[1]
    seg_a, seg_b, head = segments(rows)
    tail = seg_b[0]
    z_a = dot(act_ref[0, : seg_a[1], :], w_down[e_ref[0, i]], NT)
    z_b = dot(act_ref[0, seg_a[1] :, :], w_down[e_ref[1, i]], NT)
    image = lax.broadcasted_iota(jnp.int32, (head - tail, 1), 0) + tail < IMG
    middle = jnp.where(image, z_a[tail:], z_b[: head - tail])
    for cond, z_ref in ((i < own, zo_ref), (i >= own, zp_ref)):

        @pl.when(cond)
        def _(z_ref=z_ref):
            store_joined(z_ref, z_a, middle, z_b, tail, head)


def experts_down(experts, offsets, act, pieces, rows, own):
    items, seg_rows, hidden = act.shape
    e_count = pieces[0].shape[1]
    width = sum(p.shape[0] * p.shape[2] for p in pieces)
    count = len(pieces) * pieces[0].shape[0]
    grid_spec = pltpu.PrefetchScalarGridSpec(
        num_scalar_prefetch=2,
        grid=(items,),
        in_specs=[per_item((1, seg_rows, hidden))] + [ANY] * len(pieces),
        out_specs=own_and_other(rows, width, own),
        scratch_shapes=[
            pltpu.VMEM((e_count, width, hidden), BF),
            pltpu.SemaphoreType.DMA((count,)),
        ],
    )
    return pl.pallas_call(
        functools.partial(k_down, own=own),
        grid_spec=grid_spec,
        out_shape=[
            jax.ShapeDtypeStruct((own, rows, width), BF),
            jax.ShapeDtypeStruct((items - own, rows, width), BF),
        ],
        compiler_params=params(),
        cost_estimate=SHORT,
        name="experts_down",
    )(experts, offsets, act, *pieces)


def k_output(e_ref, h_ref, zm_ref, zp_ref, bias_ref, o_ref):
    i = pl.program_id(0)
    rows, keep = h_ref.shape[1], o_ref.shape[1]
    image = lax.broadcasted_iota(jnp.int32, (rows, 1), 0) < IMG
    bias = jnp.where(image, bias_ref[pl.ds(e_ref[0, i], 1), :], bias_ref[pl.ds(e_ref[1, i], 1), :])
    out = h_ref[0] + ((zm_ref[0].astype(F32) + zp_ref[0].astype(F32)) + bias)
    o_ref[0] = out[:keep].astype(BF)


def finish_output(experts, h, mine, theirs, bias, keep):
    items, rows, width = h.shape
    grid_spec = pltpu.PrefetchScalarGridSpec(
        num_scalar_prefetch=1,
        grid=(items,),
        in_specs=[per_item((1, rows, width))] * 3 + [full(bias.shape)],
        out_specs=per_item((1, keep, width)),
    )
    return pl.pallas_call(
        k_output,
        grid_spec=grid_spec,
        out_shape=jax.ShapeDtypeStruct((items, keep, width), BF),
        compiler_params=params(),
        cost_estimate=SHORT,
        name="finish_output",
    )(experts, h, mine, theirs, bias)


def k_attend_back(
    len_ref, slot_ref, dm_ref, dp_ref, h_ref, g_ref, tok_ref, a_ref, c_ref, q_ref, k_ref, v_ref,
    w_ref, wo_ref, vec_ref, dh_ref, da_ref, one_ref, two_ref, bias_ref, *rest, scale,
):
    dqkv, acc, stage, sems = rest[-4:]
    outs = rest[:-4]
    rows, width = dh_ref.shape[1:]
    cols = q_ref.shape[3]
    i = pl.program_id(0)

    @pl.when(i == 0)
    def _():
        one_ref[...] = jnp.zeros_like(one_ref)
        two_ref[...] = jnp.zeros_like(two_ref)
        bias_ref[...] = jnp.zeros_like(bias_ref)
        acc[...] = jnp.zeros_like(acc)

    def add_rows(ref, at, value):
        ref[at : at + 1, :] += jnp.sum(value, axis=0, keepdims=True)

    db = dm_ref[0].astype(F32) + dp_ref[0].astype(F32)
    hat, spread = normed(h_ref[0])
    dh = g_ref[0].astype(F32) + norm_back(db, hat, spread, vec_ref[3:4, :])
    dh_ref[0] = dh
    dy = dh.astype(BF)
    add_rows(two_ref, 0, db * hat)
    add_rows(two_ref, 1, db)
    add_rows(two_ref, 2, dy.astype(F32))
    dctx = dot(dy, wo_ref[0], NN).astype(BF)
    valid = lax.broadcasted_iota(jnp.int32, (rows, 1), 0) < IMG + len_ref[i]
    low = lax.broadcasted_iota(jnp.int32, (1, LANES), 1) < HDIM
    for pair in range(cols // LANES):
        at = slice(pair * LANES, (pair + 1) * LANES)
        q, k, v = q_ref[0, 0, :, at], k_ref[0, 0, :, at], v_ref[0, 0, :, at]
        dc = dctx[:, at]
        parts = []
        for side in (low, ~low):
            only = side.astype(BF)
            s = dot(k * only, q, NT) * scale
            s = jnp.where(valid, s, -1e30)
            e = jnp.exp(s - jnp.max(s, axis=0, keepdims=True))
            p = e / jnp.sum(e, axis=0, keepdims=True)
            dp = dot(v * only, dc, NT)
            ds = (p * (dp - jnp.sum(p * dp, axis=0, keepdims=True))).astype(BF)
            parts.append((dot(ds, k, TN), dot(ds, q, NN), dot(p.astype(BF), dc, NN)))
        dqkv[0, :, at] = (jnp.where(low, parts[0][0], parts[1][0]) * scale).astype(BF)
        dqkv[1, :, at] = (jnp.where(low, parts[0][1], parts[1][1]) * scale).astype(BF)
        dqkv[2, :, at] = jnp.where(low, parts[0][2], parts[1][2]).astype(BF)
    da = dot(dqkv[0], w_ref[0], NT)
    da += dot(dqkv[1], w_ref[1], NT)
    da += dot(dqkv[2], w_ref[2], NT)
    add_rows(bias_ref, 0, dqkv[0].astype(F32))
    add_rows(bias_ref, 1, dqkv[2].astype(F32))
    hat, _ = normed(tok_ref[0].astype(F32))
    add_rows(one_ref, 0, da * hat)
    add_rows(one_ref, 1, da)
    da_ref[0] = da.astype(BF)
    for t in range(3):
        acc[t] += dot(a_ref[0], dqkv[t], TN)
    acc[3] += dot(dy, c_ref[0], TN)

    @pl.when(i == pl.num_programs(0) - 1)
    def _():
        write_chunks(slot_ref, 0, acc, stage, outs, sems)


def attend_back(
    text_len, slots, mine, theirs, h, g, tokens, a, ctx, qkv, weights, w_out, vectors, chunk, n_out, scale
):
    items, rows, width = h.shape
    cols = qkv.shape[3]
    block = per_item((1, rows, width))
    grid_spec = pltpu.PrefetchScalarGridSpec(
        num_scalar_prefetch=2,
        grid=(items,),
        in_specs=[block] * 6
        + [per_item((1, rows, cols))]
        + qkv_specs(rows, cols)
        + [full(weights.shape), full(w_out.shape), full(vectors.shape)],
        out_specs=[block, block, full((2, width)), full((3, width)), full((2, cols))]
        + [ANY] * n_out,
        scratch_shapes=[
            pltpu.VMEM((3, rows, cols), BF),
            pltpu.VMEM((4, width, cols), F32),
            pltpu.VMEM((chunk[0] * n_out,) + chunk[1:], BF),
            pltpu.SemaphoreType.DMA((n_out,)),
        ],
    )
    return pl.pallas_call(
        functools.partial(k_attend_back, scale=scale),
        grid_spec=grid_spec,
        out_shape=[
            jax.ShapeDtypeStruct((items, rows, width), F32),
            jax.ShapeDtypeStruct((items, rows, width), BF),
            jax.ShapeDtypeStruct((2, width), F32),
            jax.ShapeDtypeStruct((3, width), F32),
            jax.ShapeDtypeStruct((2, cols), F32),
        ]
        + [jax.ShapeDtypeStruct(chunk, BF)] * n_out,
        compiler_params=params(),
        cost_estimate=SHORT,
        name="attend_back",
    )(text_len, slots, mine, theirs, h, g, tokens, a, ctx, qkv, qkv, qkv, weights, w_out, vectors)


def k_token_grad(dh_ref, dm_ref, dp_ref, tok_ref, vec_ref, o_ref):
    keep = o_ref.shape[1]
    da = dm_ref[0].astype(F32) + dp_ref[0].astype(F32)
    hat, spread = normed(tok_ref[0].astype(F32))
    out = dh_ref[0] + norm_back(da, hat, spread, vec_ref[0:1, :])
    o_ref[0] = out[:keep]


def token_grad(dh, mine, theirs, tokens, vectors, keep):
    items, rows, width = dh.shape
    return pl.pallas_call(
        k_token_grad,
        grid=(items,),
        in_specs=[per_item((1, rows, width))] * 4 + [full(vectors.shape)],
        out_specs=per_item((1, keep, width)),
        out_shape=jax.ShapeDtypeStruct((items, keep, width), F32),
        compiler_params=params(),
        cost_estimate=SHORT,
        name="token_grad",
    )(dh, mine, theirs, tokens, vectors)


def swap(value, axis, size, mask):
    return lax.ppermute(value, axis, [(i, i ^ mask) for i in range(size)])


def tie(value, *others):
    return lax.optimization_barrier((value,) + others)[0]


def add_low(a, b):
    return (a.astype(F32) + b.astype(F32)).astype(BF)


def per_device(
    tokens, text_len, routes, attn_gain, attn_shift, w_qkv, b_qv, w_out, b_out, ffn_gain, ffn_shift,
    w_up, b_up, w_down, b_down, cotangent, *, dp, rep,
):
    items, seq, width = tokens.shape
    rows = up_to(seq, SUB)
    share = w_qkv.shape[1]
    cols = w_qkv.shape[2]
    hidden = w_up.shape[2] // 2
    e_count = w_up.shape[0]
    scale = 1.0 / math.sqrt(HDIM)
    me = lax.axis_index("dp")
    core = me % 2
    by_permute = dp == 16 and share % SUB == 0
    masks = [m for m in (1, 4, 128, 64, 32, 16, 8, 2) if m < dp]

    def peer(value):
        return lax.ppermute(value, "rep", [(i, i ^ 1) for i in range(rep)])

    def partner(value):
        return swap(value, "dp", dp, 1)

    def dp_swap(value, mask):
        return swap(value, "dp", dp, mask)

    def halves(w):
        mine = lax.dynamic_slice_in_dim(w, core * hidden, hidden, 2)
        other = lax.dynamic_slice_in_dim(w, (1 - core) * hidden, hidden, 2)
        return mine, other

    attn_shard = jnp.concatenate([w_qkv, w_out[None]], axis=0)
    vectors = jnp.stack([attn_gain, attn_shift, b_out, ffn_gain, ffn_shift])
    pad = ((0, 0), (0, rows - seq), (0, 0))
    tok = jnp.pad(tokens, pad)
    bias = jnp.stack([b_qv[0], jnp.zeros_like(b_qv[0]), b_qv[1]])
    experts = jnp.stack([routes[:, 0], routes[:, seq - 1]]).astype(jnp.int32)
    b_up_mine = lax.dynamic_slice_in_dim(b_up, core * hidden, hidden, 1)
    cot_partner = partner(cotangent)
    tok_tied = tie(tok, cot_partner)

    if by_permute:
        here = me.astype(jnp.int32)
        own_attn = attn_shard[None]
        z8a, z4a = dp_swap(own_attn, 8), dp_swap(own_attn, 4)
        za = [own_attn, z4a, z8a, dp_swap(z8a, 4)]
        xa = [dp_swap(p, 2) for p in za]
        attn_pieces = za + xa + [partner(p) for p in za + xa]
        rel = [0, 4, 8, 12]
        rel = rel + [r ^ 2 for r in rel]
        attn_off = (here ^ jnp.array(rel + [r ^ 1 for r in rel], jnp.int32)) * share
        rel = jnp.array([r ^ j for r in rel for j in (0, 1)], jnp.int32)
        ffn_off = (here ^ rel) * share
        mine, other = halves(w_up)
        up_own = jnp.stack([mine, partner(other)])
        mine, other = halves(w_down)
        down_own = jnp.stack([mine, partner(other)])
        ids = jnp.arange(dp, dtype=jnp.int32) ^ here
        slots = (
            (ids & 1) * (dp // 2)
            + (ids & 2) // 2 * (dp // 4)
            + (ids & 4) // 4 * (dp // 8)
            + (ids & 8) // 8
        )
        n_out = 4
        ffn_chunk, attn_chunk = (dp // 4, e_count, share, hidden), (dp // 4, 4, share, cols)

        up_own = tie(up_own, *za)
        z8u, z4u = dp_swap(up_own, 8), dp_swap(up_own, 4)
        x0u = dp_swap(tie(up_own, *xa), 2)
        x0d = dp_swap(tie(down_own, *xa), 2)
    else:
        attn_pieces = [lax.all_gather(attn_shard, "dp", axis=1, tiled=True)[None]]
        gathered = lax.all_gather(w_up, "dp", axis=1, tiled=True)
        up_pieces = [halves(gathered)[0][None]]
        gathered = lax.all_gather(w_down, "dp", axis=1, tiled=True)
        down_pieces = [halves(gathered)[0][None]]
        attn_off = ffn_off = slots = jnp.zeros((1,), jnp.int32)
        n_out = 1
        ffn_chunk, attn_chunk = (1, e_count, width, hidden), (1, 4, width, cols)

    a, qkv, attn_w, out_w = project(tok_tied, vectors, bias, attn_pieces, attn_off)
    half = width // 2
    out_mine = lax.dynamic_slice_in_dim(out_w, core * half, half, 1)
    stage = [out_w]
    if by_permute:
        stage = stage + [z4u, z8u, x0u, x0d]
        z12u = dp_swap(tie(z8u, *stage), 4)
        x1u = dp_swap(tie(z4u, *stage), 2)
    out_half = peer(tie(out_mine, *stage))
    experts_partner = partner(tie(experts, *stage))
    ctx = attend(tie(text_len, *stage), qkv, scale)
    stage = [ctx, out_half, experts_partner]
    if by_permute:
        stage = stage + [z12u, x1u]
        x2u = dp_swap(tie(z8u, *stage), 2)
        x3u = dp_swap(tie(z12u, *stage), 2)
        z8d, z4d = (dp_swap(tie(down_own, *stage), r) for r in (8, 4))
    ctx_theirs = peer(tie(ctx, *stage))
    out_other = partner(tie(out_half, *stage))
    out_theirs = jnp.where(
        core == 0,
        jnp.concatenate([out_half, out_other], axis=1),
        jnp.concatenate([out_other, out_half], axis=1),
    )
    cots = [jnp.pad(tie(v, *stage), pad) for v in (cotangent, cot_partner)]
    experts_two = jnp.concatenate([experts, experts_partner], axis=1)
    stage = [*cots, ctx]
    if by_permute:
        stage = stage + [x2u]
    h, b = residual(tok, ctx, ctx_theirs, out_w, out_theirs, tie(vectors, *stage))
    stage = [h]
    if by_permute:
        stage = stage + [x3u, z8d, z4d]
        x1d = dp_swap(tie(z4d, *stage), 2)
        x2d = dp_swap(tie(z8d, *stage), 2)
        z12d = dp_swap(tie(z8d, *stage), 4)
        up_pieces = [up_own, z4u, z8u, z12u, x0u, x1u, x2u, x3u]
    b_two = [b, partner(tie(b, *stage))]

    act, slope = experts_up(tie(experts_two, *stage), ffn_off, b_two, b_up_mine, up_pieces)
    stage = [act]
    if by_permute:
        stage = stage + [x1d, z12d]
        x3d = dp_swap(tie(z12d, *stage), 2)
    *down_grad, grad_b_down = weight_grad(
        tie(experts_two, *stage), slots, 0, cots, act, ffn_chunk, n_out, e_count, items
    )
    stage = [grad_b_down]
    if by_permute:
        down_pieces = [down_own, z4d, z8d, z12d, x0d, x1d, x2d, x3d]

        def near(parts, core_slot, *others):
            return dp_swap(tie(parts[2 * core_slot + 1], *others), 2)

        def middle(parts, core_slot, got, *others):
            keep, got = tie(parts[2 * core_slot], got, *others), tie(got, *others)
            both = keep[2:4].astype(F32) + got[2:4].astype(F32)
            return keep, got, both.astype(BF)

        def last(state, mid, *others):
            keep, got, _ = state
            mid = tie(mid, *others)
            part = keep[1].astype(F32) + got[1].astype(F32) + mid[1].astype(F32)
            return keep, got, mid, part.astype(BF)

        def total(state, end, *others, planes=slice(None)):
            keep, got, mid, _ = state
            end = tie(end, *others)
            return (
                keep[0, planes].astype(F32)
                + got[0, planes].astype(F32)
                + mid[0, planes].astype(F32)
                + end[planes].astype(F32)
            )

        ffn_off = (tie(here, x2d, *stage) ^ rel) * share
        stage = stage + [tie(x3d, ffn_off)]
        dn1 = near(down_grad, 1, *stage)
    db_own, db_other, du, grad_b_up = experts_back(
        tie(experts_two, *stage), ffn_off, cots, slope, up_pieces, down_pieces, items
    )
    stage = [du]
    if by_permute:
        d1 = middle(down_grad, 1, dn1, du)
        stage = [d1[2]]
    db = add_low(db_own, partner(tie(db_other, *stage)))
    stage = stage + [db]
    if by_permute:
        df1 = dp_swap(tie(d1[2], *stage), 4)
        dn0 = near(down_grad, 0, *stage)
    db_theirs = peer(tie(db, *stage))
    *up_grad, _ = weight_grad(
        tie(experts_two, *stage), slots, 0, b_two, du, ffn_chunk, n_out, e_count, 0
    )
    stage = [up_grad[0]]
    if by_permute:
        stage = stage + [df1]
        un1 = near(up_grad, 1, *stage)
        d1 = last(d1, df1, *stage)
        dg1 = dp_swap(d1[3], 8)
    z_own, z_other = experts_down(
        tie(experts_two, *stage), ffn_off, act, down_pieces, rows, items
    )
    stage = [z_own, db_theirs]
    if by_permute:
        d0 = middle(down_grad, 0, dn0, *stage)
        stage = stage + [d0[2], dg1]
    z = add_low(z_own, partner(tie(z_other, *stage)))
    stage = stage + [z]
    z_theirs = peer(tie(z, *stage))
    if by_permute:
        df0 = dp_swap(tie(d0[2], *stage), 4)
        un0 = near(up_grad, 0, *stage)

    dh, da, norm_one, norm_two, bias_sums, *attn_parts = attend_back(
        tie(text_len, *stage), slots, db, db_theirs, h, cots[0], tok, a, ctx, qkv, attn_w, out_w, vectors,
        attn_chunk, n_out, scale,
    )
    stage = [bias_sums, z_theirs]
    if by_permute:
        u1 = middle(up_grad, 1, un1, *stage)
        stage = stage + [u1[2], df0]
        uf1 = dp_swap(tie(u1[2], *stage), 4)
        d0 = last(d0, df0, *stage)
        dg0 = dp_swap(d0[3], 8)
    da_theirs = peer(tie(da, bias_sums, z_theirs))
    norm_one_theirs = peer(tie(norm_one, *stage))
    attn_parts = [tie(v, *stage) for v in attn_parts]

    up_pair = jnp.zeros((2, e_count, hidden), F32)
    up_pair = lax.dynamic_update_slice_in_dim(up_pair, grad_b_up[None], core, 0)
    small = jnp.concatenate(
        [
            norm_one + norm_one_theirs,
            norm_two,
            grad_b_down,
            up_pair.reshape(-1, width),
            bias_sums.reshape(-1, width),
        ]
    )
    steps = list(masks)

    def add_step(*others):
        nonlocal small
        small = tie(small, *others)
        got = swap(small, "dp", dp, steps.pop(0))
        small = small + got
        return got

    stage = [norm_one_theirs]
    if by_permute:
        u0 = middle(up_grad, 0, un0, *stage)
        stage = stage + [u0[2]]
        send = add_low(tie(attn_parts[1], *stage), partner(attn_parts[3]))
        keep = add_low(tie(attn_parts[0], *stage), partner(attn_parts[2]))
        an = near([keep, send], 0, *stage)
        uf0 = dp_swap(tie(u0[2], *stage), 4)
        stage = stage + [keep, send]
    got = add_step(*stage)
    output = finish_output(tie(experts, *stage), h, z, z_theirs, b_down, seq)
    stage = [output, got]
    if by_permute:
        stage = stage + [uf1, dg0]
        u1 = last(u1, uf1, *stage)
        ug1 = dp_swap(u1[3], 8)
        stage = [u1[3], got]
        got = add_step(*stage)
        down_other = total(d1, dg1, *stage)
        down_got = partner(down_other)
        u0 = last(u0, uf0, *stage)
        ug0 = dp_swap(u0[3], 8)
        stage = [u0[3], down_other, da_theirs]
        a0 = middle([keep, send], 0, an, *stage)
        stage = stage + [a0[2]]
        af = dp_swap(tie(a0[2], *stage), 4)
        down_mine = total(d0, dg0, *stage)
        stage = stage + [down_mine]
    else:
        got = add_step(*stage)
    stage = [got, *stage]
    grad_tokens = token_grad(dh, da, da_theirs, tok, tie(vectors, *stage), seq)
    stage = [grad_tokens]
    got = add_step(*stage)
    if by_permute:
        up_other = total(u1, ug1, *stage)
        up_got = partner(up_other)
        a0 = last(a0, af, up_other, *stage)
        stage = stage + [a0[3], got]
        got = add_step(*stage)

    if by_permute:

        def joined(own, got):
            whole = jnp.zeros((e_count, share, 2 * hidden), F32)
            whole = lax.dynamic_update_slice_in_dim(whole, got, (1 - core) * hidden, 2)
            return lax.dynamic_update_slice_in_dim(whole, own, core * hidden, 2)

        ag = dp_swap(a0[3], 8)
        grad_w_down = joined(tie(down_mine, a0[3]), down_got)
        grad_w_up = joined(total(u0, ug0, a0[3]), up_got)
        ag = tie(ag, grad_w_up)
        grad_w_qkv = total(a0, ag, planes=slice(0, 3))
        grad_w_out = total(a0, ag, planes=3)
    else:

        def finish(chunk):
            whole = jnp.zeros((e_count, width, 2 * hidden), BF)
            whole = lax.dynamic_update_slice_in_dim(whole, chunk[0], core * hidden, 2)
            return lax.psum_scatter(whole, "dp", scatter_dimension=1, tiled=True).astype(F32)

        grad_w_down, grad_w_up = finish(down_grad[0]), finish(up_grad[0])
        grad_attn = lax.psum_scatter(attn_parts[0][0], "dp", scatter_dimension=1, tiled=True)
        grad_w_qkv, grad_w_out = grad_attn[:3].astype(F32), grad_attn[3].astype(F32)

    while steps:
        add_step()
    at = 5 + e_count
    end = at + e_count * hidden // width
    total_up = jnp.concatenate(
        [small[n : n + end - at].reshape(e_count, hidden) for n in (at, end)], axis=1
    )
    total_qv = small[2 * end - at :].reshape(2, cols)
    return (
        output,
        grad_tokens,
        grad_w_qkv,
        grad_w_out,
        grad_w_up,
        grad_w_down,
        total_qv,
        small[4],
        total_up,
        small[5:at],
        small[:4],
    )


def solution(mesh):
    body = functools.partial(per_device, dp=mesh.shape["dp"], rep=mesh.shape["rep"])
    return jax.shard_map(
        body,
        mesh=mesh,
        in_specs=(
            P("dp", None, None),
            P("dp"),
            P("dp", None),
            P(),
            P(),
            P(None, "dp", "rep"),
            P(None, "rep"),
            P("dp", "rep"),
            P(),
            P(),
            P(),
            P(None, "dp", "rep"),
            P(None, "rep"),
            P(None, "dp", "rep"),
            P(),
            P("dp", None, None),
        ),
        out_specs=(
            P("dp", None, None),
            P("dp", None, None),
            P(None, "dp", "rep"),
            P("dp", "rep"),
            P(None, "dp", "rep"),
            P(None, "dp", "rep"),
            P(None, "rep"),
            P(),
            P(None, "rep"),
            P(),
            P(),
        ),
        check_vma=False,
    )
```
